8 devices in a mesh: dp: 2 (over z, y), cp: 4 (over x, core).
Axes of the slice: x: 2, y: 2, z: 1, core: 2. Of those that a mesh axis runs over, the one named last changes fastest.
Arguments:
- hidden: bfloat16 [64, 32, 1024], P('dp'), parts along dimension 0
- memory: bfloat16 [64, 1500, 1024], P('dp', 'cp'), parts along dimension 0
- ln_gain: bfloat16 [1024], replicated
- ln_bias: bfloat16 [1024], replicated
- w_q: bfloat16 [1024, 1024], replicated
- b_q: bfloat16 [1024], replicated
- w_k: bfloat16 [1024, 1024], replicated
- w_v: bfloat16 [1024, 1024], replicated
- b_v: bfloat16 [1024], replicated
- w_o: bfloat16 [1024, 1024], replicated
- b_o: bfloat16 [1024], replicated
- grad_y: bfloat16 [64, 32, 1024], P('dp'), parts along dimension 0
Outputs:
- output 1: bfloat16 [64, 32, 1024], P('dp'), parts along dimension 0
- output 2: bfloat16 [64, 32, 1024], P('dp'), parts along dimension 0
- output 3: bfloat16 [64, 1500, 1024], P('dp', 'cp'), parts along dimension 0
- output 4: float32 [2048], P('dp'), parts along dimension 0
- output 5: float32 [2048], P('dp'), parts along dimension 0
- output 6: float32 [2048, 1024], P('dp'), parts along dimension 0
- output 7: float32 [2048], P('dp'), parts along dimension 0
- output 8: float32 [2048, 1024], P('dp'), parts along dimension 0
- output 9: float32 [2048, 1024], P('dp'), parts along dimension 0
- output 10: float32 [2048], P('dp'), parts along dimension 0
- output 11: float32 [2048, 1024], P('dp'), parts along dimension 0
- output 12: float32 [2048], P('dp'), parts along dimension 0
There are 2 independent parts. The reference program is written for one: setup_inputs(seed, part) draws one part's arguments, and reference() takes and returns one part's arrays. A program takes and returns all parts, laid end to end along the dimension named above; an argument that names none is the same for every part.
All inputs are finite; a program needn't handle non-finite values.
Results may differ from the reference program's by a relative error of at most 0.00976617.
Values are sent between devices in bfloat16 or wider.
A program may use at most 1 GiB of HBM per device.

```python
import math
import jax
import jax.numpy as jnp
from jax import lax

BATCH = 32
TOKENS = 32
FRAMES = 1500
D = 1024
HEADS = 16
HEAD = 64
EPS = 1e-5


def setup_inputs(seed: int = 0, part: int = 0) -> dict:
    root_key = jax.random.key(seed)
    shared_key, group_key = jax.random.split(root_key)
    group_key = jax.random.fold_in(group_key, part)
    act_keys = jax.random.split(group_key, 3)
    weight_keys = jax.random.split(shared_key, 9)
    inv_root = D ** -0.5
    sharpness = math.sqrt(math.log(FRAMES / 16.0))
    qk_std = math.sqrt(sharpness) * inv_root

    def draw(draw_key, dims, spread):
        return (jax.random.normal(draw_key, dims, jnp.float32) * spread).astype(jnp.bfloat16)

    return {
        "hidden": draw(act_keys[0], (BATCH, TOKENS, D), 1.0),
        "memory": draw(act_keys[1], (BATCH, FRAMES, D), 1.0),
        "ln_gain": (1.0 + 0.2 * jax.random.normal(weight_keys[0], (D,), jnp.float32)).astype(jnp.bfloat16),
        "ln_bias": draw(weight_keys[1], (D,), 0.2),
        "w_q": draw(weight_keys[2], (D, D), qk_std),
        "b_q": draw(weight_keys[3], (D,), 0.3),
        "w_k": draw(weight_keys[4], (D, D), qk_std),
        "w_v": draw(weight_keys[5], (D, D), inv_root),
        "b_v": draw(weight_keys[6], (D,), 0.3),
        "w_o": draw(weight_keys[7], (D, D), 2.0 * inv_root),
        "b_o": draw(weight_keys[8], (D,), 0.3),
        "grad_y": draw(act_keys[2], (BATCH, TOKENS, D), 1.0),
    }


def widen(array_in):
    return array_in.astype(jnp.float32)


def reference(hidden, memory, ln_gain, ln_bias, w_q, b_q, w_k, w_v, b_v, w_o, b_o, grad_y):
    logit_scale = HEAD ** -0.5
    hidden_f32 = widen(hidden)
    memory_f32 = widen(memory)
    centered = hidden_f32 - jnp.mean(hidden_f32, axis=-1, keepdims=True)
    inv_std = lax.rsqrt(jnp.mean(centered * centered, axis=-1, keepdims=True) + EPS)
    x_hat = centered * inv_std
    x_norm = (x_hat * widen(ln_gain) + widen(ln_bias)).astype(jnp.bfloat16)
    q_proj = (jnp.einsum("btd,de->bte", widen(x_norm), widen(w_q)) + widen(b_q)).astype(jnp.bfloat16)
    k_proj = jnp.einsum("bfd,de->bfe", memory_f32, widen(w_k)).astype(jnp.bfloat16)
    v_proj = (jnp.einsum("bfd,de->bfe", memory_f32, widen(w_v)) + widen(b_v)).astype(jnp.bfloat16)
    q_heads = widen(q_proj).reshape(BATCH, TOKENS, HEADS, HEAD)
    k_heads = widen(k_proj).reshape(BATCH, FRAMES, HEADS, HEAD)
    v_heads = widen(v_proj).reshape(BATCH, FRAMES, HEADS, HEAD)
    logits = jnp.einsum("bthe,bfhe->bhtf", q_heads, k_heads) * logit_scale
    attn_probs = jax.nn.softmax(logits, axis=-1)
    probs_low = widen(attn_probs.astype(jnp.bfloat16))
    attn_out = jnp.einsum("bhtf,bfhe->bthe", probs_low, v_heads).reshape(BATCH, TOKENS, D).astype(jnp.bfloat16)
    out_y = (hidden_f32 + jnp.einsum("btd,de->bte", widen(attn_out), widen(w_o)) + widen(b_o)).astype(jnp.bfloat16)

    dy_f32 = widen(grad_y)
    grad_wo = jnp.einsum("btd,bte->de", widen(attn_out), dy_f32)
    grad_bo = jnp.sum(dy_f32, axis=(0, 1))
    d_attn = jnp.einsum("bte,de->btd", dy_f32, widen(w_o)).astype(jnp.bfloat16)
    d_heads = widen(d_attn).reshape(BATCH, TOKENS, HEADS, HEAD)
    d_probs = jnp.einsum("bthe,bfhe->bhtf", d_heads, v_heads)
    row_dot = jnp.sum(attn_probs * d_probs, axis=-1, keepdims=True)
    d_logits = widen((attn_probs * (d_probs - row_dot) * logit_scale).astype(jnp.bfloat16))
    grad_q = jnp.einsum("bhtf,bfhe->bthe", d_logits, k_heads).reshape(BATCH, TOKENS, D)
    grad_k = jnp.einsum("bhtf,bthe->bfhe", d_logits, q_heads).reshape(BATCH, FRAMES, D).astype(jnp.bfloat16)
    grad_v = jnp.einsum("bhtf,bthe->bfhe", probs_low, d_heads).reshape(BATCH, FRAMES, D)
    grad_bq = jnp.sum(grad_q, axis=(0, 1))
    grad_bv = jnp.sum(grad_v, axis=(0, 1))
    dq_low = widen(grad_q.astype(jnp.bfloat16))
    dk_low = widen(grad_k)
    dv_low = widen(grad_v.astype(jnp.bfloat16))
    grad_wq = jnp.einsum("btd,bte->de", widen(x_norm), dq_low)
    d_xnorm = jnp.einsum("bte,de->btd", dq_low, widen(w_q))
    grad_wk = jnp.einsum("bfd,bfe->de", memory_f32, dk_low)
    grad_wv = jnp.einsum("bfd,bfe->de", memory_f32, dv_low)
    grad_mem = (jnp.einsum("bfe,de->bfd", dk_low, widen(w_k)) + jnp.einsum("bfe,de->bfd", dv_low, widen(w_v))).astype(jnp.bfloat16)
    grad_ln_gain = jnp.sum(d_xnorm * x_hat, axis=(0, 1))
    grad_ln_bias = jnp.sum(d_xnorm, axis=(0, 1))
    d_hat = d_xnorm * widen(ln_gain)
    d_hidden = inv_std * (d_hat - jnp.mean(d_hat, axis=-1, keepdims=True) - x_hat * jnp.mean(d_hat * x_hat, axis=-1, keepdims=True))
    grad_h = (dy_f32 + d_hidden).astype(jnp.bfloat16)
    return (out_y, grad_h, grad_mem, grad_ln_gain, grad_ln_bias, grad_wq, grad_bq, grad_wk, grad_wv, grad_bv, grad_wo, grad_bo)
```

```python
import functools
import math
import jax
import jax.numpy as jnp
from jax import lax
from jax.experimental import pallas as pl
from jax.experimental.pallas import tpu as pltpu
from jax.sharding import PartitionSpec as P

EPS = 1e-5
HEAD = 64
F, FP, D, T = 375, 384, 1024, 32
NB = 32
NP = NB // 2
STEPS = 2 * NP
W = 512
ROWS = 2 * FP
ACC = D + 8
BF, F32 = jnp.bfloat16, jnp.float32
LOG2 = 0.125 * math.log2(math.e)
MESH = pl.DeviceIdType.MESH
VMEM = pltpu.VMEM


def dotg(a, b, ca, cb):
    return lax.dot_general(a, b, (((ca,), (cb,)), ((), ())), preferred_element_type=F32)


def split_kernel(x_ref, o_ref, s_ref):
    x = x_ref[...].astype(F32).reshape(8 * F, 256)
    for t in range(2):
        s_ref[t] = x[:, 128 * t:128 * (t + 1)]
    for b in range(8):
        for t in range(2):
            y = s_ref[t, pl.ds(b, F, stride=8), :].astype(BF)
            o_ref[b, 0:F, 128 * t:128 * (t + 1)] = y
            o_ref[b, 368:FP, 128 * t:128 * (t + 1)] = jnp.concatenate([y[368:F], jnp.zeros((FP - F, 128), BF)], axis=0)


def split_frames(mt):
    return pl.pallas_call(
        split_kernel, grid=(NB // 8, D // 256), name="split_frames",
        out_shape=jax.ShapeDtypeStruct((NB, FP, D), BF),
        in_specs=[pl.BlockSpec((F, 8, 256), lambda b, c: (0, b, c))],
        out_specs=pl.BlockSpec((8, FP, 256), lambda b, c: (b, 0, c)),
        scratch_shapes=[VMEM((2, 8 * F, 128), F32)],
        compiler_params=pltpu.CompilerParams(vmem_limit_bytes=40 << 20),
    )(mt)


def join_kernel(x_ref, o_ref, s_ref):
    for b in range(8):
        x = x_ref[b, 0:F, :].astype(F32)
        for t in range(2):
            s_ref[t, pl.ds(b, F, stride=8), :] = x[:, 128 * t:128 * (t + 1)]
    y = jnp.concatenate([s_ref[0], s_ref[1]], axis=1)
    o_ref[...] = y.reshape(F, 8, 256).astype(BF)


def join_frames(x):
    return pl.pallas_call(
        join_kernel, grid=(NB // 8, D // 256), name="join_frames",
        out_shape=jax.ShapeDtypeStruct((F, NB, D), BF),
        in_specs=[pl.BlockSpec((8, FP, 256), lambda b, c: (b, 0, c))],
        out_specs=pl.BlockSpec((F, 8, 256), lambda b, c: (0, b, c)),
        scratch_shapes=[VMEM((2, 8 * F, 128), F32)],
        compiler_params=pltpu.CompilerParams(vmem_limit_bytes=40 << 20),
    )(x)


def dm_kernel(a_ref, b_ref, wk_ref, wv_ref, o_ref):
    x = jnp.concatenate([a_ref[0, 0], b_ref[0, 0]], axis=1)
    w = jnp.concatenate([wk_ref[:, :W], wv_ref[:, :W], wk_ref[:, W:], wv_ref[:, W:]], axis=1)
    o_ref[...] = dotg(x, w, 1, 1).astype(BF).reshape(2, FP, D)


def dm_product(dkv, w_k, w_v):
    full = pl.BlockSpec((D, D), lambda p: (0, 0))
    return pl.pallas_call(
        dm_kernel, grid=(NP,), name="dm_product",
        out_shape=jax.ShapeDtypeStruct((NB, FP, D), BF),
        in_specs=[pl.BlockSpec((1, 1, ROWS, D), lambda p: (0, p, 0, 0)), pl.BlockSpec((1, 1, ROWS, D), lambda p: (1, p, 0, 0)), full, full],
        out_specs=pl.BlockSpec((2, FP, D), lambda p: (p, 0, 0)),
        compiler_params=pltpu.CompilerParams(vmem_limit_bytes=56 << 20),
    )(dkv, dkv, w_k, w_v)


def block_mask():
    return lax.broadcasted_iota(jnp.int32, (128, 256), 0) // T == lax.broadcasted_iota(jnp.int32, (128, 256), 1) // HEAD


def block_diag(x, mask):
    return jnp.where(mask, jnp.concatenate([x] * 4, axis=0), jnp.zeros((), BF))


def attn_kernel(m_hbm, q, do, wk, wv, bv, od_hbm, dw_hbm, dkv_hbm,
                mbuf, kv, e_s, dp_s, mt, stats, coef, dkv, acc, od,
                m_sem, dkv_sem, od_sem, dw_sem, st_send, st_recv):
    me = lax.axis_index("cp")

    def m_copy(i):
        return pltpu.make_async_copy(m_hbm.at[pl.ds(2 * (i % NP), 2)], mbuf.at[i % 2], m_sem.at[i % 2])

    def stat_copy(i, k):
        return pltpu.make_async_remote_copy(
            src_ref=stats.at[i % 4, me], dst_ref=stats.at[i % 4, me],
            send_sem=st_send.at[i % 4, k - 1], recv_sem=st_recv.at[i % 4, me],
            device_id={"cp": (me + k) % 4}, device_id_type=MESH)

    def stat_wait(i, k):
        src = (me + k) % 4
        pltpu.make_async_remote_copy(
            src_ref=stats.at[i % 4, src], dst_ref=stats.at[i % 4, src],
            send_sem=st_send.at[i % 4, k - 1], recv_sem=st_recv.at[i % 4, src],
            device_id={"cp": src}, device_id_type=MESH).wait_recv()

    def dkv_copy(i):
        return pltpu.make_async_copy(dkv.at[i % 2], dkv_hbm.at[i // NP, i % NP], dkv_sem.at[i % 2])

    def od_copy(i):
        return pltpu.make_async_copy(
            od.at[i % 2], od_hbm.at[:, pl.ds(64 * (i % NP), 64), pl.ds(pl.multiple_of(W * (i // NP), W), W)], od_sem.at[i % 2])

    def operands(i, j, h):
        cols = pl.ds(pl.multiple_of(W * (i // NP) + 256 * h, 256), 256)
        rows = pl.ds(pl.multiple_of(64 * (i % NP) + T * j, T), T)
        mask = block_mask()
        return block_diag(q[rows, cols], mask), block_diag(do[rows, cols], mask), mask

    def stage_a(i):
        slot = i % 2
        m = mbuf[slot].reshape(ROWS, D)
        cols = pl.ds(pl.multiple_of(W * (i // NP), W), W)
        kv[slot, :, 0:W] = jnp.dot(m, wk[:, cols], preferred_element_type=F32).astype(BF)
        kv[slot, :, W:] = (jnp.dot(m, wv[:, cols], preferred_element_type=F32) + bv[:, cols]).astype(BF)
        mt[slot] = m.T
        real = lax.broadcasted_iota(jnp.int32, (FP, 128), 0) < F
        for j in range(2):
            rows = slice(FP * j, FP * (j + 1))
            for h in range(2):
                n = 2 * j + h
                qb, db, _ = operands(i, j, h)
                s = dotg(kv[slot, rows, 256 * h:256 * (h + 1)], qb, 1, 1)
                dp = dotg(kv[slot, rows, W + 256 * h:W + 256 * (h + 1)], db, 1, 1)
                s = jnp.where(real, s, -1e30)
                top = jnp.max(s, axis=0, keepdims=True)
                e = jnp.exp2((s - top) * LOG2)
                e_s[slot, n] = e
                dp_s[slot, n] = dp
                stats[i % 4, me, n:n + 1, :] = top
                stats[i % 4, me, 4 + n:5 + n, :] = jnp.sum(e, axis=0, keepdims=True)
                stats[i % 4, me, 8 + n:9 + n, :] = jnp.sum(e * dp, axis=0, keepdims=True)

    def combine(i):
        slot = i % 4
        tops = [stats[slot, d, 0:4, :] for d in range(4)]
        top = jnp.maximum(jnp.maximum(tops[0], tops[1]), jnp.maximum(tops[2], tops[3]))
        ws = [jnp.exp2((t - top) * LOG2) for t in tops]
        total = sum(stats[slot, d, 4:8, :] * ws[d] for d in range(4))
        dots = sum(stats[slot, d, 8:12, :] * ws[d] for d in range(4))
        coef[0:4, :] = jnp.exp2((stats[slot, me, 0:4, :] - top) * LOG2) / total
        coef[4:8, :] = dots / total

    def stage_b(i):
        slot = i % 2
        grp = i // NP
        for j in range(2):
            rows = slice(FP * j, FP * (j + 1))
            for h in range(2):
                n = 2 * j + h
                qb, db, mask = operands(i, j, h)
                ck, cv = slice(256 * h, 256 * (h + 1)), slice(W + 256 * h, W + 256 * (h + 1))
                p = e_s[slot, n] * coef[n:n + 1, :]
                pb = p.astype(BF)
                gb = (p * (dp_s[slot, n] - coef[4 + n:5 + n, :]) * 0.125).astype(BF)
                o = dotg(pb, kv[slot, rows, cv], 0, 0)
                dq = dotg(gb, kv[slot, rows, ck], 0, 0)
                for which, x in ((0, o), (1, dq)):
                    x = jnp.where(mask, x, 0.0)
                    x = (x[0:32] + x[32:64]) + (x[64:96] + x[96:128])
                    od[slot, which, T * j:T * (j + 1), ck] = x
                    if which == 1:
                        acc[grp, D:D + 1, ck] += jnp.sum(x, axis=0, keepdims=True)
                dk = jnp.dot(gb, qb, preferred_element_type=F32)
                dv = jnp.dot(pb, db, preferred_element_type=F32)
                dkv[slot, rows, ck] = dk.astype(BF)
                dkv[slot, rows, cv] = dv.astype(BF)
                acc[grp, D:D + 1, cv] += jnp.sum(dv, axis=0, keepdims=True)
        acc[grp, 0:D, :] += jnp.dot(mt[slot], dkv[slot], preferred_element_type=F32)

    def part_a(i):
        m_copy(i).wait()

        @pl.when(i + 1 < STEPS)
        def _():
            m_copy(i + 1).start()

        stage_a(i)
        for k in range(1, 4):
            stat_copy(i, k).start()

    def part_b(i):
        for k in range(1, 4):
            stat_wait(i, k)
            stat_copy(i, k).wait_send()

        @pl.when(i >= 2)
        def _():
            dkv_copy(i - 2).wait()
            od_copy(i - 2).wait()

        combine(i)
        stage_b(i)
        dkv_copy(i).start()
        od_copy(i).start()

    m_copy(0).start()
    for g in range(2):
        acc[g] = jnp.zeros((ACC, D), F32)
    barrier = pltpu.get_barrier_semaphore()
    for k in range(1, 4):
        pl.semaphore_signal(barrier, inc=1, device_id={"cp": (me + k) % 4}, device_id_type=MESH)
    pl.semaphore_wait(barrier, 3)
    part_a(jnp.int32(0))

    def step(i, carry):
        part_a(i)
        part_b(i - 1)
        return carry

    lax.fori_loop(1, STEPS, step, 0)
    part_b(jnp.int32(STEPS - 1))
    out = pltpu.make_async_copy(acc, dw_hbm, dw_sem)
    out.start()
    for i in (STEPS - 2, STEPS - 1):
        dkv_copy(i).wait()
        od_copy(i).wait()
    out.wait()


def attention(m_pad, q, do, w_k, w_v, b_v):
    vm = pl.BlockSpec(memory_space=VMEM)
    hbm = pl.BlockSpec(memory_space=pl.ANY)
    dma = pltpu.SemaphoreType.DMA
    return pl.pallas_call(
        attn_kernel, name="attention",
        out_shape=(jax.ShapeDtypeStruct((2, NB * T, D), F32), jax.ShapeDtypeStruct((2, ACC, D), F32),
                   jax.ShapeDtypeStruct((2, NP, ROWS, D), BF)),
        in_specs=[hbm, vm, vm, vm, vm, vm],
        out_specs=(hbm, hbm, hbm),
        scratch_shapes=[
            VMEM((2, 2, FP, D), BF), VMEM((2, ROWS, D), BF), VMEM((2, 4, FP, 128), F32), VMEM((2, 4, FP, 128), F32),
            VMEM((2, D, ROWS), BF), VMEM((4, 4, 16, 128), F32), VMEM((8, 128), F32), VMEM((2, ROWS, D), BF),
            VMEM((2, ACC, D), F32), VMEM((2, 2, 64, W), F32),
            dma((2,)), dma((2,)), dma((2,)), dma, dma((4, 3)), dma((4, 4))],
        compiler_params=pltpu.CompilerParams(vmem_limit_bytes=60 << 20, collective_id=0, has_side_effects=True),
    )(m_pad, q, do, w_k, w_v, b_v)


def solution(mesh):
    act_spec = P("dp", None, None)
    mem_spec = P("dp", "cp", None)
    vec_out = P("dp")
    mat_out = P("dp", None)
    in_specs = (act_spec, mem_spec, P(), P(), P(), P(), P(), P(), P(), P(), P(), act_spec)
    out_specs = (act_spec, act_spec, mem_spec, vec_out, vec_out, mat_out, vec_out, mat_out, mat_out, vec_out, mat_out, vec_out)

    def device_step(hidden, memory, ln_gain, ln_bias, w_q, b_q, w_k, w_v, b_v, w_o, b_o, grad_y):
        h = hidden.reshape(NB * T, D).astype(F32)
        dy = grad_y.reshape(NB * T, D)
        centered = h - jnp.mean(h, axis=-1, keepdims=True)
        inv_std = lax.rsqrt(jnp.mean(centered * centered, axis=-1, keepdims=True) + EPS)
        x_hat = centered * inv_std
        gain = ln_gain.astype(F32)
        x = (x_hat * gain + ln_bias.astype(F32)).astype(BF)
        q = (jnp.dot(x, w_q, preferred_element_type=F32) + b_q.astype(F32)).astype(BF)
        do = dotg(dy, w_o, 1, 1).astype(BF)
        m_pad = split_frames(memory.transpose(1, 0, 2))
        od, dw, dkv = attention(m_pad, q, do, w_k, w_v, b_v.astype(F32).reshape(1, D))
        od = lax.psum(od, "cp")
        dw = lax.psum(dw, "cp")
        grad_mem = join_frames(dm_product(dkv, w_k, w_v)).transpose(1, 0, 2)
        o = od[0].astype(BF)
        dq = od[1].astype(BF)
        out_y = (h + jnp.dot(o, w_o, preferred_element_type=F32) + b_o.astype(F32)).astype(BF)
        grad_wo = dotg(o, dy, 0, 0)
        grad_bo = jnp.sum(dy, axis=0, dtype=F32)
        grad_wk = jnp.concatenate([dw[0, :D, :W], dw[1, :D, :W]], axis=1)
        grad_wv = jnp.concatenate([dw[0, :D, W:], dw[1, :D, W:]], axis=1)
        grad_bq = jnp.concatenate([dw[0, D, :W], dw[1, D, :W]])
        grad_bv = jnp.concatenate([dw[0, D, W:], dw[1, D, W:]])
        grad_wq = dotg(x, dq, 0, 0)
        d_x = dotg(dq, w_q, 1, 1)
        grad_gain = jnp.sum(d_x * x_hat, axis=0)
        grad_bias = jnp.sum(d_x, axis=0)
        d_hat = d_x * gain
        d_h = inv_std * (d_hat - jnp.mean(d_hat, axis=-1, keepdims=True) - x_hat * jnp.mean(d_hat * x_hat, axis=-1, keepdims=True))
        grad_h = (dy.astype(F32) + d_h).astype(BF)
        return (out_y.reshape(NB, T, D), grad_h.reshape(NB, T, D), grad_mem, grad_gain, grad_bias, grad_wq, grad_bq,
                grad_wk, grad_wv, grad_bv, grad_wo, grad_bo)

    return jax.shard_map(device_step, mesh=mesh, in_specs=in_specs, out_specs=out_specs, check_vma=False)
```

```python
import functools
import math
import jax
import jax.numpy as jnp
from jax import lax
from jax.experimental import pallas as pl
from jax.experimental.pallas import tpu as pltpu
from jax.sharding import PartitionSpec as P

EPS = 1e-5
HEAD = 64
F, FP, D, T = 375, 384, 1024, 32
NB = 32
NP = NB // 2
STEPS = 2 * NP
W = 512
ROWS = 2 * FP
BF, F32 = jnp.bfloat16, jnp.float32
LOG2 = 0.125 * math.log2(math.e)
MESH = pl.DeviceIdType.MESH
VMEM = pltpu.VMEM


def dotg(a, b, ca, cb):
    return lax.dot_general(a, b, (((ca,), (cb,)), ((), ())), preferred_element_type=F32)


def split_kernel(x_ref, o_ref, s_ref):
    x = x_ref[...].astype(F32).reshape(8 * F, 256)
    for t in range(2):
        s_ref[t] = x[:, 128 * t:128 * (t + 1)]
    for b in range(8):
        for t in range(2):
            y = s_ref[t, pl.ds(b, F, stride=8), :].astype(BF)
            o_ref[b, 0:F, 128 * t:128 * (t + 1)] = y
            o_ref[b, 368:FP, 128 * t:128 * (t + 1)] = jnp.concatenate([y[368:F], jnp.zeros((FP - F, 128), BF)], axis=0)


def split_frames(mt):
    return pl.pallas_call(
        split_kernel, grid=(NB // 8, D // 256), name="split_frames",
        out_shape=jax.ShapeDtypeStruct((NB, FP, D), BF),
        in_specs=[pl.BlockSpec((F, 8, 256), lambda b, c: (0, b, c))],
        out_specs=pl.BlockSpec((8, FP, 256), lambda b, c: (b, 0, c)),
        scratch_shapes=[VMEM((2, 8 * F, 128), F32)],
        compiler_params=pltpu.CompilerParams(vmem_limit_bytes=40 << 20),
    )(mt)


def join_kernel(x_ref, o_ref, s_ref):
    for b in range(8):
        x = x_ref[b, 0:F, :].astype(F32)
        for t in range(2):
            s_ref[t, pl.ds(b, F, stride=8), :] = x[:, 128 * t:128 * (t + 1)]
    y = jnp.concatenate([s_ref[0], s_ref[1]], axis=1)
    o_ref[...] = y.reshape(F, 8, 256).astype(BF)


def join_frames(x):
    return pl.pallas_call(
        join_kernel, grid=(NB // 8, D // 256), name="join_frames",
        out_shape=jax.ShapeDtypeStruct((F, NB, D), BF),
        in_specs=[pl.BlockSpec((8, FP, 256), lambda b, c: (b, 0, c))],
        out_specs=pl.BlockSpec((F, 8, 256), lambda b, c: (0, b, c)),
        scratch_shapes=[VMEM((2, 8 * F, 128), F32)],
        compiler_params=pltpu.CompilerParams(vmem_limit_bytes=40 << 20),
    )(x)


def block_mask():
    return lax.broadcasted_iota(jnp.int32, (128, 256), 0) // T == lax.broadcasted_iota(jnp.int32, (128, 256), 1) // HEAD


def block_diag(x, mask):
    return jnp.where(mask, jnp.concatenate([x] * 4, axis=0), jnp.zeros((), BF))


def when(cond):
    if isinstance(cond, bool):
        return (lambda f: f()) if cond else (lambda f: None)
    return pl.when(cond)


CH = 64
NCH = D // 2 // CH


def attn_kernel(m_hbm, q, do, wk, wv, bv, res_hbm, dw_hbm, bias_hbm, dm_hbm, dkv_hbm,
                mbuf, kv, e_s, dp_s, mt, stats, coef, dkv, acc, bias, od, r1, keep, x2, r2, res, big1, big2,
                m_sem, dkv_sem, dm_sem, out_sem, st_send, st_recv, s1_send, s1_recv, s2_send, s2_recv,
                s3_send, s3_recv, s3s_send, s4_send, res_recv, e1_send, e1_recv, e2_send, e2_recv,
                e3_send, e3_recv, e3s_send, e4_send, acc_recv, b_send, b_recv, free_sib, free_xn):
    me = lax.axis_index("cp")
    cx, cc = me // 2, me % 2
    sib, xn = 2 * cx + 1 - cc, 2 * (1 - cx) + cc

    def remote(src, dst, ss, rs, dev):
        return pltpu.make_async_remote_copy(src_ref=src, dst_ref=dst, send_sem=ss, recv_sem=rs,
                                            device_id={"cp": dev}, device_id_type=MESH)

    def m_copy(i):
        return pltpu.make_async_copy(m_hbm.at[pl.ds(2 * (i % NP), 2)], mbuf.at[i % 2], m_sem.at[i % 2])

    def dkv_copy(i):
        return pltpu.make_async_copy(dkv.at[i % 2], dkv_hbm.at[i // NP, i % NP], dkv_sem.at[i % 2])

    def stat_copy(i, src, k):
        return remote(stats.at[i % 4, src], stats.at[i % 4, src], st_send.at[i % 4, k - 1], st_recv.at[i % 4, src], (me + k) % 4)

    def s1(b):
        return remote(od.at[b % 2, 1 - cc], r1.at[b % 4], s1_send.at[b % 4], s1_recv.at[b % 4], sib)

    def s2(b):
        return remote(x2.at[b % 4], r2.at[b % 8], s2_send.at[b % 8], s2_recv.at[b % 8], xn)

    def res_at(b, x):
        return res.at[cc, pl.ds(pl.multiple_of(64 * (b % NP) + T * x, T), T), pl.ds(pl.multiple_of(W * (b // NP), W), W)]

    def s3(b, x):
        return remote(res_at(b, x), res_at(b, x), s3_send.at[b % 8], s3_recv.at[b % 8], xn)

    def s3s(b):
        return remote(res_at(b, cx), res_at(b, cx), s3s_send.at[b % 4], res_recv, sib)

    def s4(b):
        return remote(res_at(b, 1 - cx), res_at(b, 1 - cx), s4_send.at[b % 4], res_recv, sib)

    def od_pre(b, inside):
        def on(k):
            return (b >= k) if inside else (b - k < STEPS)

        @when(on(7))
        def _():
            s4(b - 7).wait_send()

        @when(on(5))
        def _():
            s3(b - 5, 1 - cx).wait_recv()
            s4(b - 5).start()
            s3(b - 5, cx).wait_send()
            s3s(b - 5).wait_send()

        @when(on(3))
        def _():
            s2(b - 3).wait_recv()
            s2(b - 3).wait_send()
            res_at(b - 3, cx)[...] = (keep[(b - 3) % 4] + r2[(b - 3) % 8]).astype(BF)

        @when(on(2))
        def _():
            s1(b - 2).wait_send()

        @when(on(1))
        def _():
            s1(b - 1).wait_recv()
            for ref, x in ((keep, cx), (x2, 1 - cx)):
                rows = pl.ds(pl.multiple_of(T * x, T), T)
                ref[(b - 1) % 4] = od[(b - 1) % 2, cc, rows, :] + r1[(b - 1) % 4, rows, :]

    def od_post(b, inside):
        def on(k):
            return (b >= k) if inside else (b - k < STEPS)

        if inside:
            s1(b).start()

        @when(on(1))
        def _():
            s2(b - 1).start()

        @when(on(3))
        def _():
            s3(b - 3, cx).start()
            s3s(b - 3).start()

    own = pl.ds(pl.multiple_of(W * cc, W), W)
    other = pl.ds(pl.multiple_of(W * (1 - cc), W), W)

    def rows_of(x, n):
        return pl.ds(pl.multiple_of(x * (D // 2) + CH * n, CH), CH)

    def e1(g):
        return remote(acc.at[g, :, other], big1, e1_send.at[g], e1_recv.at[g], sib)

    def e2(g, n):
        return remote(acc.at[g, rows_of(1 - cx, n), own], big2.at[g, pl.ds(pl.multiple_of(CH * n, CH), CH)],
                      e2_send.at[g, n], e2_recv.at[g, n], xn)

    def e3(g, n, x):
        ref = acc.at[g, rows_of(x, n), own]
        return remote(ref, ref, e3_send.at[g, n], e3_recv.at[g, n], xn)

    def to_sib(g, n, x, sem):
        ref = acc.at[g, rows_of(x, n), own]
        return remote(ref, ref, sem.at[g, n], acc_recv.at[g], sib)

    def dw_copy(g):
        return pltpu.make_async_copy(acc.at[g], dw_hbm.at[g], out_sem.at[g])

    def exchange(g, t, t3, t4):
        @when(t == 0)
        def _():
            e1(g).start()

        @when(t == 1)
        def _():
            e1(g).wait_send()
            pl.semaphore_signal(free_sib.at[g], inc=1, device_id={"cp": sib}, device_id_type=MESH)
            e1(g).wait_recv()

        @when(t == t3)
        def _():
            pl.semaphore_wait(free_sib.at[g], 1)

        def chunk(t0, f):
            n = t - t0
            if isinstance(n, int):
                if 0 <= n < NCH:
                    f(n)
            else:
                pl.when((n >= 0) & (n < NCH))(lambda: f(n))

        def reduce_core(n):
            for x in (cx, 1 - cx):
                acc[g, rows_of(x, n), own] += big1[rows_of(x, n), :]
            e2(g, n).start()

        def sent(n):
            e2(g, n).wait_send()
            pl.semaphore_signal(free_xn.at[g], inc=1, device_id={"cp": xn}, device_id_type=MESH)

        def reduce_chip(n):
            e2(g, n).wait_recv()
            pl.semaphore_wait(free_xn.at[g], 1)
            acc[g, rows_of(cx, n), own] += big2[g, pl.ds(pl.multiple_of(CH * n, CH), CH), :]
            e3(g, n, cx).start()
            to_sib(g, n, cx, e3s_send).start()

        def forward(n):
            e3(g, n, 1 - cx).wait_recv()
            to_sib(g, n, 1 - cx, e4_send).start()

        chunk(1, reduce_core)
        chunk(t3 - 1, sent)
        chunk(t3, reduce_chip)
        chunk(t4, forward)

        @when(t == t4 + NCH + 1)
        def _():
            remote(acc.at[g, :, other], acc.at[g, :, other], e1_send.at[g], acc_recv.at[g], sib).wait_recv()
            for n in range(NCH):
                e3(g, n, cx).wait_send()
                to_sib(g, n, cx, e3s_send).wait_send()
                to_sib(g, n, 1 - cx, e4_send).wait_send()
            dw_copy(g).start()

    def operands(i, j, h):
        cols = pl.ds(pl.multiple_of(W * (i // NP) + 256 * h, 256), 256)
        rows = pl.ds(pl.multiple_of(64 * (i % NP) + T * j, T), T)
        mask = block_mask()
        return block_diag(q[rows, cols], mask), block_diag(do[rows, cols], mask), mask

    def stage_a(i):
        slot = i % 2
        m = mbuf[slot].reshape(ROWS, D)
        cols = pl.ds(pl.multiple_of(W * (i // NP), W), W)
        kv[slot, :, 0:W] = jnp.dot(m, wk[:, cols], preferred_element_type=F32).astype(BF)
        kv[slot, :, W:] = (jnp.dot(m, wv[:, cols], preferred_element_type=F32) + bv[:, cols]).astype(BF)
        mt[slot] = m.T
        real = lax.broadcasted_iota(jnp.int32, (FP, 128), 0) < F
        for j in range(2):
            rows = slice(FP * j, FP * (j + 1))
            for h in range(2):
                n = 2 * j + h
                qb, db, _ = operands(i, j, h)
                s = dotg(kv[slot, rows, 256 * h:256 * (h + 1)], qb, 1, 1)
                dp = dotg(kv[slot, rows, W + 256 * h:W + 256 * (h + 1)], db, 1, 1)
                s = jnp.where(real, s, -1e30)
                top = jnp.max(s, axis=0, keepdims=True)
                e = jnp.exp2((s - top) * LOG2)
                e_s[slot, n] = e
                dp_s[slot, n] = dp
                stats[i % 4, me, n:n + 1, :] = top
                stats[i % 4, me, 4 + n:5 + n, :] = jnp.sum(e, axis=0, keepdims=True)
                stats[i % 4, me, 8 + n:9 + n, :] = jnp.sum(e * dp, axis=0, keepdims=True)

    def combine(i):
        slot = i % 4
        tops = [stats[slot, d, 0:4, :] for d in range(4)]
        top = jnp.maximum(jnp.maximum(tops[0], tops[1]), jnp.maximum(tops[2], tops[3]))
        ws = [jnp.exp2((t - top) * LOG2) for t in tops]
        total = sum(stats[slot, d, 4:8, :] * ws[d] for d in range(4))
        dots = sum(stats[slot, d, 8:12, :] * ws[d] for d in range(4))
        coef[0:4, :] = jnp.exp2((stats[slot, me, 0:4, :] - top) * LOG2) / total
        coef[4:8, :] = dots / total

    def stage_b(i):
        slot = i % 2
        grp = i // NP
        for j in range(2):
            rows = slice(FP * j, FP * (j + 1))
            for h in range(2):
                n = 2 * j + h
                qb, db, mask = operands(i, j, h)
                ck, cv = slice(256 * h, 256 * (h + 1)), slice(W + 256 * h, W + 256 * (h + 1))
                p = e_s[slot, n] * coef[n:n + 1, :]
                pb = p.astype(BF)
                gb = (p * (dp_s[slot, n] - coef[4 + n:5 + n, :]) * 0.125).astype(BF)
                o = dotg(pb, kv[slot, rows, cv], 0, 0)
                dq = dotg(gb, kv[slot, rows, ck], 0, 0)
                for which, x in ((0, o), (1, dq)):
                    x = jnp.where(mask, x, 0.0)
                    x = (x[0:32] + x[32:64]) + (x[64:96] + x[96:128])
                    od[slot, which, T * j:T * (j + 1), ck] = x
                    if which == 1:
                        bias[me, pl.ds(grp, 1), ck] += jnp.sum(x, axis=0, keepdims=True)
                dk = jnp.dot(gb, qb, preferred_element_type=F32)
                dv = jnp.dot(pb, db, preferred_element_type=F32)
                dkv[slot, rows, ck] = dk.astype(BF)
                dkv[slot, rows, cv] = dv.astype(BF)
                bias[me, pl.ds(grp, 1), cv] += jnp.sum(dv, axis=0, keepdims=True)
        acc[grp] += jnp.dot(mt[slot], dkv[slot], preferred_element_type=F32)

    def part_a(i):
        m_copy(i).wait()

        @pl.when(i + 1 < STEPS)
        def _():
            m_copy(i + 1).start()

        stage_a(i)
        for k in range(1, 4):
            stat_copy(i, me, k).start()

    def part_b(b):
        exchange(0, b - NP, 9, 12)
        for k in range(1, 4):
            stat_copy(b, (me + k) % 4, k).wait_recv()

        @pl.when(b >= 1)
        def _():
            for k in range(1, 4):
                stat_copy(b - 1, me, k).wait_send()

        @pl.when(b >= 2)
        def _():
            dkv_copy(b - 2).wait()

        od_pre(b, True)
        combine(b)
        stage_b(b)
        dkv_copy(b).start()
        od_post(b, True)

    m_copy(0).start()
    for g in range(2):
        acc[g] = jnp.zeros((D, D), F32)
    bias[me] = jnp.zeros((8, D), F32)
    barrier = pltpu.get_barrier_semaphore()
    for k in range(1, 4):
        pl.semaphore_signal(barrier, inc=1, device_id={"cp": (me + k) % 4}, device_id_type=MESH)
    pl.semaphore_wait(barrier, 3)
    part_a(jnp.int32(0))

    def step(i, carry):
        part_a(i)
        part_b(i - 1)
        return carry

    lax.fori_loop(1, STEPS, step, 0)
    part_b(jnp.int32(STEPS - 1))

    def b_copy(k, src):
        return remote(bias.at[src], bias.at[src], b_send.at[k - 1], b_recv.at[src], (me + k) % 4)

    for k in range(1, 4):
        b_copy(k, me).start()
        stat_copy(STEPS - 1, me, k).wait_send()
    dkv_copy(STEPS - 2).wait()
    dkv_copy(STEPS - 1).wait()

    bufs = (kv, dkv)

    def c_load(c, s):
        return [pltpu.make_async_copy(dkv_hbm.at[g, c], bufs[s].at[g], m_sem.at[g] if s == 0 else dkv_sem.at[g]) for g in range(2)]

    def dm_copy(c, s):
        return pltpu.make_async_copy(mbuf.at[s], dm_hbm.at[pl.ds(2 * c, 2)], dm_sem.at[s])

    for cp in c_load(0, 0):
        cp.start()

    def c_step(u, carry):
        for s in range(2):
            c = 2 * u + s
            for cp in c_load(c, s):
                cp.wait()

            @pl.when(c + 1 < NP)
            def _():
                for cp in c_load(c + 1, 1 - s):
                    cp.start()

            @pl.when(c >= 2)
            def _():
                dm_copy(c - 2, s).wait()

            exchange(0, c + NP, 9, 12)
            exchange(1, c, 6, 10)

            @pl.when(c < 7)
            def _():
                od_pre(c + STEPS, False)

            x = jnp.concatenate([bufs[s][0], bufs[s][1]], axis=1)
            w = jnp.concatenate([wk[:, :W], wv[:, :W], wk[:, W:], wv[:, W:]], axis=1)
            mbuf[s] = dotg(x, w, 1, 1).astype(BF).reshape(2, FP, D)
            dm_copy(c, s).start()

            @pl.when(c < 7)
            def _():
                od_post(c + STEPS, False)

            @pl.when(c == 9)
            def _():
                pltpu.make_async_copy(res.at[0], res.at[0], res_recv).wait()
                pltpu.make_async_copy(res, res_hbm, out_sem.at[2]).start()
        return carry

    lax.fori_loop(0, NP // 2, c_step, 0)
    for t in range(NP, 10 + NCH + 2):
        exchange(1, t, 6, 10)
    for k in range(1, 4):
        b_copy(k, (me + k) % 4).wait_recv()
        b_copy(k, me).wait_send()
    big1[0:8, :] = (bias[0, :, 0:W] + bias[1, :, 0:W]) + (bias[2, :, 0:W] + bias[3, :, 0:W])
    big1[8:16, :] = (bias[0, :, W:] + bias[1, :, W:]) + (bias[2, :, W:] + bias[3, :, W:])
    bias_out = pltpu.make_async_copy(big1.at[0:16], bias_hbm, out_sem.at[3])
    bias_out.start()
    dm_copy(NP - 2, 0).wait()
    dm_copy(NP - 1, 1).wait()
    dw_copy(0).wait()
    dw_copy(1).wait()
    pltpu.make_async_copy(res, res_hbm, out_sem.at[2]).wait()
    bias_out.wait()


def attention(m_pad, q, do, w_k, w_v, b_v):
    vm = pl.BlockSpec(memory_space=VMEM)
    hbm = pl.BlockSpec(memory_space=pl.ANY)
    dma = pltpu.SemaphoreType.DMA
    return pl.pallas_call(
        attn_kernel, name="attention",
        out_shape=(jax.ShapeDtypeStruct((2, NB * T, D), BF), jax.ShapeDtypeStruct((2, D, D), F32),
                   jax.ShapeDtypeStruct((16, W), F32), jax.ShapeDtypeStruct((NB, FP, D), BF),
                   jax.ShapeDtypeStruct((2, NP, ROWS, D), BF)),
        in_specs=[hbm, vm, vm, vm, vm, vm],
        out_specs=(hbm,) * 5,
        scratch_shapes=[
            VMEM((2, 2, FP, D), BF), VMEM((2, ROWS, D), BF), VMEM((2, 4, FP, 128), F32), VMEM((2, 4, FP, 128), F32),
            VMEM((2, D, ROWS), BF), VMEM((4, 4, 16, 128), F32), VMEM((8, 128), F32), VMEM((2, ROWS, D), BF),
            VMEM((2, D, D), F32), VMEM((4, 8, D), F32), VMEM((2, 2, 64, W), F32), VMEM((4, 64, W), F32),
            VMEM((4, T, W), F32), VMEM((4, T, W), F32), VMEM((8, T, W), F32), VMEM((2, NB * T, D), BF),
            VMEM((D, W), F32), VMEM((2, D // 2, W), F32),
            dma((2,)), dma((2,)), dma((2,)), dma((4,)), dma((4, 3)), dma((4, 4)), dma((4,)), dma((4,)), dma((8,)), dma((8,)),
            dma((8,)), dma((8,)), dma((4,)), dma((4,)), dma, dma((2,)), dma((2,)), dma((2, NCH)), dma((2, NCH)),
            dma((2, NCH)), dma((2, NCH)), dma((2, NCH)), dma((2, NCH)), dma((2,)), dma((3,)), dma((4,)),
            pltpu.SemaphoreType.REGULAR((2,)), pltpu.SemaphoreType.REGULAR((2,))],
        compiler_params=pltpu.CompilerParams(vmem_limit_bytes=62 << 20, collective_id=0, has_side_effects=True),
    )(m_pad, q, do, w_k, w_v, b_v)


def solution(mesh):
    act_spec = P("dp", None, None)
    mem_spec = P("dp", "cp", None)
    vec_out = P("dp")
    mat_out = P("dp", None)
    in_specs = (act_spec, mem_spec, P(), P(), P(), P(), P(), P(), P(), P(), P(), act_spec)
    out_specs = (act_spec, act_spec, mem_spec, vec_out, vec_out, mat_out, vec_out, mat_out, mat_out, vec_out, mat_out, vec_out)

    def device_step(hidden, memory, ln_gain, ln_bias, w_q, b_q, w_k, w_v, b_v, w_o, b_o, grad_y):
        h = hidden.reshape(NB * T, D).astype(F32)
        dy = grad_y.reshape(NB * T, D)
        centered = h - jnp.mean(h, axis=-1, keepdims=True)
        inv_std = lax.rsqrt(jnp.mean(centered * centered, axis=-1, keepdims=True) + EPS)
        x_hat = centered * inv_std
        gain = ln_gain.astype(F32)
        x = (x_hat * gain + ln_bias.astype(F32)).astype(BF)
        q = (jnp.dot(x, w_q, preferred_element_type=F32) + b_q.astype(F32)).astype(BF)
        do = dotg(dy, w_o, 1, 1).astype(BF)
        m_pad = split_frames(memory.transpose(1, 0, 2))
        res, dw, bias, dm, _ = attention(m_pad, q, do, w_k, w_v, b_v.astype(F32).reshape(1, D))
        grad_mem = join_frames(dm).transpose(1, 0, 2)
        o, dq = res[0], res[1]
        out_y = (h + jnp.dot(o, w_o, preferred_element_type=F32) + b_o.astype(F32)).astype(BF)
        grad_wo = dotg(o, dy, 0, 0)
        grad_bo = jnp.sum(dy, axis=0, dtype=F32)
        grad_wk = jnp.concatenate([dw[0, :, :W], dw[1, :, :W]], axis=1)
        grad_wv = jnp.concatenate([dw[0, :, W:], dw[1, :, W:]], axis=1)
        grad_bq = jnp.concatenate([bias[0], bias[1]])
        grad_bv = jnp.concatenate([bias[8], bias[9]])
        grad_wq = dotg(x, dq, 0, 0)
        d_x = dotg(dq, w_q, 1, 1)
        grad_gain = jnp.sum(d_x * x_hat, axis=0)
        grad_bias = jnp.sum(d_x, axis=0)
        d_hat = d_x * gain
        d_h = inv_std * (d_hat - jnp.mean(d_hat, axis=-1, keepdims=True) - x_hat * jnp.mean(d_hat * x_hat, axis=-1, keepdims=True))
        grad_h = (dy.astype(F32) + d_h).astype(BF)
        return (out_y.reshape(NB, T, D), grad_h.reshape(NB, T, D), grad_mem, grad_gain, grad_bias, grad_wq, grad_bq,
                grad_wk, grad_wv, grad_bv, grad_wo, grad_bo)

    return jax.shard_map(device_step, mesh=mesh, in_specs=in_specs, out_specs=out_specs, check_vma=False)
```

```python
import functools
import math
import jax
import jax.numpy as jnp
from jax import lax
from jax.experimental import pallas as pl
from jax.experimental.pallas import tpu as pltpu
from jax.sharding import PartitionSpec as P

EPS = 1e-5
HEAD = 64
F, FP, D, T = 375, 384, 1024, 32
NB = 32
NP = NB // 2
STEPS = 2 * NP
W = 512
ROWS = 2 * FP
BF, F32 = jnp.bfloat16, jnp.float32
LOG2 = 0.125 * math.log2(math.e)
MESH = pl.DeviceIdType.MESH
VMEM = pltpu.VMEM
B2, B4, B8, LANES = 2, 4, 8, 128
TOK = NB * T
SDS = jax.ShapeDtypeStruct


def dotg(a, b, ca, cb):
    return lax.dot_general(a, b, (((ca,), (cb,)), ((), ())), preferred_element_type=F32)


FC = 64
NFC = FP // FC


def fixed(rows):
    return pl.BlockSpec((rows, D), lambda s: (0, 0), pipeline_mode=pl.Buffered(1))


def lanes(t):
    return slice(LANES * t, LANES * (t + 1))


def norm_parts(h):
    centered = h - jnp.mean(h, axis=-1, keepdims=True)
    inv_std = lax.rsqrt(jnp.mean(centered * centered, axis=-1, keepdims=True) + EPS)
    return centered * inv_std, inv_std


def prep_kernel(m_ref, h_ref, dy_ref, gain, shift, wq, bq, wo, mp_ref, q_ref, do_ref, s_ref):
    step = pl.program_id(0)

    @pl.when(step < TOK // LANES)
    def _():
        x_hat, _ = norm_parts(h_ref[...].astype(F32))
        x = (x_hat * gain[...] + shift[...]).astype(BF)
        q_ref[...] = (jnp.dot(x, wq[...], preferred_element_type=F32) + bq[...]).astype(BF)
        do_ref[...] = dotg(dy_ref[...], wo[...], 1, 1).astype(BF)

    x = m_ref[...].astype(F32).reshape(B8 * FC, D)
    for t in range(D // LANES):
        s_ref[t] = x[:, lanes(t)]
    real = lax.broadcasted_iota(jnp.int32, (FC, LANES), 0) + FC * (step % NFC) < F
    for b in range(B8):
        for t in range(D // LANES):
            y = jnp.where(real, s_ref[t, pl.ds(b, FC, stride=B8), :], 0.0)
            mp_ref[b, :, lanes(t)] = y.astype(BF)


def prepare(mt, h, dy, gain, shift, w_q, b_q, w_o):
    tok = pl.BlockSpec((LANES, D), lambda s: (jnp.minimum(s, TOK // LANES - 1), 0))
    vec, mat = fixed(1), fixed(D)
    return pl.pallas_call(
        prep_kernel, grid=(NB // B8 * NFC,), name="prepare",
        out_shape=(SDS((NB, FP, D), BF), SDS((TOK, D), BF), SDS((TOK, D), BF)),
        in_specs=[pl.BlockSpec((FC, B8, D), lambda s: (s % NFC, s // NFC, 0)), tok, tok, vec, vec, mat, vec, mat],
        out_specs=(pl.BlockSpec((B8, FC, D), lambda s: (s // NFC, s % NFC, 0)), tok, tok),
        scratch_shapes=[VMEM((D // LANES, B8 * FC, LANES), F32)],
        compiler_params=pltpu.CompilerParams(vmem_limit_bytes=40 << 20),
    )(mt, h, dy, gain, shift, w_q, b_q, w_o)


JOB0, JOBS, RC = 3, 4, 256


def finish_kernel(dm_ref, res_hbm, h_hbm, dy_hbm, wo_hbm, wq_hbm, dw_hbm, gain, shift, bo,
                  gm_ref, y_hbm, gh_hbm, gwo_hbm, gwq_hbm, gwk_hbm, gwv_hbm, vec_ref,
                  s_ref, res, h, dy, wo, wq, x, y, gh, gw, stage, in_sem, y_sem, gh_sem, gw_sem, ld_sem, st_sem):
    step = pl.program_id(0)
    loads = [pltpu.make_async_copy(a, b, in_sem.at[k]) for k, (a, b) in enumerate(
        ((h_hbm, h), (res_hbm, res), (wo_hbm, wo), (dy_hbm, dy), (wq_hbm, wq)))]

    def rows(n):
        return pl.ds(pl.multiple_of(RC * n, RC), RC)

    def out_copy(src, dst, sem, n):
        return pltpu.make_async_copy(src.at[rows(n)], dst.at[rows(n)], sem.at[n])

    def gw_copy(dst, n):
        return pltpu.make_async_copy(gw.at[n], dst.at[rows(n)], gw_sem.at[n])

    def piece_in(k):
        g, v = k // 2, k % 2
        return pltpu.make_async_copy(dw_hbm.at[g, :, pl.ds(W * v, W)], stage.at[k % 2], ld_sem.at[k % 2])

    def piece_out(k):
        g, v = k // 2, k % 2
        return pltpu.make_async_copy(stage.at[k % 2], (gwk_hbm, gwv_hbm)[v].at[:, pl.ds(W * g, W)], st_sem.at[k % 2])

    @pl.when(step == 0)
    def _():
        for cp in loads:
            cp.start()
        piece_in(0).start()
        piece_in(1).start()
        vec_ref[...] = jnp.zeros_like(vec_ref)

    for k in range(4):
        @pl.when(step == 4 + 5 * (k // 2) + k % 2)
        def _():
            piece_in(k).wait()
            piece_out(k).start()

        @pl.when(step == 7 + 5 * (k // 2) + k % 2)
        def _():
            if k < 2:
                piece_out(k).wait()
                piece_in(k + 2).start()

    @pl.when(step == JOB0)
    def _():
        for cp in loads:
            cp.wait()

    job = step - JOB0
    n = job % JOBS

    @pl.when((job >= 0) & (job < JOBS))
    def _():
        hf = h[rows(n)].astype(F32)
        x_hat, _ = norm_parts(hf)
        x[rows(n)] = (x_hat * gain[...] + shift[...]).astype(BF)
        y[rows(n)] = (hf + jnp.dot(res[0, rows(n)], wo[...], preferred_element_type=F32) + bo[...]).astype(BF)
        out_copy(y, y_hbm, y_sem, n).start()

    @pl.when((job >= JOBS) & (job < 2 * JOBS))
    def _():
        gw[n] = dotg(res[0, :, rows(n)], dy[...], 0, 0)
        gw_copy(gwo_hbm, n).start()

    @pl.when((job >= 2 * JOBS) & (job < 3 * JOBS))
    def _():
        x_hat, inv_std = norm_parts(h[rows(n)].astype(F32))
        dyf = dy[rows(n)].astype(F32)
        d_x = dotg(res[1, rows(n)], wq[...], 1, 1)
        vec_ref[0:1] += jnp.sum(d_x * x_hat, axis=0, keepdims=True)
        vec_ref[1:2] += jnp.sum(d_x, axis=0, keepdims=True)
        vec_ref[2:3] += jnp.sum(dyf, axis=0, keepdims=True)
        d_hat = d_x * gain[...]
        d_h = inv_std * (d_hat - jnp.mean(d_hat, axis=-1, keepdims=True) - x_hat * jnp.mean(d_hat * x_hat, axis=-1, keepdims=True))
        gh[rows(n)] = (dyf + d_h).astype(BF)
        out_copy(gh, gh_hbm, gh_sem, n).start()

    @pl.when((job >= 3 * JOBS) & (job < 4 * JOBS))
    def _():
        gw_copy(gwo_hbm, n).wait()
        gw[n] = dotg(x[:, rows(n)], res[1], 0, 0)
        gw_copy(gwq_hbm, n).start()

    for b in range(B8):
        z = dm_ref[b].astype(F32)
        for t in range(D // LANES):
            s_ref[t, pl.ds(b, FC, stride=B8), :] = z[:, lanes(t)]
    z = jnp.concatenate([s_ref[t] for t in range(D // LANES)], axis=1)
    gm_ref[...] = z.reshape(FC, B8, D).astype(BF)

    @pl.when(step == pl.num_programs(0) - 1)
    def _():
        for k in range(JOBS):
            out_copy(y, y_hbm, y_sem, k).wait()
            out_copy(gh, gh_hbm, gh_sem, k).wait()
            gw_copy(gwq_hbm, k).wait()
        for k in (2, 3):
            piece_out(k).wait()


def finish(dm, res, h, dy, w_o, w_q, dw, gain, shift, b_o):
    hbm = pl.BlockSpec(memory_space=pl.ANY)
    vec = fixed(1)
    dma = pltpu.SemaphoreType.DMA
    mat, dj = VMEM((D, D), BF), dma((JOBS,))
    return pl.pallas_call(
        finish_kernel, grid=(NB // B8 * NFC,), name="finish",
        out_shape=(SDS((F, NB, D), BF), SDS((TOK, D), BF), SDS((TOK, D), BF), SDS((D, D), F32), SDS((D, D), F32),
                   SDS((D, D), F32), SDS((D, D), F32), SDS((B8, D), F32)),
        in_specs=[pl.BlockSpec((B8, FC, D), lambda s: (s // NFC, s % NFC, 0))] + [hbm] * 6 + [vec] * 3,
        out_specs=(pl.BlockSpec((FC, B8, D), lambda s: (s % NFC, s // NFC, 0)),) + (hbm,) * 6 + (pl.BlockSpec((B8, D), lambda s: (0, 0)),),
        scratch_shapes=[
            VMEM((D // LANES, B8 * FC, LANES), F32), VMEM((B2, TOK, D), BF), mat, mat, mat, mat, mat, mat, mat, VMEM((JOBS, RC, D), F32),
            VMEM((B2, D, W), F32), dma((B8,)), dj, dj, dj, dma((B2,)), dma((B2,))],
        compiler_params=pltpu.CompilerParams(vmem_limit_bytes=50 << 20),
    )(dm, res, h, dy, w_o, w_q, dw, gain, shift, b_o)


def block_mask():
    return lax.broadcasted_iota(jnp.int32, (128, 256), 0) // T == lax.broadcasted_iota(jnp.int32, (128, 256), 1) // HEAD


def block_diag(x, mask):
    return jnp.where(mask, jnp.concatenate([x] * 4, axis=0), jnp.zeros((), BF))


def when(cond):
    if isinstance(cond, bool):
        return (lambda f: f()) if cond else (lambda f: None)
    return pl.when(cond)


CH = 64
NCH = D // 2 // CH


def attn_kernel(m_hbm, q, do, wk, wv, bv, res_hbm, dw_hbm, bias_hbm, dm_hbm, dkv_hbm,
                mbuf, kv, e_s, dp_s, mt, stats, coef, dkv, acc, bias, od, r1, keep, x2, r2, res, big1, big2,
                m_sem, dkv_sem, dm_sem, out_sem, st_send, st_recv, s1_send, s1_recv, s2_send, s2_recv,
                s3_send, s3_recv, s3s_send, s4_send, res_recv, e1_send, e1_recv, e2_send, e2_recv,
                e3_send, e3_recv, e3s_send, e4_send, acc_recv, b_send, b_recv, free_sib, free_xn):
    me = lax.axis_index("cp")
    cx, cc = me // 2, me % 2
    sib, xn = 2 * cx + 1 - cc, 2 * (1 - cx) + cc

    def remote(src, dst, ss, rs, dev):
        return pltpu.make_async_remote_copy(src_ref=src, dst_ref=dst, send_sem=ss, recv_sem=rs,
                                            device_id={"cp": dev}, device_id_type=MESH)

    def m_copy(i):
        return pltpu.make_async_copy(m_hbm.at[pl.ds(2 * (i % NP), 2)], mbuf.at[i % 2], m_sem.at[i % 2])

    def dkv_copy(i):
        return pltpu.make_async_copy(dkv.at[i % 2], dkv_hbm.at[i // NP, i % NP], dkv_sem.at[i % 2])

    def stat_copy(i, src, k):
        return remote(stats.at[i % 4, src], stats.at[i % 4, src], st_send.at[i % 4, k - 1], st_recv.at[i % 4, src], (me + k) % 4)

    def s1(b):
        return remote(od.at[b % 2, 1 - cc], r1.at[b % 4], s1_send.at[b % 4], s1_recv.at[b % 4], sib)

    def s2(b):
        return remote(x2.at[b % 4], r2.at[b % 8], s2_send.at[b % 8], s2_recv.at[b % 8], xn)

    def res_at(b, x):
        return res.at[cc, pl.ds(pl.multiple_of(64 * (b % NP) + T * x, T), T), pl.ds(pl.multiple_of(W * (b // NP), W), W)]

    def s3(b, x):
        return remote(res_at(b, x), res_at(b, x), s3_send.at[b % 8], s3_recv.at[b % 8], xn)

    def s3s(b):
        return remote(res_at(b, cx), res_at(b, cx), s3s_send.at[b % 4], res_recv, sib)

    def s4(b):
        return remote(res_at(b, 1 - cx), res_at(b, 1 - cx), s4_send.at[b % 4], res_recv, sib)

    def od_pre(b, inside):
        def on(k):
            return (b >= k) if inside else (b - k < STEPS)

        @when(on(7))
        def _():
            s4(b - 7).wait_send()

        @when(on(5))
        def _():
            s3(b - 5, 1 - cx).wait_recv()
            s4(b - 5).start()
            s3(b - 5, cx).wait_send()
            s3s(b - 5).wait_send()

        @when(on(3))
        def _():
            s2(b - 3).wait_recv()
            s2(b - 3).wait_send()
            res_at(b - 3, cx)[...] = (keep[(b - 3) % 4] + r2[(b - 3) % 8]).astype(BF)

        @when(on(2))
        def _():
            s1(b - 2).wait_send()

        @when(on(1))
        def _():
            s1(b - 1).wait_recv()
            for ref, x in ((keep, cx), (x2, 1 - cx)):
                rows = pl.ds(pl.multiple_of(T * x, T), T)
                ref[(b - 1) % 4] = od[(b - 1) % 2, cc, rows, :] + r1[(b - 1) % 4, rows, :]

    def od_post(b, inside):
        def on(k):
            return (b >= k) if inside else (b - k < STEPS)

        if inside:
            s1(b).start()

        @when(on(1))
        def _():
            s2(b - 1).start()

        @when(on(3))
        def _():
            s3(b - 3, cx).start()
            s3s(b - 3).start()

    own = pl.ds(pl.multiple_of(W * cc, W), W)
    other = pl.ds(pl.multiple_of(W * (1 - cc), W), W)

    def rows_of(x, n):
        return pl.ds(pl.multiple_of(x * (D // 2) + CH * n, CH), CH)

    def e1(g):
        return remote(acc.at[g, :, other], big1, e1_send.at[g], e1_recv.at[g], sib)

    def e2(g, n):
        return remote(acc.at[g, rows_of(1 - cx, n), own], big2.at[g, pl.ds(pl.multiple_of(CH * n, CH), CH)],
                      e2_send.at[g, n], e2_recv.at[g, n], xn)

    def e3(g, n, x):
        ref = acc.at[g, rows_of(x, n), own]
        return remote(ref, ref, e3_send.at[g, n], e3_recv.at[g, n], xn)

    def to_sib(g, n, x, sem):
        ref = acc.at[g, rows_of(x, n), own]
        return remote(ref, ref, sem.at[g, n], acc_recv.at[g], sib)

    def dw_copy(g):
        return pltpu.make_async_copy(acc.at[g], dw_hbm.at[g], out_sem.at[g])

    def exchange(g, t, t3, t4):
        @when(t == 0)
        def _():
            e1(g).start()

        @when(t == 1)
        def _():
            e1(g).wait_send()
            pl.semaphore_signal(free_sib.at[g], inc=1, device_id={"cp": sib}, device_id_type=MESH)
            e1(g).wait_recv()

        @when(t == t3)
        def _():
            pl.semaphore_wait(free_sib.at[g], 1)

        def chunk(t0, f):
            n = t - t0
            if isinstance(n, int):
                if 0 <= n < NCH:
                    f(n)
            else:
                pl.when((n >= 0) & (n < NCH))(lambda: f(n))

        def reduce_core(n):
            for x in (cx, 1 - cx):
                acc[g, rows_of(x, n), own] += big1[rows_of(x, n), :]
            e2(g, n).start()

        def sent(n):
            e2(g, n).wait_send()
            pl.semaphore_signal(free_xn.at[g], inc=1, device_id={"cp": xn}, device_id_type=MESH)

        def reduce_chip(n):
            e2(g, n).wait_recv()
            pl.semaphore_wait(free_xn.at[g], 1)
            acc[g, rows_of(cx, n), own] += big2[g, pl.ds(pl.multiple_of(CH * n, CH), CH), :]
            e3(g, n, cx).start()
            to_sib(g, n, cx, e3s_send).start()

        def forward(n):
            e3(g, n, 1 - cx).wait_recv()
            to_sib(g, n, 1 - cx, e4_send).start()

        chunk(1, reduce_core)
        chunk(t3 - 1, sent)
        chunk(t3, reduce_chip)
        chunk(t4, forward)

        @when(t == t4 + NCH + 1)
        def _():
            remote(acc.at[g, :, other], acc.at[g, :, other], e1_send.at[g], acc_recv.at[g], sib).wait_recv()
            for n in range(NCH):
                e3(g, n, cx).wait_send()
                to_sib(g, n, cx, e3s_send).wait_send()
                to_sib(g, n, 1 - cx, e4_send).wait_send()
            dw_copy(g).start()

    def operands(i, j, h):
        cols = pl.ds(pl.multiple_of(W * (i // NP) + 256 * h, 256), 256)
        rows = pl.ds(pl.multiple_of(64 * (i % NP) + T * j, T), T)
        mask = block_mask()
        return block_diag(q[rows, cols], mask), block_diag(do[rows, cols], mask), mask

    def stage_a(i):
        slot = i % 2
        m = mbuf[slot].reshape(ROWS, D)
        cols = pl.ds(pl.multiple_of(W * (i // NP), W), W)
        kv[slot, :, 0:W] = jnp.dot(m, wk[:, cols], preferred_element_type=F32).astype(BF)
        kv[slot, :, W:] = (jnp.dot(m, wv[:, cols], preferred_element_type=F32) + bv[:, cols]).astype(BF)
        mt[slot] = m.T
        real = lax.broadcasted_iota(jnp.int32, (FP, 128), 0) < F
        for j in range(2):
            rows = slice(FP * j, FP * (j + 1))
            for h in range(2):
                n = 2 * j + h
                qb, db, _ = operands(i, j, h)
                s = dotg(kv[slot, rows, 256 * h:256 * (h + 1)], qb, 1, 1)
                dp = dotg(kv[slot, rows, W + 256 * h:W + 256 * (h + 1)], db, 1, 1)
                s = jnp.where(real, s, -1e30)
                top = jnp.max(s, axis=0, keepdims=True)
                e = jnp.exp2((s - top) * LOG2)
                e_s[slot, n] = e
                dp_s[slot, n] = dp
                stats[i % 4, me, n:n + 1, :] = top
                stats[i % 4, me, 4 + n:5 + n, :] = jnp.sum(e, axis=0, keepdims=True)
                stats[i % 4, me, 8 + n:9 + n, :] = jnp.sum(e * dp, axis=0, keepdims=True)

    def combine(i):
        slot = i % 4
        tops = [stats[slot, d, 0:4, :] for d in range(4)]
        top = jnp.maximum(jnp.maximum(tops[0], tops[1]), jnp.maximum(tops[2], tops[3]))
        ws = [jnp.exp2((t - top) * LOG2) for t in tops]
        total = sum(stats[slot, d, 4:8, :] * ws[d] for d in range(4))
        dots = sum(stats[slot, d, 8:12, :] * ws[d] for d in range(4))
        coef[0:4, :] = jnp.exp2((stats[slot, me, 0:4, :] - top) * LOG2) / total
        coef[4:8, :] = dots / total

    def stage_b(i):
        slot = i % 2
        grp = i // NP
        for j in range(2):
            rows = slice(FP * j, FP * (j + 1))
            for h in range(2):
                n = 2 * j + h
                qb, db, mask = operands(i, j, h)
                ck, cv = slice(256 * h, 256 * (h + 1)), slice(W + 256 * h, W + 256 * (h + 1))
                p = e_s[slot, n] * coef[n:n + 1, :]
                pb = p.astype(BF)
                gb = (p * (dp_s[slot, n] - coef[4 + n:5 + n, :]) * 0.125).astype(BF)
                o = dotg(pb, kv[slot, rows, cv], 0, 0)
                dq = dotg(gb, kv[slot, rows, ck], 0, 0)
                for which, x in ((0, o), (1, dq)):
                    x = jnp.where(mask, x, 0.0)
                    x = (x[0:32] + x[32:64]) + (x[64:96] + x[96:128])
                    od[slot, which, T * j:T * (j + 1), ck] = x
                    if which == 1:
                        bias[me, pl.ds(grp, 1), ck] += jnp.sum(x, axis=0, keepdims=True)
                dk = jnp.dot(gb, qb, preferred_element_type=F32)
                dv = jnp.dot(pb, db, preferred_element_type=F32)
                dkv[slot, rows, ck] = dk.astype(BF)
                dkv[slot, rows, cv] = dv.astype(BF)
                bias[me, pl.ds(grp, 1), cv] += jnp.sum(dv, axis=0, keepdims=True)
        acc[grp] += jnp.dot(mt[slot], dkv[slot], preferred_element_type=F32)

    def part_a(i):
        m_copy(i).wait()

        @pl.when(i + 1 < STEPS)
        def _():
            m_copy(i + 1).start()

        stage_a(i)
        for k in range(1, 4):
            stat_copy(i, me, k).start()

    def part_b(b):
        exchange(0, b - NP, 9, 12)
        for k in range(1, 4):
            stat_copy(b, (me + k) % 4, k).wait_recv()

        @pl.when(b >= 1)
        def _():
            for k in range(1, 4):
                stat_copy(b - 1, me, k).wait_send()

        @pl.when(b >= 2)
        def _():
            dkv_copy(b - 2).wait()

        od_pre(b, True)
        combine(b)
        stage_b(b)
        dkv_copy(b).start()
        od_post(b, True)

    m_copy(0).start()
    for g in range(2):
        acc[g] = jnp.zeros((D, D), F32)
    bias[me] = jnp.zeros((8, D), F32)
    barrier = pltpu.get_barrier_semaphore()
    for k in range(1, 4):
        pl.semaphore_signal(barrier, inc=1, device_id={"cp": (me + k) % 4}, device_id_type=MESH)
    pl.semaphore_wait(barrier, 3)
    part_a(jnp.int32(0))

    def step(i, carry):
        part_a(i)
        part_b(i - 1)
        return carry

    lax.fori_loop(1, STEPS, step, 0)
    part_b(jnp.int32(STEPS - 1))

    def b_copy(k, src):
        return remote(bias.at[src], bias.at[src], b_send.at[k - 1], b_recv.at[src], (me + k) % 4)

    for k in range(1, 4):
        b_copy(k, me).start()
        stat_copy(STEPS - 1, me, k).wait_send()
    dkv_copy(STEPS - 2).wait()
    dkv_copy(STEPS - 1).wait()

    bufs = (kv, dkv)

    def c_load(c, s):
        return [pltpu.make_async_copy(dkv_hbm.at[g, c], bufs[s].at[g], m_sem.at[g] if s == 0 else dkv_sem.at[g]) for g in range(2)]

    def dm_copy(c, s):
        return pltpu.make_async_copy(mbuf.at[s], dm_hbm.at[pl.ds(2 * c, 2)], dm_sem.at[s])

    for cp in c_load(0, 0):
        cp.start()

    def c_step(u, carry):
        for s in range(2):
            c = 2 * u + s
            for cp in c_load(c, s):
                cp.wait()

            @pl.when(c + 1 < NP)
            def _():
                for cp in c_load(c + 1, 1 - s):
                    cp.start()

            @pl.when(c >= 2)
            def _():
                dm_copy(c - 2, s).wait()

            exchange(0, c + NP, 9, 12)
            exchange(1, c, 6, 10)

            @pl.when(c < 7)
            def _():
                od_pre(c + STEPS, False)

            x = jnp.concatenate([bufs[s][0], bufs[s][1]], axis=1)
            w = jnp.concatenate([wk[:, :W], wv[:, :W], wk[:, W:], wv[:, W:]], axis=1)
            mbuf[s] = dotg(x, w, 1, 1).astype(BF).reshape(2, FP, D)
            dm_copy(c, s).start()

            @pl.when(c < 7)
            def _():
                od_post(c + STEPS, False)

            @pl.when(c == 9)
            def _():
                pltpu.make_async_copy(res.at[0], res.at[0], res_recv).wait()
                pltpu.make_async_copy(res, res_hbm, out_sem.at[2]).start()
        return carry

    lax.fori_loop(0, NP // 2, c_step, 0)
    for t in range(NP, 10 + NCH + 2):
        exchange(1, t, 6, 10)
    for k in range(1, 4):
        b_copy(k, (me + k) % 4).wait_recv()
        b_copy(k, me).wait_send()
    big1[0:8, :] = (bias[0, :, 0:W] + bias[1, :, 0:W]) + (bias[2, :, 0:W] + bias[3, :, 0:W])
    big1[8:16, :] = (bias[0, :, W:] + bias[1, :, W:]) + (bias[2, :, W:] + bias[3, :, W:])
    bias_out = pltpu.make_async_copy(big1.at[0:16], bias_hbm, out_sem.at[3])
    bias_out.start()
    dm_copy(NP - 2, 0).wait()
    dm_copy(NP - 1, 1).wait()
    dw_copy(0).wait()
    dw_copy(1).wait()
    pltpu.make_async_copy(res, res_hbm, out_sem.at[2]).wait()
    bias_out.wait()


def attention(m_pad, q, do, w_k, w_v, b_v):
    vm = pl.BlockSpec(memory_space=VMEM)
    hbm = pl.BlockSpec(memory_space=pl.ANY)
    dma = pltpu.SemaphoreType.DMA
    d2, d4, d8, dn = dma((B2,)), dma((B4,)), dma((B8,)), dma((B2, NCH))
    credit = pltpu.SemaphoreType.REGULAR((B2,))
    probs = VMEM((B2, B4, FP, LANES), F32)
    return pl.pallas_call(
        attn_kernel, name="attention",
        out_shape=(SDS((B2, TOK, D), BF), SDS((B2, D, D), F32), SDS((2 * B8, W), F32), SDS((NB, FP, D), BF),
                   SDS((B2, NP, ROWS, D), BF)),
        in_specs=[hbm, vm, vm, vm, vm, vm],
        out_specs=(hbm,) * 5,
        scratch_shapes=[
            VMEM((B2, B2, FP, D), BF), VMEM((B2, ROWS, D), BF), probs, probs, VMEM((B2, D, ROWS), BF),
            VMEM((B4, B4, 2 * B8, LANES), F32), VMEM((B8, LANES), F32), VMEM((B2, ROWS, D), BF),
            VMEM((B2, D, D), F32), VMEM((B4, B8, D), F32), VMEM((B2, B2, 2 * T, W), F32), VMEM((B4, 2 * T, W), F32),
            VMEM((B4, T, W), F32), VMEM((B4, T, W), F32), VMEM((B8, T, W), F32), VMEM((B2, TOK, D), BF),
            VMEM((D, W), F32), VMEM((B2, D // 2, W), F32),
            d2, d2, d2, d4, dma((B4, B4)), dma((B4, B4)), d4, d4, d8, d8, d8, d8, d4, d4, dma, d2, d2, dn, dn, dn, dn, dn, dn, d2, d4, d4,
            credit, credit],
        compiler_params=pltpu.CompilerParams(vmem_limit_bytes=62 << 20, collective_id=0, has_side_effects=True),
    )(m_pad, q, do, w_k, w_v, b_v)


def solution(mesh):
    act_spec = P("dp", None, None)
    mem_spec = P("dp", "cp", None)
    vec_out = P("dp")
    mat_out = P("dp", None)
    in_specs = (act_spec, mem_spec, P(), P(), P(), P(), P(), P(), P(), P(), P(), act_spec)
    out_specs = (act_spec, act_spec, mem_spec, vec_out, vec_out, mat_out, vec_out, mat_out, mat_out, vec_out, mat_out, vec_out)

    def device_step(hidden, memory, ln_gain, ln_bias, w_q, b_q, w_k, w_v, b_v, w_o, b_o, grad_y):
        h = hidden.reshape(TOK, D)
        dy = grad_y.reshape(TOK, D)
        gain, shift, bq, bv, bo = (a.astype(F32).reshape(1, D) for a in (ln_gain, ln_bias, b_q, b_v, b_o))
        m_pad, q, do = prepare(memory.transpose(1, 0, 2), h, dy, gain, shift, w_q, bq, w_o)
        res, dw, bias, dm, _ = attention(m_pad, q, do, w_k, w_v, bv)
        gm, y, gh, gwo, gwq, gwk, gwv, vec = finish(dm, res, h, dy, w_o, w_q, dw, gain, shift, bo)
        grad_bq = bias[0:2].reshape(D)
        grad_bv = bias[8:10].reshape(D)
        return (y.reshape(NB, T, D), gh.reshape(NB, T, D), gm.transpose(1, 0, 2), vec[0], vec[1], gwq, grad_bq,
                gwk, gwv, grad_bv, gwo, vec[2])

    return jax.shard_map(device_step, mesh=mesh, in_specs=in_specs, out_specs=out_specs, check_vma=False)
```

```python
import functools
import math
import jax
import jax.numpy as jnp
from jax import lax
from jax.experimental import pallas as pl
from jax.experimental.pallas import tpu as pltpu
from jax.sharding import PartitionSpec as P

EPS = 1e-5
HEAD = 64
F, FP, D, T = 375, 384, 1024, 32
NB = 32
NP = NB // 2
STEPS = 2 * NP
W = 512
ROWS = 2 * FP
QW = 256
BF, F32 = jnp.bfloat16, jnp.float32
LOG2 = 0.125 * math.log2(math.e)
MESH = pl.DeviceIdType.MESH
VMEM = pltpu.VMEM
B2, B4, B8, LANES = 2, 4, 8, 128
RC = 256
TOK = NB * T
SDS = jax.ShapeDtypeStruct


def dotg(a, b, ca, cb):
    return lax.dot_general(a, b, (((ca,), (cb,)), ((), ())), preferred_element_type=F32)


FC = 64
NFC = FP // FC


def fixed(rows):
    return pl.BlockSpec((rows, D), lambda s: (0, 0), pipeline_mode=pl.Buffered(1))


def lanes(t):
    return slice(LANES * t, LANES * (t + 1))


def norm_parts(h):
    centered = h - jnp.mean(h, axis=-1, keepdims=True)
    inv_std = lax.rsqrt(jnp.mean(centered * centered, axis=-1, keepdims=True) + EPS)
    return centered * inv_std, inv_std


JOB0, JOBS = 3, 4


def finish_kernel(dm_ref, res_hbm, h_hbm, dy_hbm, wo_hbm, wq_hbm, dw_hbm, gain, shift, bo,
                  gm_ref, y_hbm, gh_hbm, gwo_hbm, gwq_hbm, gwk_hbm, gwv_hbm, vec_ref,
                  s_ref, res, h, dy, wo, wq, x, y, gh, gw, stage, in_sem, y_sem, gh_sem, gw_sem, ld_sem, st_sem):
    step = pl.program_id(0)
    loads = [pltpu.make_async_copy(a, b, in_sem.at[k]) for k, (a, b) in enumerate(
        ((h_hbm, h), (res_hbm, res), (wo_hbm, wo), (dy_hbm, dy), (wq_hbm, wq)))]

    def rows(n):
        return pl.ds(pl.multiple_of(RC * n, RC), RC)

    def out_copy(src, dst, sem, n):
        return pltpu.make_async_copy(src.at[rows(n)], dst.at[rows(n)], sem.at[n])

    def gw_copy(dst, n):
        return pltpu.make_async_copy(gw.at[n], dst.at[rows(n)], gw_sem.at[n])

    def piece_in(k):
        g, v = k // 2, k % 2
        return pltpu.make_async_copy(dw_hbm.at[g, :, pl.ds(W * v, W)], stage.at[k % 2], ld_sem.at[k % 2])

    def piece_out(k):
        g, v = k // 2, k % 2
        return pltpu.make_async_copy(stage.at[k % 2], (gwk_hbm, gwv_hbm)[v].at[:, pl.ds(W * g, W)], st_sem.at[k % 2])

    @pl.when(step == 0)
    def _():
        for cp in loads:
            cp.start()
        piece_in(0).start()
        piece_in(1).start()
        vec_ref[...] = jnp.zeros_like(vec_ref)

    for k in range(4):
        @pl.when(step == 4 + 5 * (k // 2) + k % 2)
        def _():
            piece_in(k).wait()
            piece_out(k).start()

        @pl.when(step == 7 + 5 * (k // 2) + k % 2)
        def _():
            if k < 2:
                piece_out(k).wait()
                piece_in(k + 2).start()

    @pl.when(step == JOB0)
    def _():
        for cp in loads:
            cp.wait()

    job = step - JOB0
    n = job % JOBS

    @pl.when((job >= 0) & (job < JOBS))
    def _():
        hf = h[rows(n)].astype(F32)
        x_hat, _ = norm_parts(hf)
        x[rows(n)] = (x_hat * gain[...] + shift[...]).astype(BF)
        y[rows(n)] = (hf + jnp.dot(res[0, rows(n)], wo[...], preferred_element_type=F32) + bo[...]).astype(BF)
        out_copy(y, y_hbm, y_sem, n).start()

    @pl.when((job >= JOBS) & (job < 2 * JOBS))
    def _():
        gw[n] = dotg(res[0, :, rows(n)], dy[...], 0, 0)
        gw_copy(gwo_hbm, n).start()

    @pl.when((job >= 2 * JOBS) & (job < 3 * JOBS))
    def _():
        x_hat, inv_std = norm_parts(h[rows(n)].astype(F32))
        dyf = dy[rows(n)].astype(F32)
        d_x = dotg(res[1, rows(n)], wq[...], 1, 1)
        vec_ref[0:1] += jnp.sum(d_x * x_hat, axis=0, keepdims=True)
        vec_ref[1:2] += jnp.sum(d_x, axis=0, keepdims=True)
        vec_ref[2:3] += jnp.sum(dyf, axis=0, keepdims=True)
        d_hat = d_x * gain[...]
        d_h = inv_std * (d_hat - jnp.mean(d_hat, axis=-1, keepdims=True) - x_hat * jnp.mean(d_hat * x_hat, axis=-1, keepdims=True))
        gh[rows(n)] = (dyf + d_h).astype(BF)
        out_copy(gh, gh_hbm, gh_sem, n).start()

    @pl.when((job >= 3 * JOBS) & (job < 4 * JOBS))
    def _():
        gw_copy(gwo_hbm, n).wait()
        gw[n] = dotg(x[:, rows(n)], res[1], 0, 0)
        gw_copy(gwq_hbm, n).start()

    for b in range(B8):
        z = dm_ref[b].astype(F32)
        for t in range(D // LANES):
            s_ref[t, pl.ds(b, FC, stride=B8), :] = z[:, lanes(t)]
    z = jnp.concatenate([s_ref[t] for t in range(D // LANES)], axis=1)
    gm_ref[...] = z.reshape(FC, B8, D).astype(BF)

    @pl.when(step == pl.num_programs(0) - 1)
    def _():
        for k in range(JOBS):
            out_copy(y, y_hbm, y_sem, k).wait()
            out_copy(gh, gh_hbm, gh_sem, k).wait()
            gw_copy(gwq_hbm, k).wait()
        for k in (2, 3):
            piece_out(k).wait()


def finish(dm, res, h, dy, w_o, w_q, dw, gain, shift, b_o):
    hbm = pl.BlockSpec(memory_space=pl.ANY)
    vec = fixed(1)
    dma = pltpu.SemaphoreType.DMA
    mat, dj = VMEM((D, D), BF), dma((JOBS,))
    return pl.pallas_call(
        finish_kernel, grid=(NB // B8 * NFC,), name="finish",
        out_shape=(SDS((F, NB, D), BF), SDS((TOK, D), BF), SDS((TOK, D), BF), SDS((D, D), F32), SDS((D, D), F32),
                   SDS((D, D), F32), SDS((D, D), F32), SDS((B8, D), F32)),
        in_specs=[pl.BlockSpec((B8, FC, D), lambda s: (s // NFC, s % NFC, 0))] + [hbm] * 6 + [vec] * 3,
        out_specs=(pl.BlockSpec((FC, B8, D), lambda s: (s % NFC, s // NFC, 0)),) + (hbm,) * 6 + (pl.BlockSpec((B8, D), lambda s: (0, 0)),),
        scratch_shapes=[
            VMEM((D // LANES, B8 * FC, LANES), F32), VMEM((B2, TOK, D), BF), mat, mat, mat, mat, mat, mat, mat, VMEM((JOBS, RC, D), F32),
            VMEM((B2, D, W), F32), dma((B8,)), dj, dj, dj, dma((B2,)), dma((B2,))],
        compiler_params=pltpu.CompilerParams(vmem_limit_bytes=50 << 20),
    )(dm, res, h, dy, w_o, w_q, dw, gain, shift, b_o)


def block_mask():
    return lax.broadcasted_iota(jnp.int32, (128, 256), 0) // T == lax.broadcasted_iota(jnp.int32, (128, 256), 1) // HEAD


def block_diag(x, mask):
    return jnp.where(mask, jnp.concatenate([x] * 4, axis=0), jnp.zeros((), BF))


def when(cond):
    if isinstance(cond, bool):
        return (lambda f: f()) if cond else (lambda f: None)
    return pl.when(cond)


CH = 64
NCH = D // 2 // CH


def attn_kernel(m_hbm, h_hbm, dy_hbm, wq_hbm, wo_hbm, wk_hbm, wv_hbm, gain, shift, bq, bv,
                res_hbm, dw_hbm, bias_hbm, dm_hbm, dkv_hbm,
                raw, fine, frames, q, do, wk, wv, kv, e_s, dp_s, mt, stats, coef, dkv, acc, bias, od, r1, keep, x2, r2, res, big1, big2,
                raw_sem, in_sem, dkv_sem, dm_sem, out_sem, st_send, st_recv, s1_send, s1_recv, s2_send, s2_recv,
                s3_send, s3_recv, s3s_send, s4_send, res_recv, e1_send, e1_recv, e2_send, e2_recv,
                e3_send, e3_recv, e3s_send, e4_send, acc_recv, b_send, b_recv, free_sib, free_xn):
    me = lax.axis_index("cp")
    cx, cc = me // 2, me % 2
    sib, xn = 2 * cx + 1 - cc, 2 * (1 - cx) + cc

    def remote(src, dst, ss, rs, dev):
        return pltpu.make_async_remote_copy(src_ref=src, dst_ref=dst, send_sem=ss, recv_sem=rs,
                                            device_id={"cp": dev}, device_id_type=MESH)

    def raw_copy(c):
        seqs = pl.ds(pl.multiple_of(B8 * (c // B4 % B4), B8), B8)
        return pltpu.make_async_copy(m_hbm.at[:, seqs, quarter(c)], raw.at[c % 2], raw_sem.at[c % 2])

    def quarter(c):
        return pl.ds(pl.multiple_of(c % B4 * QW, QW), QW)

    def sort_frames(c):
        x = raw[c % 2].astype(F32)
        for f in range(F):
            for t in range(QW // LANES):
                fine[t, 9 * f:9 * f + B8] = x[f, :, lanes(t)]
        for b in range(B8):
            y = jnp.concatenate([fine[t, pl.ds(b, FP, stride=9), :] for t in range(QW // LANES)], axis=1)
            frames[c // B4 % 2, FP * b:FP * (b + 1), quarter(c)] = y.astype(BF)

    def dkv_copy(i):
        return pltpu.make_async_copy(dkv.at[i % 2], dkv_hbm.at[i // NP, i % NP], dkv_sem.at[i % 2])

    def stat_send(i):
        for k in range(1, B4):
            remote(stats.at[i % B4, me], stats.at[i % B4, me], st_send.at[i % B4], st_recv.at[i % B4], (me + k) % B4).start()

    def stat_wait(i):
        three = stats.at[i % B4, 0:3]
        for sem in (st_recv, st_send):
            pltpu.make_async_copy(three, three, sem.at[i % B4]).wait()

    def s1(b):
        return remote(od.at[b % 2, 1 - cc], r1.at[b % 4], s1_send.at[b % 4], s1_recv.at[b % 4], sib)

    def s2(b):
        return remote(x2.at[b % 4], r2.at[b % 8], s2_send.at[b % 8], s2_recv.at[b % 8], xn)

    def res_at(b, x):
        return res.at[cc, pl.ds(pl.multiple_of(64 * (b % NP) + T * x, T), T), pl.ds(pl.multiple_of(W * (b // NP), W), W)]

    def s3(b, x):
        return remote(res_at(b, x), res_at(b, x), s3_send.at[b % 8], s3_recv.at[b % 8], xn)

    def s3s(b):
        return remote(res_at(b, cx), res_at(b, cx), s3s_send.at[b % 4], res_recv, sib)

    def s4(b):
        return remote(res_at(b, 1 - cx), res_at(b, 1 - cx), s4_send.at[b % 4], res_recv, sib)

    def od_pre(b, inside):
        def on(k):
            return (b >= k) if inside else (b - k < STEPS)

        @when(on(7))
        def _():
            s4(b - 7).wait_send()

        @when(on(5))
        def _():
            s3(b - 5, 1 - cx).wait_recv()
            s4(b - 5).start()
            s3(b - 5, cx).wait_send()
            s3s(b - 5).wait_send()

        @when(on(3))
        def _():
            s2(b - 3).wait_recv()
            s2(b - 3).wait_send()
            res_at(b - 3, cx)[...] = (keep[(b - 3) % 4] + r2[(b - 3) % 8]).astype(BF)

        @when(on(2))
        def _():
            s1(b - 2).wait_send()

        @when(on(1))
        def _():
            s1(b - 1).wait_recv()
            for ref, x in ((keep, cx), (x2, 1 - cx)):
                rows = pl.ds(pl.multiple_of(T * x, T), T)
                ref[(b - 1) % 4] = od[(b - 1) % 2, cc, rows, :] + r1[(b - 1) % 4, rows, :]

    def od_post(b, inside):
        def on(k):
            return (b >= k) if inside else (b - k < STEPS)

        if inside:
            s1(b).start()

        @when(on(1))
        def _():
            s2(b - 1).start()

        @when(on(3))
        def _():
            s3(b - 3, cx).start()
            s3s(b - 3).start()

    own = pl.ds(pl.multiple_of(W * cc, W), W)
    other = pl.ds(pl.multiple_of(W * (1 - cc), W), W)

    def rows_of(x, n):
        return pl.ds(pl.multiple_of(x * (D // 2) + CH * n, CH), CH)

    def e1(g):
        return remote(acc.at[g, :, other], big1, e1_send.at[g], e1_recv.at[g], sib)

    def e2(g, n):
        return remote(acc.at[g, rows_of(1 - cx, n), own], big2.at[g, pl.ds(pl.multiple_of(CH * n, CH), CH)],
                      e2_send.at[g, n], e2_recv.at[g, n], xn)

    def e3(g, n, x):
        ref = acc.at[g, rows_of(x, n), own]
        return remote(ref, ref, e3_send.at[g, n], e3_recv.at[g, n], xn)

    def to_sib(g, n, x, sem):
        ref = acc.at[g, rows_of(x, n), own]
        return remote(ref, ref, sem.at[g, n], acc_recv.at[g], sib)

    def dw_copy(g):
        return pltpu.make_async_copy(acc.at[g], dw_hbm.at[g], out_sem.at[g])

    def exchange(g, t, t3, t4):
        @when(t == 0)
        def _():
            e1(g).start()

        @when(t == 1)
        def _():
            e1(g).wait_send()
            pl.semaphore_signal(free_sib.at[g], inc=1, device_id={"cp": sib}, device_id_type=MESH)
            e1(g).wait_recv()

        @when(t == t3)
        def _():
            pl.semaphore_wait(free_sib.at[g], 1)

        def chunk(t0, f):
            n = t - t0
            if isinstance(n, int):
                if 0 <= n < NCH:
                    f(n)
            else:
                pl.when((n >= 0) & (n < NCH))(lambda: f(n))

        def reduce_core(n):
            for x in (cx, 1 - cx):
                acc[g, rows_of(x, n), own] += big1[rows_of(x, n), :]
            e2(g, n).start()

        def sent(n):
            e2(g, n).wait_send()
            pl.semaphore_signal(free_xn.at[g], inc=1, device_id={"cp": xn}, device_id_type=MESH)

        def reduce_chip(n):
            e2(g, n).wait_recv()
            pl.semaphore_wait(free_xn.at[g], 1)
            acc[g, rows_of(cx, n), own] += big2[g, pl.ds(pl.multiple_of(CH * n, CH), CH), :]
            e3(g, n, cx).start()
            to_sib(g, n, cx, e3s_send).start()

        def forward(n):
            e3(g, n, 1 - cx).wait_recv()
            to_sib(g, n, 1 - cx, e4_send).start()

        chunk(1, reduce_core)
        chunk(t3 - 1, sent)
        chunk(t3, reduce_chip)
        chunk(t4, forward)

        @when(t == t4 + NCH + 1)
        def _():
            remote(acc.at[g, :, other], acc.at[g, :, other], e1_send.at[g], acc_recv.at[g], sib).wait_recv()
            for n in range(NCH):
                e3(g, n, cx).wait_send()
                to_sib(g, n, cx, e3s_send).wait_send()
                to_sib(g, n, 1 - cx, e4_send).wait_send()
            dw_copy(g).start()

    def operands(i, j, h):
        cols = pl.ds(pl.multiple_of(W * (i // NP) + 256 * h, 256), 256)
        rows = pl.ds(pl.multiple_of(64 * (i % NP) + T * j, T), T)
        mask = block_mask()
        return block_diag(q[rows, cols], mask), block_diag(do[rows, cols], mask), mask

    def stage_a(i):
        slot = i % 2
        m = frames[i // B4 % 2, pl.ds(pl.multiple_of(i % B4 * ROWS, ROWS), ROWS), :]
        cols = pl.ds(pl.multiple_of(W * (i // NP), W), W)
        mt[i % 3] = m.T
        kv[slot, :, 0:W] = jnp.dot(m, wk[:, cols], preferred_element_type=F32).astype(BF)
        kv[slot, :, W:] = (jnp.dot(m, wv[:, cols], preferred_element_type=F32) + bv[:, cols]).astype(BF)
        real = lax.broadcasted_iota(jnp.int32, (FP, LANES), 0) < F
        for j in range(2):
            rows = slice(FP * j, FP * (j + 1))
            for h in range(2):
                n = 2 * j + h
                qb, db, _ = operands(i, j, h)
                s = dotg(kv[slot, rows, QW * h:QW * (h + 1)], qb, 1, 1)
                dp = dotg(kv[slot, rows, W + QW * h:W + QW * (h + 1)], db, 1, 1)
                s = jnp.where(real, s, -1e30)
                top = jnp.max(s, axis=0, keepdims=True)
                e = jnp.exp2((s - top) * LOG2)
                e_s[slot, n] = e
                dp_s[slot, n] = dp
                for k, row in enumerate((top, jnp.sum(e, axis=0, keepdims=True), jnp.sum(e * dp, axis=0, keepdims=True))):
                    stats[i % B4, me, B4 * k + n:B4 * k + n + 1, :] = row

    def combine(i):
        slot = i % 4
        tops = [stats[slot, d, 0:4, :] for d in range(4)]
        top = jnp.maximum(jnp.maximum(tops[0], tops[1]), jnp.maximum(tops[2], tops[3]))
        ws = [jnp.exp2((t - top) * LOG2) for t in tops]
        total = sum(stats[slot, d, 4:8, :] * ws[d] for d in range(4))
        dots = sum(stats[slot, d, 8:12, :] * ws[d] for d in range(4))
        coef[0:4, :] = jnp.exp2((stats[slot, me, 0:4, :] - top) * LOG2) / total
        coef[4:8, :] = dots / total

    def stage_b(i):
        slot = i % 2
        grp = i // NP
        for j in range(2):
            rows = slice(FP * j, FP * (j + 1))
            for h in range(2):
                n = 2 * j + h
                qb, db, mask = operands(i, j, h)
                ck, cv = slice(256 * h, 256 * (h + 1)), slice(W + 256 * h, W + 256 * (h + 1))
                p = e_s[slot, n] * coef[n:n + 1, :]
                pb = p.astype(BF)
                gb = (p * (dp_s[slot, n] - coef[4 + n:5 + n, :]) * 0.125).astype(BF)
                o = dotg(pb, kv[slot, rows, cv], 0, 0)
                dq = dotg(gb, kv[slot, rows, ck], 0, 0)
                for which, x in ((0, o), (1, dq)):
                    x = jnp.where(mask, x, 0.0)
                    x = (x[0:32] + x[32:64]) + (x[64:96] + x[96:128])
                    od[slot, which, T * j:T * (j + 1), ck] = x
                    if which == 1:
                        bias[me, pl.ds(grp, 1), ck] += jnp.sum(x, axis=0, keepdims=True)
                dk = jnp.dot(gb, qb, preferred_element_type=F32)
                dv = jnp.dot(pb, db, preferred_element_type=F32)
                dkv[slot, rows, ck] = dk.astype(BF)
                dkv[slot, rows, cv] = dv.astype(BF)
                bias[me, pl.ds(grp, 1), cv] += jnp.sum(dv, axis=0, keepdims=True)

    def step(i, do_a, do_b):
        b = i - 2
        if do_b:
            @pl.when(b >= NP)
            def _():
                exchange(0, b - NP, 9, 12)

            stat_wait(b)

            @pl.when(b >= 2)
            def _():
                dkv_copy(b - 2).wait()

            od_pre(b, True)
        if do_a:
            @pl.when(i + B4 < STEPS)
            def _():
                raw_copy(i + B4).wait()

            @pl.when(i + B4 + 1 < STEPS)
            def _():
                raw_copy(i + B4 + 1).start()

        if do_b:
            combine(b)
            stage_b(b)
        if do_a:
            stage_a(i)
            sort_frames(i + B4)
        if do_b:
            acc[b // NP] += jnp.dot(mt[b % 3], dkv[b % 2], preferred_element_type=F32)
        if do_a:
            stat_send(i)
        if do_b:
            dkv_copy(b).start()
            od_post(b, True)

    barrier = pltpu.get_barrier_semaphore()
    for k in range(1, B4):
        pl.semaphore_signal(barrier, inc=1, device_id={"cp": (me + k) % B4}, device_id_type=MESH)
    top, low = pl.ds(0, ROWS), pl.ds(ROWS, D - ROWS)
    rest = pl.ds(0, D - ROWS)
    loads = [pltpu.make_async_copy(x, y, in_sem.at[k]) for k, (x, y) in enumerate((
        (h_hbm, res.at[0]), (wq_hbm.at[top], kv.at[0]), (wq_hbm.at[low], dkv.at[0, rest]), (dy_hbm, res.at[1]),
        (wo_hbm.at[top], kv.at[1]), (wo_hbm.at[low], dkv.at[1, rest]), (wk_hbm, wk), (wv_hbm, wv)))]
    raw_copy(0).start()
    for cp in loads:
        cp.start()
    fine[...] = jnp.zeros(fine.shape, F32)
    bias[me] = jnp.zeros((B8, D), F32)
    for cp in loads[:-2]:
        cp.wait()

    def first(n, carry):
        raw_copy(n).wait()
        raw_copy(n + 1).start()
        rows = pl.ds(pl.multiple_of(RC * n, RC), RC)
        x_hat, _ = norm_parts(res[0, rows].astype(F32))
        x = (x_hat * gain[...] + shift[...]).astype(BF)
        q[rows] = (jnp.dot(x[:, :ROWS], kv[0], preferred_element_type=F32)
                   + jnp.dot(x[:, ROWS:], dkv[0, rest], preferred_element_type=F32) + bq[...]).astype(BF)
        do[rows, :ROWS] = dotg(res[1, rows], kv[1], 1, 1).astype(BF)
        do[rows, ROWS:] = dotg(res[1, rows], dkv[1, rest], 1, 1).astype(BF)
        sort_frames(n)
        for g in range(2):
            acc[g, rows] = jnp.zeros((RC, D), F32)
        return carry

    lax.fori_loop(0, TOK // RC, first, 0)
    for cp in loads[-2:]:
        cp.wait()
    pl.semaphore_wait(barrier, 3)

    def run(lo, hi, do_a, do_b):
        def body(i, carry):
            step(i, do_a, do_b)
            return carry
        lax.fori_loop(lo, hi, body, 0)

    run(0, 2, True, False)
    run(2, STEPS, True, True)
    run(STEPS, STEPS + 2, False, True)

    def b_copy(k, src):
        return remote(bias.at[src], bias.at[src], b_send.at[k - 1], b_recv.at[src], (me + k) % 4)

    for k in range(1, 4):
        b_copy(k, me).start()
    dkv_copy(STEPS - 2).wait()
    dkv_copy(STEPS - 1).wait()

    bufs = (kv, dkv)

    def c_load(c, s):
        return [pltpu.make_async_copy(dkv_hbm.at[g, c], bufs[s].at[g], raw_sem.at[g] if s == 0 else dkv_sem.at[g]) for g in range(2)]

    def dm_copy(c, s):
        return pltpu.make_async_copy(frames.at[0, pl.ds(ROWS * s, ROWS)], dm_hbm.at[c], dm_sem.at[s])

    for cp in c_load(0, 0):
        cp.start()

    def c_step(u, carry):
        for s in range(2):
            c = 2 * u + s
            for cp in c_load(c, s):
                cp.wait()

            @pl.when(c + 1 < NP)
            def _():
                for cp in c_load(c + 1, 1 - s):
                    cp.start()

            @pl.when(c >= 2)
            def _():
                dm_copy(c - 2, s).wait()

            exchange(0, c + NP, 9, 12)
            exchange(1, c, 6, 10)

            @pl.when(c < 7)
            def _():
                od_pre(c + STEPS, False)

            x = jnp.concatenate([bufs[s][0], bufs[s][1]], axis=1)
            w = jnp.concatenate([wk[:, :W], wv[:, :W], wk[:, W:], wv[:, W:]], axis=1)
            frames[0, pl.ds(ROWS * s, ROWS)] = dotg(x, w, 1, 1).astype(BF)
            dm_copy(c, s).start()

            @pl.when(c < 7)
            def _():
                od_post(c + STEPS, False)

            @pl.when(c == 9)
            def _():
                pltpu.make_async_copy(res.at[0], res.at[0], res_recv).wait()
                pltpu.make_async_copy(res, res_hbm, out_sem.at[2]).start()
        return carry

    lax.fori_loop(0, NP // 2, c_step, 0)
    for t in range(NP, 10 + NCH + 2):
        exchange(1, t, 6, 10)
    for k in range(1, 4):
        b_copy(k, (me + k) % 4).wait_recv()
        b_copy(k, me).wait_send()
    big1[0:8, :] = (bias[0, :, 0:W] + bias[1, :, 0:W]) + (bias[2, :, 0:W] + bias[3, :, 0:W])
    big1[8:16, :] = (bias[0, :, W:] + bias[1, :, W:]) + (bias[2, :, W:] + bias[3, :, W:])
    bias_out = pltpu.make_async_copy(big1.at[0:16], bias_hbm, out_sem.at[3])
    bias_out.start()
    dm_copy(NP - 2, 0).wait()
    dm_copy(NP - 1, 1).wait()
    dw_copy(0).wait()
    dw_copy(1).wait()
    pltpu.make_async_copy(res, res_hbm, out_sem.at[2]).wait()
    bias_out.wait()


def attention(mt, h, dy, w_q, w_o, w_k, w_v, gain, shift, b_q, b_v):
    vm = pl.BlockSpec(memory_space=VMEM)
    hbm = pl.BlockSpec(memory_space=pl.ANY)
    dma = pltpu.SemaphoreType.DMA
    d2, d4, d8, dn = dma((B2,)), dma((B4,)), dma((B8,)), dma((B2, NCH))
    credit = pltpu.SemaphoreType.REGULAR((B2,))
    probs, mat, rows32 = VMEM((B2, B4, FP, LANES), F32), VMEM((D, D), BF), VMEM((B4, T, W), F32)
    return pl.pallas_call(
        attn_kernel, name="attention",
        out_shape=(SDS((B2, TOK, D), BF), SDS((B2, D, D), F32), SDS((2 * B8, W), F32), SDS((NP, ROWS, D), BF),
                   SDS((B2, NP, ROWS, D), BF)),
        in_specs=[hbm] * 7 + [vm] * B4,
        out_specs=(hbm,) * 5,
        scratch_shapes=[
            VMEM((B2, F, B8, QW), BF), VMEM((QW // LANES, 9 * FP, LANES), F32), VMEM((B2, B8 * FP, D), BF), mat, mat, mat, mat,
            VMEM((B2, ROWS, D), BF), probs, probs, VMEM((3, D, ROWS), BF), VMEM((B4, B4, 2 * B8, LANES), F32),
            VMEM((B8, LANES), F32), VMEM((B2, ROWS, D), BF), VMEM((B2, D, D), F32), VMEM((B4, B8, D), F32),
            VMEM((B2, B2, 2 * T, W), F32), VMEM((B4, 2 * T, W), F32), rows32, rows32, VMEM((B8, T, W), F32),
            VMEM((B2, TOK, D), BF), VMEM((D, W), F32), VMEM((B2, D // 2, W), F32),
            d2, d8, d2, d2, d4, d4, d4, d4, d4, d8, d8, d8, d8, d4, d4, dma, d2, d2, dn, dn, dn, dn, dn, dn, d2, d4, d4,
            credit, credit],
        compiler_params=pltpu.CompilerParams(vmem_limit_bytes=67043328, collective_id=0, has_side_effects=True),
    )(mt, h, dy, w_q, w_o, w_k, w_v, gain, shift, b_q, b_v)


def solution(mesh):
    act_spec = P("dp", None, None)
    mem_spec = P("dp", "cp", None)
    vec_out = P("dp")
    mat_out = P("dp", None)
    in_specs = (act_spec, mem_spec, P(), P(), P(), P(), P(), P(), P(), P(), P(), act_spec)
    out_specs = (act_spec, act_spec, mem_spec, vec_out, vec_out, mat_out, vec_out, mat_out, mat_out, vec_out, mat_out, vec_out)

    def device_step(hidden, memory, ln_gain, ln_bias, w_q, b_q, w_k, w_v, b_v, w_o, b_o, grad_y):
        h = hidden.reshape(TOK, D)
        dy = grad_y.reshape(TOK, D)
        gain, shift, bq, bv, bo = (a.astype(F32).reshape(1, D) for a in (ln_gain, ln_bias, b_q, b_v, b_o))
        res, dw, bias, dm, _ = attention(memory.transpose(1, 0, 2), h, dy, w_q, w_o, w_k, w_v, gain, shift, bq, bv)
        gm, y, gh, gwo, gwq, gwk, gwv, vec = finish(dm.reshape(NB, FP, D), res, h, dy, w_o, w_q, dw, gain, shift, bo)
        grad_bq = bias[0:2].reshape(D)
        grad_bv = bias[8:10].reshape(D)
        return (y.reshape(NB, T, D), gh.reshape(NB, T, D), gm.transpose(1, 0, 2), vec[0], vec[1], gwq, grad_bq,
                gwk, gwv, grad_bv, gwo, vec[2])

    return jax.shard_map(device_step, mesh=mesh, in_specs=in_specs, out_specs=out_specs, check_vma=False)
```

```python
import functools
import math
import jax
import jax.numpy as jnp
from jax import lax
from jax.experimental import pallas as pl
from jax.experimental.pallas import tpu as pltpu
from jax.sharding import PartitionSpec as P

EPS = 1e-5
HEAD = 64
F, FP, D, T = 375, 384, 1024, 32
NB = 32
NP = NB // 2
STEPS = 2 * NP
W = 512
ROWS = 2 * FP
QW = 256
BF, F32 = jnp.bfloat16, jnp.float32
LOG2 = 0.125 * math.log2(math.e)
MESH = pl.DeviceIdType.MESH
VMEM = pltpu.VMEM
B2, B4, B8, LANES = 2, 4, 8, 128
RC = 256
TOK = NB * T
SDS = jax.ShapeDtypeStruct


def dotg(a, b, ca, cb):
    return lax.dot_general(a, b, (((ca,), (cb,)), ((), ())), preferred_element_type=F32)


FC = 32
NFC = FP // FC


def fixed(rows):
    return pl.BlockSpec((rows, D), lambda s: (0, 0), pipeline_mode=pl.Buffered(1))


def lanes(t):
    return slice(LANES * t, LANES * (t + 1))


def permutation(axis):
    r = lax.broadcasted_iota(jnp.int32, (QW, QW), axis)
    k = lax.broadcasted_iota(jnp.int32, (QW, QW), 1 - axis)
    return (k == r % FC * B8 + r // FC).astype(F32).astype(BF)


def norm_parts(h):
    centered = h - jnp.mean(h, axis=-1, keepdims=True)
    inv_std = lax.rsqrt(jnp.mean(centered * centered, axis=-1, keepdims=True) + EPS)
    return centered * inv_std, inv_std


JOB0, JOBS = 3, 4
FB = 64
NFB = FP // FB


def finish_kernel(dm_ref, res_hbm, h_hbm, dy_hbm, wo_hbm, wq_hbm, dw_hbm, gain, shift, bo,
                  gm_ref, y_hbm, gh_hbm, gwo_hbm, gwq_hbm, gwk_hbm, gwv_hbm, vec_ref,
                  perm, res, h, dy, wo, wq, x, y, gh, gw, stage, in_sem, y_sem, gh_sem, gw_sem, ld_sem, st_sem):
    step = pl.program_id(0)
    loads = [pltpu.make_async_copy(a, b, in_sem.at[k]) for k, (a, b) in enumerate(
        ((h_hbm, h), (res_hbm, res), (wo_hbm, wo), (dy_hbm, dy), (wq_hbm, wq)))]

    def rows(n):
        return pl.ds(pl.multiple_of(RC * n, RC), RC)

    def out_copy(src, dst, sem, n):
        return pltpu.make_async_copy(src.at[rows(n)], dst.at[rows(n)], sem.at[n])

    def gw_copy(dst, n):
        return pltpu.make_async_copy(gw.at[n], dst.at[rows(n)], gw_sem.at[n])

    def piece_in(k):
        g, v = k // 2, k % 2
        return pltpu.make_async_copy(dw_hbm.at[g, :, pl.ds(W * v, W)], stage.at[k % 2], ld_sem.at[k % 2])

    def piece_out(k):
        g, v = k // 2, k % 2
        return pltpu.make_async_copy(stage.at[k % 2], (gwk_hbm, gwv_hbm)[v].at[:, pl.ds(W * g, W)], st_sem.at[k % 2])

    @pl.when(step == 0)
    def _():
        for cp in loads:
            cp.start()
        piece_in(0).start()
        piece_in(1).start()
        vec_ref[...] = jnp.zeros_like(vec_ref)
        perm[...] = permutation(1)

    for k in range(4):
        @pl.when(step == 4 + 5 * (k // 2) + k % 2)
        def _():
            piece_in(k).wait()
            piece_out(k).start()

        @pl.when(step == 7 + 5 * (k // 2) + k % 2)
        def _():
            if k < 2:
                piece_out(k).wait()
                piece_in(k + 2).start()

    @pl.when(step == JOB0)
    def _():
        for cp in loads:
            cp.wait()

    job = step - JOB0
    n = job % JOBS

    @pl.when((job >= 0) & (job < JOBS))
    def _():
        hf = h[rows(n)].astype(F32)
        x_hat, _ = norm_parts(hf)
        x[rows(n)] = (x_hat * gain[...] + shift[...]).astype(BF)
        y[rows(n)] = (hf + jnp.dot(res[0, rows(n)], wo[...], preferred_element_type=F32) + bo[...]).astype(BF)
        out_copy(y, y_hbm, y_sem, n).start()

    @pl.when((job >= JOBS) & (job < 2 * JOBS))
    def _():
        gw[n] = dotg(res[0, :, rows(n)], dy[...], 0, 0)
        gw_copy(gwo_hbm, n).start()

    @pl.when((job >= 2 * JOBS) & (job < 3 * JOBS))
    def _():
        x_hat, inv_std = norm_parts(h[rows(n)].astype(F32))
        dyf = dy[rows(n)].astype(F32)
        d_x = dotg(res[1, rows(n)], wq[...], 1, 1)
        vec_ref[0:1] += jnp.sum(d_x * x_hat, axis=0, keepdims=True)
        vec_ref[1:2] += jnp.sum(d_x, axis=0, keepdims=True)
        vec_ref[2:3] += jnp.sum(dyf, axis=0, keepdims=True)
        d_hat = d_x * gain[...]
        d_h = inv_std * (d_hat - jnp.mean(d_hat, axis=-1, keepdims=True) - x_hat * jnp.mean(d_hat * x_hat, axis=-1, keepdims=True))
        gh[rows(n)] = (dyf + d_h).astype(BF)
        out_copy(gh, gh_hbm, gh_sem, n).start()

    @pl.when((job >= 3 * JOBS) & (job < 4 * JOBS))
    def _():
        gw_copy(gwo_hbm, n).wait()
        gw[n] = dotg(x[:, rows(n)], res[1], 0, 0)
        gw_copy(gwq_hbm, n).start()

    for k in range(FB // FC):
        z = dm_ref[:, FC * k:FC * (k + 1), :].reshape(QW, D)
        z = jnp.dot(perm[...], z, preferred_element_type=F32)
        gm_ref[FC * k:FC * (k + 1)] = z.astype(BF).reshape(FC, B8, D)

    @pl.when(step == pl.num_programs(0) - 1)
    def _():
        for k in range(JOBS):
            out_copy(y, y_hbm, y_sem, k).wait()
            out_copy(gh, gh_hbm, gh_sem, k).wait()
            gw_copy(gwq_hbm, k).wait()
        for k in (2, 3):
            piece_out(k).wait()


def finish(dm, res, h, dy, w_o, w_q, dw, gain, shift, b_o):
    hbm = pl.BlockSpec(memory_space=pl.ANY)
    vec = fixed(1)
    dma = pltpu.SemaphoreType.DMA
    mat, dj = VMEM((D, D), BF), dma((JOBS,))
    return pl.pallas_call(
        finish_kernel, grid=(NB // B8 * NFB,), name="finish",
        out_shape=(SDS((F, NB, D), BF), SDS((TOK, D), BF), SDS((TOK, D), BF), SDS((D, D), F32), SDS((D, D), F32),
                   SDS((D, D), F32), SDS((D, D), F32), SDS((B8, D), F32)),
        in_specs=[pl.BlockSpec((B8, FB, D), lambda s: (s // NFB, s % NFB, 0))] + [hbm] * 6 + [vec] * 3,
        out_specs=(pl.BlockSpec((FB, B8, D), lambda s: (s % NFB, s // NFB, 0)),) + (hbm,) * 6 + (pl.BlockSpec((B8, D), lambda s: (0, 0)),),
        scratch_shapes=[
            VMEM((QW, QW), BF), VMEM((B2, TOK, D), BF), mat, mat, mat, mat, mat, mat, mat, VMEM((JOBS, RC, D), F32),
            VMEM((B2, D, W), F32), dma((B8,)), dj, dj, dj, dma((B2,)), dma((B2,))],
        compiler_params=pltpu.CompilerParams(vmem_limit_bytes=50 << 20),
    )(dm, res, h, dy, w_o, w_q, dw, gain, shift, b_o)


def block_mask():
    return lax.broadcasted_iota(jnp.int32, (128, 256), 0) // T == lax.broadcasted_iota(jnp.int32, (128, 256), 1) // HEAD


def block_diag(x, mask):
    return jnp.where(mask, jnp.concatenate([x] * 4, axis=0), jnp.zeros((), BF))


def when(cond):
    if isinstance(cond, bool):
        return (lambda f: f()) if cond else (lambda f: None)
    return pl.when(cond)


CH = 64
NCH = D // 2 // CH


def attn_kernel(m_hbm, h_hbm, dy_hbm, wq_hbm, wo_hbm, wk_hbm, wv_hbm, gain, shift, bq, bv,
                res_hbm, dw_hbm, bias_hbm, dm_hbm, dkv_hbm,
                raw, perm, frames, q, do, wk, wv, kv, e_s, dp_s, mt, stats, coef, dkv, acc, bias, od, r1, keep, x2, r2, res, big1, big2,
                raw_sem, in_sem, dkv_sem, dm_sem, out_sem, st_send, st_recv, s1_send, s1_recv, s2_send, s2_recv,
                s3_send, s3_recv, s3s_send, s4_send, res_recv, e1_send, e1_recv, e2_send, e2_recv,
                e3_send, e3_recv, e3s_send, e4_send, acc_recv, b_send, b_recv, free_sib, free_xn):
    me = lax.axis_index("cp")
    cx, cc = me // 2, me % 2
    sib, xn = 2 * cx + 1 - cc, 2 * (1 - cx) + cc

    def remote(src, dst, ss, rs, dev):
        return pltpu.make_async_remote_copy(src_ref=src, dst_ref=dst, send_sem=ss, recv_sem=rs,
                                            device_id={"cp": dev}, device_id_type=MESH)

    def raw_copy(c):
        seqs = pl.ds(pl.multiple_of(B8 * (c // B4 % B4), B8), B8)
        return pltpu.make_async_copy(m_hbm.at[:, seqs, quarter(c)], raw.at[c % 2, 0:F], raw_sem.at[c % 2])

    def quarter(c):
        return pl.ds(pl.multiple_of(c % B4 * QW, QW), QW)

    def sort_frames(c):
        for n in range(NFC):
            x = raw[c % 2, FC * n:FC * (n + 1)].reshape(QW, QW)
            y = jnp.dot(perm[...], x, preferred_element_type=F32).astype(BF)
            for b in range(B8):
                frames[c // B4 % 2, FP * b + FC * n:FP * b + FC * (n + 1), quarter(c)] = y[FC * b:FC * (b + 1)]

    def dkv_copy(i):
        return pltpu.make_async_copy(dkv.at[i % 2], dkv_hbm.at[i // NP, i % NP], dkv_sem.at[i % 2])

    def stat_send(i):
        for k in range(1, B4):
            remote(stats.at[i % B4, me], stats.at[i % B4, me], st_send.at[i % B4], st_recv.at[i % B4], (me + k) % B4).start()

    def stat_wait(i):
        three = stats.at[i % B4, 0:3]
        for sem in (st_recv, st_send):
            pltpu.make_async_copy(three, three, sem.at[i % B4]).wait()

    def s1(b):
        return remote(od.at[b % 2, 1 - cc], r1.at[b % 4], s1_send.at[b % 4], s1_recv.at[b % 4], sib)

    def s2(b):
        return remote(x2.at[b % 4], r2.at[b % 8], s2_send.at[b % 8], s2_recv.at[b % 8], xn)

    def res_at(b, x):
        return res.at[cc, pl.ds(pl.multiple_of(64 * (b % NP) + T * x, T), T), pl.ds(pl.multiple_of(W * (b // NP), W), W)]

    def s3(b, x):
        return remote(res_at(b, x), res_at(b, x), s3_send.at[b % 8], s3_recv.at[b % 8], xn)

    def s3s(b):
        return remote(res_at(b, cx), res_at(b, cx), s3s_send.at[b % 4], res_recv, sib)

    def s4(b):
        return remote(res_at(b, 1 - cx), res_at(b, 1 - cx), s4_send.at[b % 4], res_recv, sib)

    def od_pre(b, inside):
        def on(k):
            return (b >= k) if inside else (b - k < STEPS)

        @when(on(7))
        def _():
            s4(b - 7).wait_send()

        @when(on(5))
        def _():
            s3(b - 5, 1 - cx).wait_recv()
            s4(b - 5).start()
            s3(b - 5, cx).wait_send()
            s3s(b - 5).wait_send()

        @when(on(3))
        def _():
            s2(b - 3).wait_recv()
            s2(b - 3).wait_send()
            res_at(b - 3, cx)[...] = (keep[(b - 3) % 4] + r2[(b - 3) % 8]).astype(BF)

        @when(on(2))
        def _():
            s1(b - 2).wait_send()

        @when(on(1))
        def _():
            s1(b - 1).wait_recv()
            for ref, x in ((keep, cx), (x2, 1 - cx)):
                rows = pl.ds(pl.multiple_of(T * x, T), T)
                ref[(b - 1) % 4] = od[(b - 1) % 2, cc, rows, :] + r1[(b - 1) % 4, rows, :]

    def od_post(b, inside):
        def on(k):
            return (b >= k) if inside else (b - k < STEPS)

        if inside:
            s1(b).start()

        @when(on(1))
        def _():
            s2(b - 1).start()

        @when(on(3))
        def _():
            s3(b - 3, cx).start()
            s3s(b - 3).start()

    own = pl.ds(pl.multiple_of(W * cc, W), W)
    other = pl.ds(pl.multiple_of(W * (1 - cc), W), W)

    def rows_of(x, n):
        return pl.ds(pl.multiple_of(x * (D // 2) + CH * n, CH), CH)

    def e1(g):
        return remote(acc.at[g, :, other], big1, e1_send.at[g], e1_recv.at[g], sib)

    def e2(g, n):
        return remote(acc.at[g, rows_of(1 - cx, n), own], big2.at[g, pl.ds(pl.multiple_of(CH * n, CH), CH)],
                      e2_send.at[g, n], e2_recv.at[g, n], xn)

    def e3(g, n, x):
        ref = acc.at[g, rows_of(x, n), own]
        return remote(ref, ref, e3_send.at[g, n], e3_recv.at[g, n], xn)

    def to_sib(g, n, x, sem):
        ref = acc.at[g, rows_of(x, n), own]
        return remote(ref, ref, sem.at[g, n], acc_recv.at[g], sib)

    def dw_copy(g):
        return pltpu.make_async_copy(acc.at[g], dw_hbm.at[g], out_sem.at[g])

    def exchange(g, t, t3, t4):
        @when(t == 0)
        def _():
            e1(g).start()

        @when(t == 1)
        def _():
            e1(g).wait_send()
            pl.semaphore_signal(free_sib.at[g], inc=1, device_id={"cp": sib}, device_id_type=MESH)
            e1(g).wait_recv()

        @when(t == t3)
        def _():
            pl.semaphore_wait(free_sib.at[g], 1)

        def chunk(t0, f):
            n = t - t0
            if isinstance(n, int):
                if 0 <= n < NCH:
                    f(n)
            else:
                pl.when((n >= 0) & (n < NCH))(lambda: f(n))

        def reduce_core(n):
            for x in (cx, 1 - cx):
                acc[g, rows_of(x, n), own] += big1[rows_of(x, n), :]
            e2(g, n).start()

        def sent(n):
            e2(g, n).wait_send()
            pl.semaphore_signal(free_xn.at[g], inc=1, device_id={"cp": xn}, device_id_type=MESH)

        def reduce_chip(n):
            e2(g, n).wait_recv()
            pl.semaphore_wait(free_xn.at[g], 1)
            acc[g, rows_of(cx, n), own] += big2[g, pl.ds(pl.multiple_of(CH * n, CH), CH), :]
            e3(g, n, cx).start()
            to_sib(g, n, cx, e3s_send).start()

        def forward(n):
            e3(g, n, 1 - cx).wait_recv()
            to_sib(g, n, 1 - cx, e4_send).start()

        chunk(1, reduce_core)
        chunk(t3 - 1, sent)
        chunk(t3, reduce_chip)
        chunk(t4, forward)

        @when(t == t4 + NCH + 1)
        def _():
            remote(acc.at[g, :, other], acc.at[g, :, other], e1_send.at[g], acc_recv.at[g], sib).wait_recv()
            for n in range(NCH):
                e3(g, n, cx).wait_send()
                to_sib(g, n, cx, e3s_send).wait_send()
                to_sib(g, n, 1 - cx, e4_send).wait_send()
            dw_copy(g).start()

    def operands(i, j, h):
        cols = pl.ds(pl.multiple_of(W * (i // NP) + 256 * h, 256), 256)
        rows = pl.ds(pl.multiple_of(64 * (i % NP) + T * j, T), T)
        mask = block_mask()
        return block_diag(q[rows, cols], mask), block_diag(do[rows, cols], mask), mask

    def stage_a(i):
        slot = i % 2
        m = frames[i // B4 % 2, pl.ds(pl.multiple_of(i % B4 * ROWS, ROWS), ROWS), :]
        cols = pl.ds(pl.multiple_of(W * (i // NP), W), W)
        mt[i % 3] = m.T
        kv[slot, :, 0:W] = jnp.dot(m, wk[:, cols], preferred_element_type=F32).astype(BF)
        kv[slot, :, W:] = (jnp.dot(m, wv[:, cols], preferred_element_type=F32) + bv[:, cols]).astype(BF)
        real = lax.broadcasted_iota(jnp.int32, (FP, LANES), 0) < F
        for j in range(2):
            rows = slice(FP * j, FP * (j + 1))
            for h in range(2):
                n = 2 * j + h
                qb, db, _ = operands(i, j, h)
                s = dotg(kv[slot, rows, QW * h:QW * (h + 1)], qb, 1, 1)
                dp = dotg(kv[slot, rows, W + QW * h:W + QW * (h + 1)], db, 1, 1)
                s = jnp.where(real, s, -1e30)
                top = jnp.max(s, axis=0, keepdims=True)
                e = jnp.exp2((s - top) * LOG2)
                e_s[slot, n] = e
                dp_s[slot, n] = dp
                for k, row in enumerate((top, jnp.sum(e, axis=0, keepdims=True), jnp.sum(e * dp, axis=0, keepdims=True))):
                    stats[i % B4, me, B4 * k + n:B4 * k + n + 1, :] = row

    def combine(i):
        slot = i % 4
        tops = [stats[slot, d, 0:4, :] for d in range(4)]
        top = jnp.maximum(jnp.maximum(tops[0], tops[1]), jnp.maximum(tops[2], tops[3]))
        ws = [jnp.exp2((t - top) * LOG2) for t in tops]
        total = sum(stats[slot, d, 4:8, :] * ws[d] for d in range(4))
        dots = sum(stats[slot, d, 8:12, :] * ws[d] for d in range(4))
        coef[0:4, :] = jnp.exp2((stats[slot, me, 0:4, :] - top) * LOG2) / total
        coef[4:8, :] = dots / total

    def stage_b(i):
        slot = i % 2
        grp = i // NP
        for j in range(2):
            rows = slice(FP * j, FP * (j + 1))
            for h in range(2):
                n = 2 * j + h
                qb, db, mask = operands(i, j, h)
                ck, cv = slice(256 * h, 256 * (h + 1)), slice(W + 256 * h, W + 256 * (h + 1))
                p = e_s[slot, n] * coef[n:n + 1, :]
                pb = p.astype(BF)
                gb = (p * (dp_s[slot, n] - coef[4 + n:5 + n, :]) * 0.125).astype(BF)
                o = dotg(pb, kv[slot, rows, cv], 0, 0)
                dq = dotg(gb, kv[slot, rows, ck], 0, 0)
                for which, x in ((0, o), (1, dq)):
                    x = jnp.where(mask, x, 0.0)
                    x = (x[0:32] + x[32:64]) + (x[64:96] + x[96:128])
                    od[slot, which, T * j:T * (j + 1), ck] = x
                    if which == 1:
                        bias[me, pl.ds(grp, 1), ck] += jnp.sum(x, axis=0, keepdims=True)
                dk = jnp.dot(gb, qb, preferred_element_type=F32)
                dv = jnp.dot(pb, db, preferred_element_type=F32)
                dkv[slot, rows, ck] = dk.astype(BF)
                dkv[slot, rows, cv] = dv.astype(BF)
                bias[me, pl.ds(grp, 1), cv] += jnp.sum(dv, axis=0, keepdims=True)

    def step(i, do_a, do_b):
        b = i - 2
        if do_b:
            @pl.when(b >= NP)
            def _():
                exchange(0, b - NP, 9, 12)

            stat_wait(b)

            @pl.when(b >= 2)
            def _():
                dkv_copy(b - 2).wait()

            od_pre(b, True)
        if do_a:
            @pl.when(i + B4 < STEPS)
            def _():
                raw_copy(i + B4).wait()

            @pl.when(i + B4 + 1 < STEPS)
            def _():
                raw_copy(i + B4 + 1).start()

        if do_b:
            combine(b)
            stage_b(b)
        if do_a:
            stage_a(i)
            sort_frames(i + B4)
        if do_b:
            acc[b // NP] += jnp.dot(mt[b % 3], dkv[b % 2], preferred_element_type=F32)
        if do_a:
            stat_send(i)
        if do_b:
            dkv_copy(b).start()
            od_post(b, True)

    barrier = pltpu.get_barrier_semaphore()
    for k in range(1, B4):
        pl.semaphore_signal(barrier, inc=1, device_id={"cp": (me + k) % B4}, device_id_type=MESH)
    top, low = pl.ds(0, ROWS), pl.ds(ROWS, D - ROWS)
    rest = pl.ds(0, D - ROWS)
    loads = [pltpu.make_async_copy(x, y, in_sem.at[k]) for k, (x, y) in enumerate((
        (h_hbm, res.at[0]), (wq_hbm.at[top], kv.at[0]), (wq_hbm.at[low], dkv.at[0, rest]), (dy_hbm, res.at[1]),
        (wo_hbm.at[top], kv.at[1]), (wo_hbm.at[low], dkv.at[1, rest]), (wk_hbm, wk), (wv_hbm, wv)))]
    raw_copy(0).start()
    for cp in loads:
        cp.start()
    raw[:, F:] = jnp.zeros((B2, FP - F, B8, QW), BF)
    perm[...] = permutation(0)
    bias[me] = jnp.zeros((B8, D), F32)
    for cp in loads[:-2]:
        cp.wait()

    def first(n, carry):
        raw_copy(n).wait()
        raw_copy(n + 1).start()
        rows = pl.ds(pl.multiple_of(RC * n, RC), RC)
        x_hat, _ = norm_parts(res[0, rows].astype(F32))
        x = (x_hat * gain[...] + shift[...]).astype(BF)
        q[rows] = (jnp.dot(x[:, :ROWS], kv[0], preferred_element_type=F32)
                   + jnp.dot(x[:, ROWS:], dkv[0, rest], preferred_element_type=F32) + bq[...]).astype(BF)
        do[rows, :ROWS] = dotg(res[1, rows], kv[1], 1, 1).astype(BF)
        do[rows, ROWS:] = dotg(res[1, rows], dkv[1, rest], 1, 1).astype(BF)
        sort_frames(n)
        for g in range(2):
            acc[g, rows] = jnp.zeros((RC, D), F32)
        return carry

    lax.fori_loop(0, TOK // RC, first, 0)
    for cp in loads[-2:]:
        cp.wait()
    pl.semaphore_wait(barrier, 3)

    def run(lo, hi, do_a, do_b):
        def body(i, carry):
            step(i, do_a, do_b)
            return carry
        lax.fori_loop(lo, hi, body, 0)

    run(0, 2, True, False)
    run(2, STEPS, True, True)
    run(STEPS, STEPS + 2, False, True)

    def b_copy(k, src):
        return remote(bias.at[src], bias.at[src], b_send.at[k - 1], b_recv.at[src], (me + k) % 4)

    for k in range(1, 4):
        b_copy(k, me).start()
    dkv_copy(STEPS - 2).wait()
    dkv_copy(STEPS - 1).wait()

    bufs = (kv, dkv)

    def c_load(c, s):
        return [pltpu.make_async_copy(dkv_hbm.at[g, c], bufs[s].at[g], raw_sem.at[g] if s == 0 else dkv_sem.at[g]) for g in range(2)]

    def dm_copy(c, s):
        return pltpu.make_async_copy(frames.at[0, pl.ds(ROWS * s, ROWS)], dm_hbm.at[c], dm_sem.at[s])

    for cp in c_load(0, 0):
        cp.start()

    def c_step(u, carry):
        for s in range(2):
            c = 2 * u + s
            for cp in c_load(c, s):
                cp.wait()

            @pl.when(c + 1 < NP)
            def _():
                for cp in c_load(c + 1, 1 - s):
                    cp.start()

            @pl.when(c >= 2)
            def _():
                dm_copy(c - 2, s).wait()

            exchange(0, c + NP, 9, 12)
            exchange(1, c, 6, 10)

            @pl.when(c < 7)
            def _():
                od_pre(c + STEPS, False)

            x = jnp.concatenate([bufs[s][0], bufs[s][1]], axis=1)
            w = jnp.concatenate([wk[:, :W], wv[:, :W], wk[:, W:], wv[:, W:]], axis=1)
            frames[0, pl.ds(ROWS * s, ROWS)] = dotg(x, w, 1, 1).astype(BF)
            dm_copy(c, s).start()

            @pl.when(c < 7)
            def _():
                od_post(c + STEPS, False)

            @pl.when(c == 9)
            def _():
                pltpu.make_async_copy(res.at[0], res.at[0], res_recv).wait()
                pltpu.make_async_copy(res, res_hbm, out_sem.at[2]).start()
        return carry

    lax.fori_loop(0, NP // 2, c_step, 0)
    for t in range(NP, 10 + NCH + 2):
        exchange(1, t, 6, 10)
    for k in range(1, 4):
        b_copy(k, (me + k) % 4).wait_recv()
        b_copy(k, me).wait_send()
    big1[0:8, :] = (bias[0, :, 0:W] + bias[1, :, 0:W]) + (bias[2, :, 0:W] + bias[3, :, 0:W])
    big1[8:16, :] = (bias[0, :, W:] + bias[1, :, W:]) + (bias[2, :, W:] + bias[3, :, W:])
    bias_out = pltpu.make_async_copy(big1.at[0:16], bias_hbm, out_sem.at[3])
    bias_out.start()
    dm_copy(NP - 2, 0).wait()
    dm_copy(NP - 1, 1).wait()
    dw_copy(0).wait()
    dw_copy(1).wait()
    pltpu.make_async_copy(res, res_hbm, out_sem.at[2]).wait()
    bias_out.wait()


def attention(mt, h, dy, w_q, w_o, w_k, w_v, gain, shift, b_q, b_v):
    vm = pl.BlockSpec(memory_space=VMEM)
    hbm = pl.BlockSpec(memory_space=pl.ANY)
    dma = pltpu.SemaphoreType.DMA
    d2, d4, d8, dn = dma((B2,)), dma((B4,)), dma((B8,)), dma((B2, NCH))
    credit = pltpu.SemaphoreType.REGULAR((B2,))
    probs, mat, rows32 = VMEM((B2, B4, FP, LANES), F32), VMEM((D, D), BF), VMEM((B4, T, W), F32)
    return pl.pallas_call(
        attn_kernel, name="attention",
        out_shape=(SDS((B2, TOK, D), BF), SDS((B2, D, D), F32), SDS((2 * B8, W), F32), SDS((NP, ROWS, D), BF),
                   SDS((B2, NP, ROWS, D), BF)),
        in_specs=[hbm] * 7 + [vm] * B4,
        out_specs=(hbm,) * 5,
        scratch_shapes=[
            VMEM((B2, FP, B8, QW), BF), VMEM((QW, QW), BF), VMEM((B2, B8 * FP, D), BF), mat, mat, mat, mat,
            VMEM((B2, ROWS, D), BF), probs, probs, VMEM((3, D, ROWS), BF), VMEM((B4, B4, 2 * B8, LANES), F32),
            VMEM((B8, LANES), F32), VMEM((B2, ROWS, D), BF), VMEM((B2, D, D), F32), VMEM((B4, B8, D), F32),
            VMEM((B2, B2, 2 * T, W), F32), VMEM((B4, 2 * T, W), F32), rows32, rows32, VMEM((B8, T, W), F32),
            VMEM((B2, TOK, D), BF), VMEM((D, W), F32), VMEM((B2, D // 2, W), F32),
            d2, d8, d2, d2, d4, d4, d4, d4, d4, d8, d8, d8, d8, d4, d4, dma, d2, d2, dn, dn, dn, dn, dn, dn, d2, d4, d4,
            credit, credit],
        compiler_params=pltpu.CompilerParams(vmem_limit_bytes=67043328, collective_id=0, has_side_effects=True),
    )(mt, h, dy, w_q, w_o, w_k, w_v, gain, shift, b_q, b_v)


def solution(mesh):
    act_spec = P("dp", None, None)
    mem_spec = P("dp", "cp", None)
    vec_out = P("dp")
    mat_out = P("dp", None)
    in_specs = (act_spec, mem_spec, P(), P(), P(), P(), P(), P(), P(), P(), P(), act_spec)
    out_specs = (act_spec, act_spec, mem_spec, vec_out, vec_out, mat_out, vec_out, mat_out, mat_out, vec_out, mat_out, vec_out)

    def device_step(hidden, memory, ln_gain, ln_bias, w_q, b_q, w_k, w_v, b_v, w_o, b_o, grad_y):
        h = hidden.reshape(TOK, D)
        dy = grad_y.reshape(TOK, D)
        gain, shift, bq, bv, bo = (a.astype(F32).reshape(1, D) for a in (ln_gain, ln_bias, b_q, b_v, b_o))
        res, dw, bias, dm, _ = attention(memory.transpose(1, 0, 2), h, dy, w_q, w_o, w_k, w_v, gain, shift, bq, bv)
        gm, y, gh, gwo, gwq, gwk, gwv, vec = finish(dm.reshape(NB, FP, D), res, h, dy, w_o, w_q, dw, gain, shift, bo)
        grad_bq = bias[0:2].reshape(D)
        grad_bv = bias[8:10].reshape(D)
        return (y.reshape(NB, T, D), gh.reshape(NB, T, D), gm.transpose(1, 0, 2), vec[0], vec[1], gwq, grad_bq,
                gwk, gwv, grad_bv, gwo, vec[2])

    return jax.shard_map(device_step, mesh=mesh, in_specs=in_specs, out_specs=out_specs, check_vma=False)
```

```python
import functools
import math
import jax
import jax.numpy as jnp
from jax import lax
from jax.experimental import pallas as pl
from jax.experimental.pallas import tpu as pltpu
from jax.sharding import PartitionSpec as P

EPS = 1e-5
HEAD = 64
F, FP, D, T = 375, 384, 1024, 32
NB = 32
NP = NB // 2
STEPS = 2 * NP
W = 512
ROWS = 2 * FP
QW = 256
BF, F32 = jnp.bfloat16, jnp.float32
LOG2 = 0.125 * math.log2(math.e)
MESH = pl.DeviceIdType.MESH
VMEM = pltpu.VMEM
B2, B4, B8, LANES = 2, 4, 8, 128
RC = 256
TOK = NB * T
SDS = jax.ShapeDtypeStruct


def dotg(a, b, ca, cb):
    return lax.dot_general(a, b, (((ca,), (cb,)), ((), ())), preferred_element_type=F32)


FC = 32
NFC = FP // FC


def fixed(rows):
    return pl.BlockSpec((rows, D), lambda s: (0, 0), pipeline_mode=pl.Buffered(1))


def lanes(t):
    return slice(LANES * t, LANES * (t + 1))


def permutation(n):
    r = lax.broadcasted_iota(jnp.int32, (QW, QW), 0)
    k = lax.broadcasted_iota(jnp.int32, (QW, QW), 1)
    return (k == r % n * (QW // n) + r // n).astype(F32).astype(BF)


def norm_parts(h):
    centered = h - jnp.mean(h, axis=-1, keepdims=True)
    inv_std = lax.rsqrt(jnp.mean(centered * centered, axis=-1, keepdims=True) + EPS)
    return centered * inv_std, inv_std


JOB0, JOBS = 3, 4
FB = 16


def finish_kernel(dm_ref, res_hbm, h_hbm, dy_hbm, wo_hbm, wq_hbm, dw_hbm, gain, shift, bo,
                  gm_ref, y_hbm, gh_hbm, gwo_hbm, gwq_hbm, gwk_hbm, gwv_hbm, vec_ref,
                  perm, res, h, dy, wo, wq, x, y, gh, gw, stage, in_sem, y_sem, gh_sem, gw_sem, ld_sem, st_sem):
    step = pl.program_id(0)
    loads = [pltpu.make_async_copy(a, b, in_sem.at[k]) for k, (a, b) in enumerate(
        ((h_hbm, h), (res_hbm, res), (wo_hbm, wo), (dy_hbm, dy), (wq_hbm, wq)))]

    def rows(n):
        return pl.ds(pl.multiple_of(RC * n, RC), RC)

    def out_copy(src, dst, sem, n):
        return pltpu.make_async_copy(src.at[rows(n)], dst.at[rows(n)], sem.at[n])

    def gw_copy(dst, n):
        return pltpu.make_async_copy(gw.at[n], dst.at[rows(n)], gw_sem.at[n])

    def piece_in(k):
        g, v = k // 2, k % 2
        return pltpu.make_async_copy(dw_hbm.at[g, :, pl.ds(W * v, W)], stage.at[k % 2], ld_sem.at[k % 2])

    def piece_out(k):
        g, v = k // 2, k % 2
        return pltpu.make_async_copy(stage.at[k % 2], (gwk_hbm, gwv_hbm)[v].at[:, pl.ds(W * g, W)], st_sem.at[k % 2])

    @pl.when(step == 0)
    def _():
        for cp in loads:
            cp.start()
        piece_in(0).start()
        piece_in(1).start()
        vec_ref[...] = jnp.zeros_like(vec_ref)
        perm[...] = permutation(FB)

    for k in range(4):
        @pl.when(step == 4 + 5 * (k // 2) + k % 2)
        def _():
            piece_in(k).wait()
            piece_out(k).start()

        @pl.when(step == 7 + 5 * (k // 2) + k % 2)
        def _():
            if k < 2:
                piece_out(k).wait()
                piece_in(k + 2).start()

    @pl.when(step == JOB0)
    def _():
        for cp in loads:
            cp.wait()

    job = step - JOB0
    n = job % JOBS

    @pl.when((job >= 0) & (job < JOBS))
    def _():
        hf = h[rows(n)].astype(F32)
        x_hat, _ = norm_parts(hf)
        x[rows(n)] = (x_hat * gain[...] + shift[...]).astype(BF)
        y[rows(n)] = (hf + jnp.dot(res[0, rows(n)], wo[...], preferred_element_type=F32) + bo[...]).astype(BF)
        out_copy(y, y_hbm, y_sem, n).start()

    @pl.when((job >= JOBS) & (job < 2 * JOBS))
    def _():
        gw[n] = dotg(res[0, :, rows(n)], dy[...], 0, 0)
        gw_copy(gwo_hbm, n).start()

    @pl.when((job >= 2 * JOBS) & (job < 3 * JOBS))
    def _():
        x_hat, inv_std = norm_parts(h[rows(n)].astype(F32))
        dyf = dy[rows(n)].astype(F32)
        d_x = dotg(res[1, rows(n)], wq[...], 1, 1)
        vec_ref[0:1] += jnp.sum(d_x * x_hat, axis=0, keepdims=True)
        vec_ref[1:2] += jnp.sum(d_x, axis=0, keepdims=True)
        vec_ref[2:3] += jnp.sum(dyf, axis=0, keepdims=True)
        d_hat = d_x * gain[...]
        d_h = inv_std * (d_hat - jnp.mean(d_hat, axis=-1, keepdims=True) - x_hat * jnp.mean(d_hat * x_hat, axis=-1, keepdims=True))
        gh[rows(n)] = (dyf + d_h).astype(BF)
        out_copy(gh, gh_hbm, gh_sem, n).start()

    @pl.when((job >= 3 * JOBS) & (job < 4 * JOBS))
    def _():
        gw_copy(gwo_hbm, n).wait()
        gw[n] = dotg(x[:, rows(n)], res[1], 0, 0)
        gw_copy(gwq_hbm, n).start()

    for k in range(NB // FB):
        z = dm_ref[FB * k:FB * (k + 1)].reshape(QW, D)
        z = jnp.dot(perm[...], z, preferred_element_type=F32)
        gm_ref[:, FB * k:FB * (k + 1), :] = z.astype(BF).reshape(FB, FB, D)

    @pl.when(step == pl.num_programs(0) - 1)
    def _():
        for k in range(JOBS):
            out_copy(y, y_hbm, y_sem, k).wait()
            out_copy(gh, gh_hbm, gh_sem, k).wait()
            gw_copy(gwq_hbm, k).wait()
        for k in (2, 3):
            piece_out(k).wait()


def finish(dm, res, h, dy, w_o, w_q, dw, gain, shift, b_o):
    hbm = pl.BlockSpec(memory_space=pl.ANY)
    vec = fixed(1)
    dma = pltpu.SemaphoreType.DMA
    mat, dj = VMEM((D, D), BF), dma((JOBS,))
    return pl.pallas_call(
        finish_kernel, grid=(FP // FB,), name="finish",
        out_shape=(SDS((F, NB, D), BF), SDS((TOK, D), BF), SDS((TOK, D), BF), SDS((D, D), F32), SDS((D, D), F32),
                   SDS((D, D), F32), SDS((D, D), F32), SDS((B8, D), F32)),
        in_specs=[pl.BlockSpec((NB, FB, D), lambda s: (0, s, 0))] + [hbm] * 6 + [vec] * 3,
        out_specs=(pl.BlockSpec((FB, NB, D), lambda s: (s, 0, 0)),) + (hbm,) * 6 + (pl.BlockSpec((B8, D), lambda s: (0, 0)),),
        scratch_shapes=[
            VMEM((QW, QW), BF), VMEM((B2, TOK, D), BF), mat, mat, mat, mat, mat, mat, mat, VMEM((JOBS, RC, D), F32),
            VMEM((B2, D, W), F32), dma((B8,)), dj, dj, dj, dma((B2,)), dma((B2,))],
        compiler_params=pltpu.CompilerParams(vmem_limit_bytes=50 << 20),
    )(dm, res, h, dy, w_o, w_q, dw, gain, shift, b_o)


def block_mask():
    return lax.broadcasted_iota(jnp.int32, (128, 256), 0) // T == lax.broadcasted_iota(jnp.int32, (128, 256), 1) // HEAD


def block_diag(x, mask):
    return jnp.where(mask, jnp.concatenate([x] * 4, axis=0), jnp.zeros((), BF))


def when(cond):
    if isinstance(cond, bool):
        return (lambda f: f()) if cond else (lambda f: None)
    return pl.when(cond)


CH = 64
NCH = D // 2 // CH


def attn_kernel(m_hbm, h_hbm, dy_hbm, wq_hbm, wo_hbm, wk_hbm, wv_hbm, gain, shift, bq, bv,
                res_hbm, dw_hbm, bias_hbm, dm_hbm, dkv_hbm,
                raw, perm, frames, q, do, wk, wv, kv, e_s, dp_s, mt, stats, coef, dkv, acc, bias, od, r1, keep, x2, r2, res, big1, big2,
                raw_sem, in_sem, dkv_sem, dm_sem, out_sem, st_send, st_recv, s1_send, s1_recv, s2_send, s2_recv,
                s3_send, s3_recv, s3s_send, s4_send, res_recv, e1_send, e1_recv, e2_send, e2_recv,
                e3_send, e3_recv, e3s_send, e4_send, acc_recv, b_send, b_recv, free_sib, free_xn):
    me = lax.axis_index("cp")
    cx, cc = me // 2, me % 2
    sib, xn = 2 * cx + 1 - cc, 2 * (1 - cx) + cc

    def remote(src, dst, ss, rs, dev):
        return pltpu.make_async_remote_copy(src_ref=src, dst_ref=dst, send_sem=ss, recv_sem=rs,
                                            device_id={"cp": dev}, device_id_type=MESH)

    def raw_copy(c):
        seqs = pl.ds(pl.multiple_of(B8 * (c // B4 % B4), B8), B8)
        return pltpu.make_async_copy(m_hbm.at[:, seqs, quarter(c)], raw.at[c % 2, 0:F], raw_sem.at[c % 2])

    def quarter(c):
        return pl.ds(pl.multiple_of(c % B4 * QW, QW), QW)

    def sort_frames(c):
        for n in range(NFC):
            x = raw[c % 2, FC * n:FC * (n + 1)].reshape(QW, QW)
            y = jnp.dot(perm[...], x, preferred_element_type=F32).astype(BF)
            for b in range(B8):
                frames[c // B4 % 2, FP * b + FC * n:FP * b + FC * (n + 1), quarter(c)] = y[FC * b:FC * (b + 1)]

    def dkv_copy(i):
        return pltpu.make_async_copy(dkv.at[i % 2], dkv_hbm.at[i // NP, i % NP], dkv_sem.at[i % 2])

    def stat_send(i):
        for k in range(1, B4):
            remote(stats.at[i % B4, me], stats.at[i % B4, me], st_send.at[i % B4], st_recv.at[i % B4], (me + k) % B4).start()

    def stat_wait(i):
        three = stats.at[i % B4, 0:3]
        for sem in (st_recv, st_send):
            pltpu.make_async_copy(three, three, sem.at[i % B4]).wait()

    def s1(b):
        return remote(od.at[b % 2, 1 - cc], r1.at[b % 4], s1_send.at[b % 4], s1_recv.at[b % 4], sib)

    def s2(b):
        return remote(x2.at[b % 4], r2.at[b % 8], s2_send.at[b % 8], s2_recv.at[b % 8], xn)

    def res_at(b, x):
        return res.at[cc, pl.ds(pl.multiple_of(64 * (b % NP) + T * x, T), T), pl.ds(pl.multiple_of(W * (b // NP), W), W)]

    def s3(b, x):
        return remote(res_at(b, x), res_at(b, x), s3_send.at[b % 8], s3_recv.at[b % 8], xn)

    def s3s(b):
        return remote(res_at(b, cx), res_at(b, cx), s3s_send.at[b % 4], res_recv, sib)

    def s4(b):
        return remote(res_at(b, 1 - cx), res_at(b, 1 - cx), s4_send.at[b % 4], res_recv, sib)

    def od_pre(b, inside):
        def on(k):
            return (b >= k) if inside else (b - k < STEPS)

        @when(on(8))
        def _():
            s4(b - 8).wait_send()

        @when(on(6))
        def _():
            s3(b - 6, 1 - cx).wait_recv()
            s4(b - 6).start()
            s3(b - 6, cx).wait_send()
            s3s(b - 6).wait_send()

        @when(on(4))
        def _():
            s2(b - 4).wait_recv()
            s2(b - 4).wait_send()
            res_at(b - 4, cx)[...] = (keep[b % B4] + r2[(b - 4) % B8]).astype(BF)

        @when(on(2))
        def _():
            s1(b - 2).wait_send()
            s1(b - 2).wait_recv()
            for ref, x in ((keep, cx), (x2, 1 - cx)):
                rows = pl.ds(pl.multiple_of(T * x, T), T)
                ref[(b - 2) % B4] = od[b % 2, cc, rows, :] + r1[(b - 2) % B4, rows, :]

    def od_post(b, inside):
        def on(k):
            return (b >= k) if inside else (b - k < STEPS)

        if inside:
            s1(b).start()

        @when(on(2))
        def _():
            s2(b - 2).start()

        @when(on(4))
        def _():
            s3(b - 4, cx).start()
            s3s(b - 4).start()

    own = pl.ds(pl.multiple_of(W * cc, W), W)
    other = pl.ds(pl.multiple_of(W * (1 - cc), W), W)

    def rows_of(x, n):
        return pl.ds(pl.multiple_of(x * (D // 2) + CH * n, CH), CH)

    def e1(g):
        return remote(acc.at[g, :, other], big1, e1_send.at[g], e1_recv.at[g], sib)

    def e2(g, n):
        return remote(acc.at[g, rows_of(1 - cx, n), own], big2.at[g, pl.ds(pl.multiple_of(CH * n, CH), CH)],
                      e2_send.at[g, n], e2_recv.at[g, n], xn)

    def e3(g, n, x):
        ref = acc.at[g, rows_of(x, n), own]
        return remote(ref, ref, e3_send.at[g, n], e3_recv.at[g, n], xn)

    def to_sib(g, n, x, sem):
        ref = acc.at[g, rows_of(x, n), own]
        return remote(ref, ref, sem.at[g, n], acc_recv.at[g], sib)

    def dw_copy(g):
        return pltpu.make_async_copy(acc.at[g], dw_hbm.at[g], out_sem.at[g])

    def exchange(g, t, t3, t4):
        @when(t == 0)
        def _():
            e1(g).start()

        @when(t == 1)
        def _():
            e1(g).wait_send()
            pl.semaphore_signal(free_sib.at[g], inc=1, device_id={"cp": sib}, device_id_type=MESH)
            e1(g).wait_recv()

        @when(t == t3)
        def _():
            pl.semaphore_wait(free_sib.at[g], 1)

        def chunk(t0, f):
            n = t - t0
            if isinstance(n, int):
                if 0 <= n < NCH:
                    f(n)
            else:
                pl.when((n >= 0) & (n < NCH))(lambda: f(n))

        def reduce_core(n):
            for x in (cx, 1 - cx):
                acc[g, rows_of(x, n), own] += big1[rows_of(x, n), :]
            e2(g, n).start()

        def sent(n):
            e2(g, n).wait_send()
            pl.semaphore_signal(free_xn.at[g], inc=1, device_id={"cp": xn}, device_id_type=MESH)

        def reduce_chip(n):
            e2(g, n).wait_recv()
            pl.semaphore_wait(free_xn.at[g], 1)
            acc[g, rows_of(cx, n), own] += big2[g, pl.ds(pl.multiple_of(CH * n, CH), CH), :]
            e3(g, n, cx).start()
            to_sib(g, n, cx, e3s_send).start()

        def forward(n):
            e3(g, n, 1 - cx).wait_recv()
            to_sib(g, n, 1 - cx, e4_send).start()

        chunk(1, reduce_core)
        chunk(t3 - 1, sent)
        chunk(t3, reduce_chip)
        chunk(t4, forward)

        @when(t == t4 + NCH + 1)
        def _():
            remote(acc.at[g, :, other], acc.at[g, :, other], e1_send.at[g], acc_recv.at[g], sib).wait_recv()
            for n in range(NCH):
                e3(g, n, cx).wait_send()
                to_sib(g, n, cx, e3s_send).wait_send()
                to_sib(g, n, 1 - cx, e4_send).wait_send()
            dw_copy(g).start()

    def operands(i, j, h):
        cols = pl.ds(pl.multiple_of(W * (i // NP) + 256 * h, 256), 256)
        rows = pl.ds(pl.multiple_of(64 * (i % NP) + T * j, T), T)
        mask = block_mask()
        return block_diag(q[rows, cols], mask), block_diag(do[rows, cols], mask), mask

    def stage_a(i):
        slot = i % 2
        m = frames[i // B4 % 2, pl.ds(pl.multiple_of(i % B4 * ROWS, ROWS), ROWS), :]
        cols = pl.ds(pl.multiple_of(W * (i // NP), W), W)
        mt[i % 3] = m.T
        kv[slot, :, 0:W] = jnp.dot(m, wk[:, cols], preferred_element_type=F32).astype(BF)
        kv[slot, :, W:] = (jnp.dot(m, wv[:, cols], preferred_element_type=F32) + bv[:, cols]).astype(BF)
        real = lax.broadcasted_iota(jnp.int32, (FP, LANES), 0) < F
        for j in range(2):
            rows = slice(FP * j, FP * (j + 1))
            for h in range(2):
                n = 2 * j + h
                qb, db, _ = operands(i, j, h)
                s = dotg(kv[slot, rows, QW * h:QW * (h + 1)], qb, 1, 1)
                dp = dotg(kv[slot, rows, W + QW * h:W + QW * (h + 1)], db, 1, 1)
                s = jnp.where(real, s, -1e30)
                top = jnp.max(s, axis=0, keepdims=True)
                e = jnp.exp2((s - top) * LOG2)
                e_s[slot, n] = e
                dp_s[slot, n] = dp
                for k, row in enumerate((top, jnp.sum(e, axis=0, keepdims=True), jnp.sum(e * dp, axis=0, keepdims=True))):
                    stats[i % B4, me, B4 * k + n:B4 * k + n + 1, :] = row

    def combine(i):
        slot = i % 4
        tops = [stats[slot, d, 0:4, :] for d in range(4)]
        top = jnp.maximum(jnp.maximum(tops[0], tops[1]), jnp.maximum(tops[2], tops[3]))
        ws = [jnp.exp2((t - top) * LOG2) for t in tops]
        total = sum(stats[slot, d, 4:8, :] * ws[d] for d in range(4))
        dots = sum(stats[slot, d, 8:12, :] * ws[d] for d in range(4))
        coef[0:4, :] = jnp.exp2((stats[slot, me, 0:4, :] - top) * LOG2) / total
        coef[4:8, :] = dots / total

    def stage_b(i):
        slot = i % 2
        grp = i // NP
        for j in range(2):
            rows = slice(FP * j, FP * (j + 1))
            for h in range(2):
                n = 2 * j + h
                qb, db, mask = operands(i, j, h)
                ck, cv = slice(256 * h, 256 * (h + 1)), slice(W + 256 * h, W + 256 * (h + 1))
                p = e_s[slot, n] * coef[n:n + 1, :]
                pb = p.astype(BF)
                gb = (p * (dp_s[slot, n] - coef[4 + n:5 + n, :]) * 0.125).astype(BF)
                o = dotg(pb, kv[slot, rows, cv], 0, 0)
                dq = dotg(gb, kv[slot, rows, ck], 0, 0)
                for which, x in ((0, o), (1, dq)):
                    x = jnp.where(mask, x, 0.0)
                    x = (x[0:32] + x[32:64]) + (x[64:96] + x[96:128])
                    od[slot, which, T * j:T * (j + 1), ck] = x
                    if which == 1:
                        bias[me, pl.ds(grp, 1), ck] += jnp.sum(x, axis=0, keepdims=True)
                dk = jnp.dot(gb, qb, preferred_element_type=F32)
                dv = jnp.dot(pb, db, preferred_element_type=F32)
                dkv[slot, rows, ck] = dk.astype(BF)
                dkv[slot, rows, cv] = dv.astype(BF)
                bias[me, pl.ds(grp, 1), cv] += jnp.sum(dv, axis=0, keepdims=True)

    def step(i, do_a, do_b):
        b = i - 2
        if do_b:
            @pl.when(b >= NP)
            def _():
                exchange(0, b - NP, 9, 12)

            stat_wait(b)

            @pl.when(b >= 2)
            def _():
                dkv_copy(b - 2).wait()

            od_pre(b, True)
        if do_a:
            @pl.when(i + B4 < STEPS)
            def _():
                raw_copy(i + B4).wait()

            @pl.when(i + B4 + 1 < STEPS)
            def _():
                raw_copy(i + B4 + 1).start()

        if do_b:
            combine(b)
            stage_b(b)
        if do_a:
            stage_a(i)
            sort_frames(i + B4)
        if do_b:
            acc[b // NP] += jnp.dot(mt[b % 3], dkv[b % 2], preferred_element_type=F32)
        if do_a:
            stat_send(i)
        if do_b:
            dkv_copy(b).start()
            od_post(b, True)

    barrier = pltpu.get_barrier_semaphore()
    for k in range(1, B4):
        pl.semaphore_signal(barrier, inc=1, device_id={"cp": (me + k) % B4}, device_id_type=MESH)
    top, low = pl.ds(0, ROWS), pl.ds(ROWS, D - ROWS)
    rest = pl.ds(0, D - ROWS)
    loads = [pltpu.make_async_copy(x, y, in_sem.at[k]) for k, (x, y) in enumerate((
        (h_hbm, res.at[0]), (wq_hbm.at[top], kv.at[0]), (wq_hbm.at[low], dkv.at[0, rest]), (dy_hbm, res.at[1]),
        (wo_hbm.at[top], kv.at[1]), (wo_hbm.at[low], dkv.at[1, rest]), (wk_hbm, wk), (wv_hbm, wv)))]
    raw_copy(0).start()
    for cp in loads:
        cp.start()
    raw[:, F:] = jnp.zeros((B2, FP - F, B8, QW), BF)
    perm[...] = permutation(FC)
    bias[me] = jnp.zeros((B8, D), F32)
    for cp in loads[:-2]:
        cp.wait()

    def first(n, carry):
        raw_copy(n).wait()
        raw_copy(n + 1).start()
        rows = pl.ds(pl.multiple_of(RC * n, RC), RC)
        x_hat, _ = norm_parts(res[0, rows].astype(F32))
        x = (x_hat * gain[...] + shift[...]).astype(BF)
        q[rows] = (jnp.dot(x[:, :ROWS], kv[0], preferred_element_type=F32)
                   + jnp.dot(x[:, ROWS:], dkv[0, rest], preferred_element_type=F32) + bq[...]).astype(BF)
        do[rows, :ROWS] = dotg(res[1, rows], kv[1], 1, 1).astype(BF)
        do[rows, ROWS:] = dotg(res[1, rows], dkv[1, rest], 1, 1).astype(BF)
        sort_frames(n)
        for g in range(2):
            acc[g, rows] = jnp.zeros((RC, D), F32)
        return carry

    lax.fori_loop(0, TOK // RC, first, 0)
    for cp in loads[-2:]:
        cp.wait()
    pl.semaphore_wait(barrier, 3)

    def run(lo, hi, do_a, do_b):
        def body(i, carry):
            step(i, do_a, do_b)
            return carry
        lax.fori_loop(lo, hi, body, 0)

    run(0, 2, True, False)
    run(2, STEPS, True, True)
    run(STEPS, STEPS + 2, False, True)

    def b_copy(k, src):
        return remote(bias.at[src], bias.at[src], b_send.at[k - 1], b_recv.at[src], (me + k) % 4)

    for k in range(1, 4):
        b_copy(k, me).start()
    dkv_copy(STEPS - 2).wait()
    dkv_copy(STEPS - 1).wait()

    bufs = (kv, dkv)

    def c_load(c, s):
        return [pltpu.make_async_copy(dkv_hbm.at[g, c], bufs[s].at[g], raw_sem.at[g] if s == 0 else dkv_sem.at[g]) for g in range(2)]

    def dm_copy(c, s):
        return pltpu.make_async_copy(frames.at[0, pl.ds(ROWS * s, ROWS)], dm_hbm.at[c], dm_sem.at[s])

    for cp in c_load(0, 0):
        cp.start()

    def c_step(u, carry):
        for s in range(2):
            c = 2 * u + s
            for cp in c_load(c, s):
                cp.wait()

            @pl.when(c + 1 < NP)
            def _():
                for cp in c_load(c + 1, 1 - s):
                    cp.start()

            @pl.when(c >= 2)
            def _():
                dm_copy(c - 2, s).wait()

            exchange(0, c + NP, 9, 12)
            exchange(1, c, 6, 10)

            @pl.when(c < B8)
            def _():
                od_pre(c + STEPS, False)

            x = jnp.concatenate([bufs[s][0], bufs[s][1]], axis=1)
            w = jnp.concatenate([wk[:, :W], wv[:, :W], wk[:, W:], wv[:, W:]], axis=1)
            frames[0, pl.ds(ROWS * s, ROWS)] = dotg(x, w, 1, 1).astype(BF)
            dm_copy(c, s).start()

            @pl.when(c < B8)
            def _():
                od_post(c + STEPS, False)

            @pl.when(c == 9)
            def _():
                pltpu.make_async_copy(res.at[0], res.at[0], res_recv).wait()
                pltpu.make_async_copy(res, res_hbm, out_sem.at[2]).start()
        return carry

    lax.fori_loop(0, NP // 2, c_step, 0)
    for t in range(NP, 10 + NCH + 2):
        exchange(1, t, 6, 10)
    for k in range(1, 4):
        b_copy(k, (me + k) % 4).wait_recv()
        b_copy(k, me).wait_send()
    big1[0:8, :] = (bias[0, :, 0:W] + bias[1, :, 0:W]) + (bias[2, :, 0:W] + bias[3, :, 0:W])
    big1[8:16, :] = (bias[0, :, W:] + bias[1, :, W:]) + (bias[2, :, W:] + bias[3, :, W:])
    bias_out = pltpu.make_async_copy(big1.at[0:16], bias_hbm, out_sem.at[3])
    bias_out.start()
    dm_copy(NP - 2, 0).wait()
    dm_copy(NP - 1, 1).wait()
    dw_copy(0).wait()
    dw_copy(1).wait()
    pltpu.make_async_copy(res, res_hbm, out_sem.at[2]).wait()
    bias_out.wait()


def attention(mt, h, dy, w_q, w_o, w_k, w_v, gain, shift, b_q, b_v):
    vm = pl.BlockSpec(memory_space=VMEM)
    hbm = pl.BlockSpec(memory_space=pl.ANY)
    dma = pltpu.SemaphoreType.DMA
    d2, d4, d8, dn = dma((B2,)), dma((B4,)), dma((B8,)), dma((B2, NCH))
    credit = pltpu.SemaphoreType.REGULAR((B2,))
    probs, mat, rows32 = VMEM((B2, B4, FP, LANES), F32), VMEM((D, D), BF), VMEM((B4, T, W), F32)
    return pl.pallas_call(
        attn_kernel, name="attention",
        out_shape=(SDS((B2, TOK, D), BF), SDS((B2, D, D), F32), SDS((2 * B8, W), F32), SDS((NP, ROWS, D), BF),
                   SDS((B2, NP, ROWS, D), BF)),
        in_specs=[hbm] * 7 + [vm] * B4,
        out_specs=(hbm,) * 5,
        scratch_shapes=[
            VMEM((B2, FP, B8, QW), BF), VMEM((QW, QW), BF), VMEM((B2, B8 * FP, D), BF), mat, mat, mat, mat,
            VMEM((B2, ROWS, D), BF), probs, probs, VMEM((3, D, ROWS), BF), VMEM((B4, B4, 2 * B8, LANES), F32),
            VMEM((B8, LANES), F32), VMEM((B2, ROWS, D), BF), VMEM((B2, D, D), F32), VMEM((B4, B8, D), F32),
            VMEM((B2, B2, 2 * T, W), F32), VMEM((B4, 2 * T, W), F32), rows32, rows32, VMEM((B8, T, W), F32),
            VMEM((B2, TOK, D), BF), VMEM((D, W), F32), VMEM((B2, D // 2, W), F32),
            d2, d8, d2, d2, d4, d4, d4, d4, d4, d8, d8, d8, d8, d4, d4, dma, d2, d2, dn, dn, dn, dn, dn, dn, d2, d4, d4,
            credit, credit],
        compiler_params=pltpu.CompilerParams(vmem_limit_bytes=67043328, collective_id=0, has_side_effects=True),
    )(mt, h, dy, w_q, w_o, w_k, w_v, gain, shift, b_q, b_v)


def solution(mesh):
    act_spec = P("dp", None, None)
    mem_spec = P("dp", "cp", None)
    vec_out = P("dp")
    mat_out = P("dp", None)
    in_specs = (act_spec, mem_spec, P(), P(), P(), P(), P(), P(), P(), P(), P(), act_spec)
    out_specs = (act_spec, act_spec, mem_spec, vec_out, vec_out, mat_out, vec_out, mat_out, mat_out, vec_out, mat_out, vec_out)

    def device_step(hidden, memory, ln_gain, ln_bias, w_q, b_q, w_k, w_v, b_v, w_o, b_o, grad_y):
        h = hidden.reshape(TOK, D)
        dy = grad_y.reshape(TOK, D)
        gain, shift, bq, bv, bo = (a.astype(F32).reshape(1, D) for a in (ln_gain, ln_bias, b_q, b_v, b_o))
        res, dw, bias, dm, _ = attention(memory.transpose(1, 0, 2), h, dy, w_q, w_o, w_k, w_v, gain, shift, bq, bv)
        gm, y, gh, gwo, gwq, gwk, gwv, vec = finish(dm.reshape(NB, FP, D), res, h, dy, w_o, w_q, dw, gain, shift, bo)
        grad_bq = bias[0:2].reshape(D)
        grad_bv = bias[8:10].reshape(D)
        return (y.reshape(NB, T, D), gh.reshape(NB, T, D), gm.transpose(1, 0, 2), vec[0], vec[1], gwq, grad_bq,
                gwk, gwv, grad_bv, gwo, vec[2])

    return jax.shard_map(device_step, mesh=mesh, in_specs=in_specs, out_specs=out_specs, check_vma=False)
```

```python
import functools
import math
import jax
import jax.numpy as jnp
from jax import lax
from jax.experimental import pallas as pl
from jax.experimental.pallas import tpu as pltpu
from jax.sharding import PartitionSpec as P

EPS = 1e-5
HEAD = 64
F, FP, D, T = 375, 384, 1024, 32
NB = 32
NP = NB // 2
STEPS = 2 * NP
W = 512
ROWS = 2 * FP
QW = 256
BF, F32 = jnp.bfloat16, jnp.float32
LOG2 = 0.125 * math.log2(math.e)
MESH = pl.DeviceIdType.MESH
VMEM = pltpu.VMEM
B2, B4, B8, LANES = 2, 4, 8, 128
RC = 256
TOK = NB * T
SDS = jax.ShapeDtypeStruct


def dotg(a, b, ca, cb):
    return lax.dot_general(a, b, (((ca,), (cb,)), ((), ())), preferred_element_type=F32)


FC = 32
NFC = FP // FC


def fixed(rows):
    return pl.BlockSpec((rows, D), lambda s: (0, 0), pipeline_mode=pl.Buffered(1))


def lanes(t):
    return slice(LANES * t, LANES * (t + 1))


def permutation(n):
    r = lax.broadcasted_iota(jnp.int32, (QW, QW), 0)
    k = lax.broadcasted_iota(jnp.int32, (QW, QW), 1)
    return (k == r % n * (QW // n) + r // n).astype(F32).astype(BF)


def norm_parts(h):
    centered = h - jnp.mean(h, axis=-1, keepdims=True)
    inv_std = lax.rsqrt(jnp.mean(centered * centered, axis=-1, keepdims=True) + EPS)
    return centered * inv_std, inv_std


JOB0, JOBS = 2, 4
FB = 16
NFB = FP // FB


def finish_kernel(dm_hbm, res_hbm, h_hbm, dy_hbm, wo_hbm, wq_hbm, dw_hbm, bias, gain, shift, bo,
                  gm_hbm, y_hbm, gh_hbm, gwo_hbm, gwq_hbm, gwk_hbm, gwv_hbm, dg, db, dbq, dbv, dbo,
                  src, dst, perm, res, h, dy, wo, wq, x, y, gh, gw, stage, sums,
                  src_sem, dst_sem, in_sem, y_sem, gh_sem, gw_sem, ld_sem, st_sem):
    loads = [pltpu.make_async_copy(a, b, in_sem.at[k]) for k, (a, b) in enumerate(
        ((h_hbm, h), (res_hbm, res), (wo_hbm, wo), (dy_hbm, dy), (wq_hbm, wq)))]

    def src_copy(s):
        return pltpu.make_async_copy(dm_hbm.at[:, pl.ds(pl.multiple_of(FB * s, FB), FB)], src.at[s % B4], src_sem.at[s % B4])

    def dst_copy(s):
        return pltpu.make_async_copy(dst.at[s % B4], gm_hbm.at[pl.ds(FB * s, FB)], dst_sem.at[s % B4])

    def last_copy():
        s = NFB - 1
        return pltpu.make_async_copy(dst.at[s % B4, 0:F - FB * s], gm_hbm.at[FB * s:F], dst_sem.at[s % B4])

    def rows(n):
        return pl.ds(pl.multiple_of(RC * n, RC), RC)

    def out_copy(a, b, sem, n):
        return pltpu.make_async_copy(a.at[rows(n)], b.at[rows(n)], sem.at[n])

    def gw_copy(b, n):
        return pltpu.make_async_copy(gw.at[n], b.at[rows(n)], gw_sem.at[n])

    def piece_in(k):
        g, v = k // 2, k % 2
        return pltpu.make_async_copy(dw_hbm.at[g, :, pl.ds(W * v, W)], stage.at[v], ld_sem.at[v])

    def piece_out(k):
        g, v = k // 2, k % 2
        return pltpu.make_async_copy(stage.at[v], (gwk_hbm, gwv_hbm)[v].at[:, pl.ds(W * g, W)], st_sem.at[v])

    def vec(ref):
        return ref[...].astype(F32).reshape(1, D)

    def move(s):
        for k in range(NB // FB):
            z = src[s % B4, FB * k:FB * (k + 1)].reshape(QW, D)
            z = jnp.dot(perm[...], z, preferred_element_type=F32)
            dst[s % B4, :, FB * k:FB * (k + 1), :] = z.astype(BF).reshape(FB, FB, D)

    def job_y(n):
        hf = h[rows(n)].astype(F32)
        x_hat, _ = norm_parts(hf)
        x[rows(n)] = (x_hat * vec(gain) + vec(shift)).astype(BF)
        y[rows(n)] = (hf + jnp.dot(res[0, rows(n)], wo[...], preferred_element_type=F32) + vec(bo)).astype(BF)

    def job_wo(n):
        gw[n] = dotg(res[0, :, rows(n)], dy[...], 0, 0)

    def job_h(n):
        x_hat, inv_std = norm_parts(h[rows(n)].astype(F32))
        dyf = dy[rows(n)].astype(F32)
        d_x = dotg(res[1, rows(n)], wq[...], 1, 1)
        for k, a in enumerate((d_x * x_hat, d_x, dyf)):
            sums[k:k + 1] += jnp.sum(a, axis=0, keepdims=True)
        d_hat = d_x * vec(gain)
        d_h = inv_std * (d_hat - jnp.mean(d_hat, axis=-1, keepdims=True) - x_hat * jnp.mean(d_hat * x_hat, axis=-1, keepdims=True))
        gh[rows(n)] = (dyf + d_h).astype(BF)

    def job_wq(n):
        gw[n] = dotg(x[:, rows(n)], res[1], 0, 0)

    for k in range(B4 - 1):
        src_copy(k).start()
    for cp in loads:
        cp.start()
    piece_in(0).start()
    piece_in(1).start()
    sums[...] = jnp.zeros_like(sums)
    perm[...] = permutation(FB)
    for ref, k in ((dbq, 0), (dbv, B8)):
        ref[...] = jnp.concatenate([bias[k:k + 1], bias[k + 1:k + 2]], axis=1).reshape(D)
    outs = ((job_y, lambda n: out_copy(y, y_hbm, y_sem, n)), (job_wo, lambda n: gw_copy(gwo_hbm, n)),
            (job_h, lambda n: out_copy(gh, gh_hbm, gh_sem, n)), (job_wq, lambda n: gw_copy(gwq_hbm, n)))
    needs = (loads[:3], loads[3:4], loads[4:], ())

    def step(s, carry):
        src_copy(s).wait()

        @pl.when(s + B4 - 1 < NFB)
        def _():
            src_copy(s + B4 - 1).start()

        @pl.when(s >= B4)
        def _():
            dst_copy(s - B4).wait()

        job = s - JOB0
        n = job % JOBS
        for kind, (f, copy) in enumerate(outs):
            @pl.when((job >= kind * JOBS) & (job < (kind + 1) * JOBS))
            def _():
                if needs[kind]:
                    @pl.when(n == 0)
                    def _():
                        for cp in needs[kind]:
                            cp.wait()
                if kind == 3:
                    gw_copy(gwo_hbm, n).wait()
                move(s)
                f(n)
                copy(n).start()

        @pl.when((job < 0) | (job >= JOBS * JOBS))
        def _():
            move(s)

        @pl.when(s < NFB - 1)
        def _():
            dst_copy(s).start()

        for v in range(2):
            @pl.when(s == JOBS + v)
            def _():
                piece_in(v).wait()
                piece_out(v).start()

            @pl.when(s == B8 + v)
            def _():
                piece_out(v).wait()
                piece_in(v + 2).start()

            @pl.when(s == B8 + JOBS + v)
            def _():
                piece_in(v + 2).wait()
                piece_out(v + 2).start()
        return carry

    lax.fori_loop(0, NFB, step, 0)
    last_copy().start()
    for k, ref in enumerate((dg, db, dbo)):
        ref[...] = sums[k:k + 1].reshape(D)
    for k in range(JOBS):
        out_copy(y, y_hbm, y_sem, k).wait()
        out_copy(gh, gh_hbm, gh_sem, k).wait()
        gw_copy(gwq_hbm, k).wait()
    piece_out(2).wait()
    piece_out(3).wait()
    for k in range(2, JOBS + 1):
        dst_copy(NFB - k).wait()
    last_copy().wait()


def finish(dm, res, h, dy, w_o, w_q, dw, bias, gain, shift, b_o):
    hbm, vm = pl.BlockSpec(memory_space=pl.ANY), pl.BlockSpec(memory_space=VMEM)
    dma = pltpu.SemaphoreType.DMA
    mat, dj, d2, vec = VMEM((D, D), BF), dma((JOBS,)), dma((B2,)), SDS((D,), F32)
    return pl.pallas_call(
        finish_kernel, name="finish",
        out_shape=(SDS((F, NB, D), BF), SDS((TOK, D), BF), SDS((TOK, D), BF)) + (SDS((D, D), F32),) * B4 + (vec,) * (B4 + 1),
        in_specs=[hbm] * (B8 - 1) + [vm] * B4,
        out_specs=(hbm,) * (B8 - 1) + (vm,) * (B4 + 1),
        scratch_shapes=[
            VMEM((B4, NB, FB, D), BF), VMEM((B4, FB, NB, D), BF), VMEM((QW, QW), BF), VMEM((B2, TOK, D), BF), mat, mat, mat, mat, mat,
            mat, mat, VMEM((JOBS, RC, D), F32), VMEM((B2, D, W), F32), VMEM((B8, D), F32), dj, dj, dma((B8,)), dj, dj, dj, d2, d2],
        compiler_params=pltpu.CompilerParams(vmem_limit_bytes=50 << 20),
    )(dm, res, h, dy, w_o, w_q, dw, bias, gain, shift, b_o)


def block_mask():
    return lax.broadcasted_iota(jnp.int32, (128, 256), 0) // T == lax.broadcasted_iota(jnp.int32, (128, 256), 1) // HEAD


def block_diag(x, mask):
    return jnp.where(mask, jnp.concatenate([x] * 4, axis=0), jnp.zeros((), BF))


def when(cond):
    if isinstance(cond, bool):
        return (lambda f: f()) if cond else (lambda f: None)
    return pl.when(cond)


CH = (64, 128)
NCH = tuple(D // 2 // rows for rows in CH)
T3, T4 = (8, 4), (11, 6)


def attn_kernel(m_hbm, h_hbm, dy_hbm, wq_hbm, wo_hbm, wk_hbm, wv_hbm, gain, shift, bq, bv,
                res_hbm, dw_hbm, bias_hbm, dm_hbm, dkv_hbm,
                raw, perm, bv32, frames, q, do, wk, wv, kv, e_s, dp_s, mt, stats, coef, dkv, acc, bias, od, r1, keep, x2, r2, res, big1, big2,
                raw_sem, in_sem, dkv_sem, dm_sem, out_sem, st_send, st_recv, s1_send, s1_recv, s2_send, s2_recv,
                s3_send, s3_recv, s3s_send, s4_send, res_recv, e1_send, e1_recv, e2_send, e2_recv,
                e3_send, e3_recv, e3s_send, e4_send, acc_recv, b_send, b_recv, free_sib, free_xn):
    me = lax.axis_index("cp")
    cx, cc = me // 2, me % 2
    sib, xn = 2 * cx + 1 - cc, 2 * (1 - cx) + cc

    def vec(ref):
        return ref[...].astype(F32).reshape(1, D)

    def remote(src, dst, ss, rs, dev):
        return pltpu.make_async_remote_copy(src_ref=src, dst_ref=dst, send_sem=ss, recv_sem=rs,
                                            device_id={"cp": dev}, device_id_type=MESH)

    def raw_copy(c):
        seqs = pl.ds(pl.multiple_of(B8 * (c // B4 % B4), B8), B8)
        return pltpu.make_async_copy(m_hbm.at[:, seqs, quarter(c)], raw.at[c % 2, 0:F], raw_sem.at[c % 2])

    def quarter(c):
        return pl.ds(pl.multiple_of(c % B4 * QW, QW), QW)

    def sort_frames(c):
        for n in range(NFC):
            x = raw[c % 2, FC * n:FC * (n + 1)].reshape(QW, QW)
            y = jnp.dot(perm[...], x, preferred_element_type=F32).astype(BF)
            for b in range(B8):
                frames[c // B4 % 2, FP * b + FC * n:FP * b + FC * (n + 1), quarter(c)] = y[FC * b:FC * (b + 1)]

    def dkv_copy(i):
        return pltpu.make_async_copy(dkv.at[i % 2], dkv_hbm.at[i // NP, i % NP], dkv_sem.at[i % 2])

    def stat_send(i):
        for k in range(1, B4):
            remote(stats.at[i % B4, me], stats.at[i % B4, me], st_send.at[i % B4], st_recv.at[i % B4], (me + k) % B4).start()

    def stat_wait(i):
        three = stats.at[i % B4, 0:3]
        for sem in (st_recv, st_send):
            pltpu.make_async_copy(three, three, sem.at[i % B4]).wait()

    def s1(b):
        return remote(od.at[b % 2, 1 - cc], r1.at[b % 4], s1_send.at[b % 4], s1_recv.at[b % 4], sib)

    def s2(b):
        return remote(x2.at[b % 4], r2.at[b % 8], s2_send.at[b % 8], s2_recv.at[b % 8], xn)

    def res_at(b, x):
        return res.at[cc, pl.ds(pl.multiple_of(64 * (b % NP) + T * x, T), T), pl.ds(pl.multiple_of(W * (b // NP), W), W)]

    def s3(b, x):
        return remote(res_at(b, x), res_at(b, x), s3_send, s3_recv.at[b % (2 * B8)], xn)

    def s3s(b):
        return remote(res_at(b, cx), res_at(b, cx), s3s_send, res_recv, sib)

    def s4(b):
        return remote(res_at(b, 1 - cx), res_at(b, 1 - cx), s4_send, res_recv, sib)

    def od_pre(b, inside):
        def on(k):
            return (b >= k) if inside else (b - k < STEPS)

        @when(on(8))
        def _():
            s3(b - 8, 1 - cx).wait_recv()
            s4(b - 8).start()

        @when(on(5))
        def _():
            s2(b - 5).wait_recv()
            s2(b - 5).wait_send()
            res_at(b - 5, cx)[...] = (keep[(b - 5) % B4] + r2[(b - 5) % B8]).astype(BF)

        @when(on(2))
        def _():
            s1(b - 2).wait_send()
            s1(b - 2).wait_recv()
            for ref, x in ((keep, cx), (x2, 1 - cx)):
                rows = pl.ds(pl.multiple_of(T * x, T), T)
                ref[(b - 2) % B4] = od[b % 2, cc, rows, :] + r1[(b - 2) % B4, rows, :]

    def od_post(b, inside):
        def on(k):
            return (b >= k) if inside else (b - k < STEPS)

        if inside:
            s1(b).start()

        @when(on(2))
        def _():
            s2(b - 2).start()

        @when(on(5))
        def _():
            s3(b - 5, cx).start()
            s3s(b - 5).start()

    own = pl.ds(pl.multiple_of(W * cc, W), W)
    other = pl.ds(pl.multiple_of(W * (1 - cc), W), W)

    def rows_of(g, x, n):
        return pl.ds(pl.multiple_of(x * (D // 2) + CH[g] * n, CH[g]), CH[g])

    def chunk_of(g, n):
        return big2.at[g, pl.ds(pl.multiple_of(CH[g] * n, CH[g]), CH[g])]

    def e1(g):
        return remote(acc.at[g, :, other], big1, e1_send.at[g], e1_recv.at[g], sib)

    def e2(g, n):
        return remote(acc.at[g, rows_of(g, 1 - cx, n), own], chunk_of(g, n), e2_send.at[g, n], e2_recv.at[g, n], xn)

    def e3(g, n, x):
        ref = acc.at[g, rows_of(g, x, n), own]
        return remote(ref, ref, e3_send.at[g, n], e3_recv.at[g, n], xn)

    def to_sib(g, n, x, sem):
        ref = acc.at[g, rows_of(g, x, n), own]
        return remote(ref, ref, sem.at[g, n], acc_recv.at[g], sib)

    def dw_copy(g):
        return pltpu.make_async_copy(acc.at[g], dw_hbm.at[g], out_sem.at[g])

    def reduce_core(g, n):
        for x in (cx, 1 - cx):
            acc[g, rows_of(g, x, n), own] += big1[rows_of(g, x, n), :]
        e2(g, n).start()

    def sent(g, n):
        e2(g, n).wait_send()
        pl.semaphore_signal(free_xn.at[g], inc=1, device_id={"cp": xn}, device_id_type=MESH)

    def reduce_chip(g, n):
        e2(g, n).wait_recv()
        pl.semaphore_wait(free_xn.at[g], 1)
        acc[g, rows_of(g, cx, n), own] += chunk_of(g, n)[...]
        e3(g, n, cx).start()
        to_sib(g, n, cx, e3s_send).start()

    def forward(g, n):
        e3(g, n, 1 - cx).wait_recv()
        to_sib(g, n, 1 - cx, e4_send).start()

    def gathered(g):
        half = acc.at[g, :, other]
        remote(half, half, e1_send.at[g], acc_recv.at[g], sib).wait_recv()
        for n in range(NCH[g]):
            e3(g, n, cx).wait_send()
            to_sib(g, n, cx, e3s_send).wait_send()
            to_sib(g, n, 1 - cx, e4_send).wait_send()
        dw_copy(g).start()

    def exchange(g, t, t3, t4):
        def chunk(t0, f):
            n = t - t0
            if isinstance(n, int):
                if 0 <= n < NCH[g]:
                    f(g, n)
            else:
                pl.when((n >= 0) & (n < NCH[g]))(lambda: f(g, n))

        @when(t == 0)
        def _():
            e1(g).start()

        @when(t == 1)
        def _():
            e1(g).wait_send()
            pl.semaphore_signal(free_sib.at[g], inc=1, device_id={"cp": sib}, device_id_type=MESH)
            e1(g).wait_recv()

        @when(t == t3)
        def _():
            pl.semaphore_wait(free_sib.at[g], 1)

        chunk(1, reduce_core)
        chunk(t3 - 1, sent)
        chunk(t3, reduce_chip)
        chunk(t4, forward)

    def operands(i, j, h):
        cols = pl.ds(pl.multiple_of(W * (i // NP) + 256 * h, 256), 256)
        rows = pl.ds(pl.multiple_of(64 * (i % NP) + T * j, T), T)
        mask = block_mask()
        return block_diag(q[rows, cols], mask), block_diag(do[rows, cols], mask), mask

    def stage_a(i):
        slot = i % 2
        m = frames[i // B4 % 2, pl.ds(pl.multiple_of(i % B4 * ROWS, ROWS), ROWS), :]
        cols = pl.ds(pl.multiple_of(W * (i // NP), W), W)
        mt[i % 3] = m.T
        kv[slot, :, 0:W] = jnp.dot(m, wk[:, cols], preferred_element_type=F32).astype(BF)
        kv[slot, :, W:] = (jnp.dot(m, wv[:, cols], preferred_element_type=F32) + bv32[:, cols]).astype(BF)
        real = lax.broadcasted_iota(jnp.int32, (FP, LANES), 0) < F
        for j in range(2):
            rows = slice(FP * j, FP * (j + 1))
            for h in range(2):
                n = 2 * j + h
                qb, db, _ = operands(i, j, h)
                s = dotg(kv[slot, rows, QW * h:QW * (h + 1)], qb, 1, 1)
                dp = dotg(kv[slot, rows, W + QW * h:W + QW * (h + 1)], db, 1, 1)
                s = jnp.where(real, s, -1e30)
                top = jnp.max(s, axis=0, keepdims=True)
                e = jnp.exp2((s - top) * LOG2)
                e_s[slot, n] = e
                dp_s[slot, n] = dp
                for k, row in enumerate((top, jnp.sum(e, axis=0, keepdims=True), jnp.sum(e * dp, axis=0, keepdims=True))):
                    stats[i % B4, me, B4 * k + n:B4 * k + n + 1, :] = row

    def combine(i):
        slot = i % 4
        tops = [stats[slot, d, 0:4, :] for d in range(4)]
        top = jnp.maximum(jnp.maximum(tops[0], tops[1]), jnp.maximum(tops[2], tops[3]))
        ws = [jnp.exp2((t - top) * LOG2) for t in tops]
        total = sum(stats[slot, d, 4:8, :] * ws[d] for d in range(4))
        dots = sum(stats[slot, d, 8:12, :] * ws[d] for d in range(4))
        coef[0:4, :] = jnp.exp2((stats[slot, me, 0:4, :] - top) * LOG2) / total
        coef[4:8, :] = dots / total

    def stage_b(i):
        slot = i % 2
        grp = i // NP
        for j in range(2):
            rows = slice(FP * j, FP * (j + 1))
            for h in range(2):
                n = 2 * j + h
                qb, db, mask = operands(i, j, h)
                ck, cv = slice(256 * h, 256 * (h + 1)), slice(W + 256 * h, W + 256 * (h + 1))
                p = e_s[slot, n] * coef[n:n + 1, :]
                pb = p.astype(BF)
                gb = (p * (dp_s[slot, n] - coef[4 + n:5 + n, :]) * 0.125).astype(BF)
                o = dotg(pb, kv[slot, rows, cv], 0, 0)
                dq = dotg(gb, kv[slot, rows, ck], 0, 0)
                for which, x in ((0, o), (1, dq)):
                    x = jnp.where(mask, x, 0.0)
                    x = (x[0:32] + x[32:64]) + (x[64:96] + x[96:128])
                    od[slot, which, T * j:T * (j + 1), ck] = x
                    if which == 1:
                        bias[me, pl.ds(grp, 1), ck] += jnp.sum(x, axis=0, keepdims=True)
                dk = jnp.dot(gb, qb, preferred_element_type=F32)
                dv = jnp.dot(pb, db, preferred_element_type=F32)
                dkv[slot, rows, ck] = dk.astype(BF)
                dkv[slot, rows, cv] = dv.astype(BF)
                bias[me, pl.ds(grp, 1), cv] += jnp.sum(dv, axis=0, keepdims=True)

    def step(i, do_a, do_b):
        b = i - 2
        if do_b:
            @pl.when(b >= NP)
            def _():
                exchange(0, b - NP, T3[0], T4[0])

            stat_wait(b)

            @pl.when(b >= 2)
            def _():
                dkv_copy(b - 2).wait()

            od_pre(b, True)
        if do_a:
            @pl.when(i + B4 < STEPS)
            def _():
                raw_copy(i + B4).wait()

            @pl.when(i + B4 + 1 < STEPS)
            def _():
                raw_copy(i + B4 + 1).start()

        if do_b:
            combine(b)
            stage_b(b)
        if do_a:
            stage_a(i)
            sort_frames(i + B4)
        if do_b:
            acc[b // NP] += jnp.dot(mt[b % 3], dkv[b % 2], preferred_element_type=F32)
        if do_a:
            stat_send(i)
        if do_b:
            dkv_copy(b).start()
            od_post(b, True)

    barrier = pltpu.get_barrier_semaphore()
    for k in range(1, B4):
        pl.semaphore_signal(barrier, inc=1, device_id={"cp": (me + k) % B4}, device_id_type=MESH)
    top, low = pl.ds(0, ROWS), pl.ds(ROWS, D - ROWS)
    rest = pl.ds(0, D - ROWS)
    loads = [pltpu.make_async_copy(x, y, in_sem.at[k]) for k, (x, y) in enumerate((
        (h_hbm, res.at[0]), (wq_hbm.at[top], kv.at[0]), (wq_hbm.at[low], dkv.at[0, rest]), (dy_hbm, res.at[1]),
        (wo_hbm.at[top], kv.at[1]), (wo_hbm.at[low], dkv.at[1, rest]), (wk_hbm, wk), (wv_hbm, wv)))]
    raw_copy(0).start()
    for cp in loads:
        cp.start()
    raw[:, F:] = jnp.zeros((B2, FP - F, B8, QW), BF)
    perm[...] = permutation(FC)
    bv32[...] = vec(bv)
    bias[me] = jnp.zeros((B8, D), F32)
    for cp in loads[:-2]:
        cp.wait()

    def first(n, carry):
        raw_copy(n).wait()
        raw_copy(n + 1).start()
        rows = pl.ds(pl.multiple_of(RC * n, RC), RC)
        x_hat, _ = norm_parts(res[0, rows].astype(F32))
        x = (x_hat * vec(gain) + vec(shift)).astype(BF)
        q[rows] = (jnp.dot(x[:, :ROWS], kv[0], preferred_element_type=F32)
                   + jnp.dot(x[:, ROWS:], dkv[0, rest], preferred_element_type=F32) + vec(bq)).astype(BF)
        do[rows, :ROWS] = dotg(res[1, rows], kv[1], 1, 1).astype(BF)
        do[rows, ROWS:] = dotg(res[1, rows], dkv[1, rest], 1, 1).astype(BF)
        sort_frames(n)
        for g in range(2):
            acc[g, rows] = jnp.zeros((RC, D), F32)
        return carry

    lax.fori_loop(0, TOK // RC, first, 0)
    for cp in loads[-2:]:
        cp.wait()
    pl.semaphore_wait(barrier, 3)

    def run(lo, hi, do_a, do_b):
        def body(i, carry):
            step(i, do_a, do_b)
            return carry
        lax.fori_loop(lo, hi, body, 0)

    run(0, 2, True, False)
    run(2, STEPS, True, True)
    run(STEPS, STEPS + 2, False, True)

    def b_copy(k, src):
        return remote(bias.at[src], bias.at[src], b_send.at[k - 1], b_recv.at[src], (me + k) % 4)

    for k in range(1, 4):
        b_copy(k, me).start()
    dkv_copy(STEPS - 2).wait()
    dkv_copy(STEPS - 1).wait()

    def part(u, k):
        return frames.at[u % 2, pl.ds(ROWS * k, ROWS)]

    def c_load(u, k):
        return pltpu.make_async_copy(dkv_hbm.at[k % 2, 2 * u + k // 2], part(u, k), in_sem.at[k])

    def dm_copy(u, k):
        return pltpu.make_async_copy((kv, dkv)[k].at[u % 2], dm_hbm.at[2 * u + k], dm_sem.at[k, u % 2])

    for k in range(B4):
        c_load(0, k).start()
    exchange(1, 0, T3[1], T4[1])

    def c_step(u, carry):
        for k in range(B4):
            c_load(u, k).wait()

        @pl.when(u + 1 < NP // 2)
        def _():
            for k in range(B4):
                c_load(u + 1, k).start()

        @pl.when(u >= 2)
        def _():
            for k in range(2):
                dm_copy(u - 2, k).wait()

        @pl.when(u < B4)
        def _():
            for k in range(2):
                od_pre(STEPS + 2 * u + k, False)
                od_post(STEPS + 2 * u + k, False)

        exchange(1, u + 1, T3[1], T4[1])

        @pl.when(u == 1)
        def _():
            for n in range(NP - T4[0], NCH[0]):
                forward(0, n)

        @pl.when(u == 3)
        def _():
            gathered(0)

        @pl.when(u == 6)
        def _():
            rows = res.at[0, 0:TOK // 2]
            for sem in (s3_send, s3s_send, s4_send):
                pltpu.make_async_copy(rows, rows, sem).wait()
            pltpu.make_async_copy(res.at[0], res.at[0], res_recv).wait()
            pltpu.make_async_copy(res, res_hbm, out_sem.at[2]).start()

        w = jnp.concatenate([wk[:, :W], wv[:, :W], wk[:, W:], wv[:, W:]], axis=1)
        for k in range(2):
            x = jnp.concatenate([part(u, 2 * k)[...], part(u, 2 * k + 1)[...]], axis=1)
            (kv, dkv)[k][u % 2] = dotg(x, w, 1, 1).astype(BF)
        for k in range(2):
            dm_copy(u, k).start()
        return carry

    lax.fori_loop(0, NP // 2, c_step, 0)
    for t in range(NP // 2 + 1, T4[1] + NCH[1]):
        exchange(1, t, T3[1], T4[1])
    gathered(1)
    for k in range(1, 4):
        b_copy(k, (me + k) % 4).wait_recv()
        b_copy(k, me).wait_send()
    big1[0:8, :] = (bias[0, :, 0:W] + bias[1, :, 0:W]) + (bias[2, :, 0:W] + bias[3, :, 0:W])
    big1[8:16, :] = (bias[0, :, W:] + bias[1, :, W:]) + (bias[2, :, W:] + bias[3, :, W:])
    bias_out = pltpu.make_async_copy(big1.at[0:16], bias_hbm, out_sem.at[3])
    bias_out.start()
    for u in (NP // 2 - 2, NP // 2 - 1):
        for k in range(2):
            dm_copy(u, k).wait()
    dw_copy(0).wait()
    dw_copy(1).wait()
    pltpu.make_async_copy(res, res_hbm, out_sem.at[2]).wait()
    bias_out.wait()


def attention(mt, h, dy, w_q, w_o, w_k, w_v, gain, shift, b_q, b_v):
    vm = pl.BlockSpec(memory_space=VMEM)
    hbm = pl.BlockSpec(memory_space=pl.ANY)
    dma = pltpu.SemaphoreType.DMA
    d2, d4, d8, dn = dma((B2,)), dma((B4,)), dma((B8,)), dma((B2, B8))
    credit = pltpu.SemaphoreType.REGULAR((B2,))
    probs, mat, rows32 = VMEM((B2, B4, FP, LANES), F32), VMEM((D, D), BF), VMEM((B4, T, W), F32)
    return pl.pallas_call(
        attn_kernel, name="attention",
        out_shape=(SDS((B2, TOK, D), BF), SDS((B2, D, D), F32), SDS((2 * B8, W), F32), SDS((NP, ROWS, D), BF),
                   SDS((B2, NP, ROWS, D), BF)),
        in_specs=[hbm] * 7 + [vm] * B4,
        out_specs=(hbm,) * 5,
        scratch_shapes=[
            VMEM((B2, FP, B8, QW), BF), VMEM((QW, QW), BF), VMEM((1, D), F32), VMEM((B2, B8 * FP, D), BF), mat, mat, mat, mat,
            VMEM((B2, ROWS, D), BF), probs, probs, VMEM((3, D, ROWS), BF), VMEM((B4, B4, 2 * B8, LANES), F32),
            VMEM((B8, LANES), F32), VMEM((B2, ROWS, D), BF), VMEM((B2, D, D), F32), VMEM((B4, B8, D), F32),
            VMEM((B2, B2, 2 * T, W), F32), VMEM((B4, 2 * T, W), F32), rows32, rows32, VMEM((B8, T, W), F32),
            VMEM((B2, TOK, D), BF), VMEM((D, W), F32), VMEM((B2, D // 2, W), F32),
            d2, d8, d2, dma((B2, B2)), d4, d4, d4, d4, d4, d8, d8, dma, dma((2 * B8,)), dma, dma, dma, d2, d2, dn, dn, dn, dn, dn, dn, d2, d4, d4,
            credit, credit],
        compiler_params=pltpu.CompilerParams(vmem_limit_bytes=67043328, collective_id=0, has_side_effects=True),
    )(mt, h, dy, w_q, w_o, w_k, w_v, gain, shift, b_q, b_v)


def solution(mesh):
    act_spec = P("dp", None, None)
    mem_spec = P("dp", "cp", None)
    vec_out = P("dp")
    mat_out = P("dp", None)
    in_specs = (act_spec, mem_spec, P(), P(), P(), P(), P(), P(), P(), P(), P(), act_spec)
    out_specs = (act_spec, act_spec, mem_spec, vec_out, vec_out, mat_out, vec_out, mat_out, mat_out, vec_out, mat_out, vec_out)

    def device_step(hidden, memory, ln_gain, ln_bias, w_q, b_q, w_k, w_v, b_v, w_o, b_o, grad_y):
        h = hidden.reshape(TOK, D)
        dy = grad_y.reshape(TOK, D)
        res, dw, bias, dm, _ = attention(memory.transpose(1, 0, 2), h, dy, w_q, w_o, w_k, w_v, ln_gain, ln_bias, b_q, b_v)
        gm, y, gh, gwo, gwq, gwk, gwv, dg, db, dbq, dbv, dbo = finish(
            dm.reshape(NB, FP, D), res, h, dy, w_o, w_q, dw, bias, ln_gain, ln_bias, b_o)
        return (y.reshape(NB, T, D), gh.reshape(NB, T, D), gm.transpose(1, 0, 2), dg, db, gwq, dbq, gwk, gwv, dbv, gwo, dbo)

    return jax.shard_map(device_step, mesh=mesh, in_specs=in_specs, out_specs=out_specs, check_vma=False)
```

```python
import functools
import math
import jax
import jax.numpy as jnp
from jax import lax
from jax.experimental import pallas as pl
from jax.experimental.pallas import tpu as pltpu
from jax.sharding import PartitionSpec as P

EPS = 1e-5
HEAD = 64
F, FP, D, T = 375, 384, 1024, 32
NB = 32
NP = NB // 2
STEPS = 2 * NP
W = 512
ROWS = 2 * FP
QW = 256
BF, F32 = jnp.bfloat16, jnp.float32
LOG2 = 0.125 * math.log2(math.e)
MESH = pl.DeviceIdType.MESH
VMEM = pltpu.VMEM
B2, B4, B8, LANES = 2, 4, 8, 128
RC = 256
TOK = NB * T
SDS = jax.ShapeDtypeStruct


def dotg(a, b, ca, cb):
    return lax.dot_general(a, b, (((ca,), (cb,)), ((), ())), preferred_element_type=F32)


FC = 32
NFC = FP // FC


def fixed(rows):
    return pl.BlockSpec((rows, D), lambda s: (0, 0), pipeline_mode=pl.Buffered(1))


def lanes(t):
    return slice(LANES * t, LANES * (t + 1))


def permutation(n):
    r = lax.broadcasted_iota(jnp.int32, (QW, QW), 0)
    k = lax.broadcasted_iota(jnp.int32, (QW, QW), 1)
    return (k == r % n * (QW // n) + r // n).astype(F32).astype(BF)


def norm_parts(h):
    centered = h - jnp.mean(h, axis=-1, keepdims=True)
    inv_std = lax.rsqrt(jnp.mean(centered * centered, axis=-1, keepdims=True) + EPS)
    return centered * inv_std, inv_std


JOB0, JOBS = 2, 4
FB = 16
NFB = FP // FB


def finish_kernel(dm_hbm, res_hbm, h_hbm, dy_hbm, wo_hbm, wq_hbm, dw_hbm, bias, gain, shift, bo,
                  gm_hbm, y_hbm, gh_hbm, gwo_hbm, gwq_hbm, gwk_hbm, gwv_hbm, dg, db, dbq, dbv, dbo,
                  src, dst, perm, res, h, dy, wo, wq, x, y, gh, gw, stage, sums,
                  src_sem, dst_sem, in_sem, y_sem, gh_sem, gw_sem, ld_sem, st_sem):
    loads = [pltpu.make_async_copy(a, b, in_sem.at[k]) for k, (a, b) in enumerate(
        ((h_hbm, h), (res_hbm, res), (wo_hbm, wo), (dy_hbm, dy), (wq_hbm, wq)))]

    def src_copy(s):
        return pltpu.make_async_copy(dm_hbm.at[:, pl.ds(pl.multiple_of(FB * s, FB), FB)], src.at[s % B4], src_sem.at[s % B4])

    def dst_copy(s):
        return pltpu.make_async_copy(dst.at[s % B4], gm_hbm.at[pl.ds(FB * s, FB)], dst_sem.at[s % B4])

    def last_copy():
        s = NFB - 1
        return pltpu.make_async_copy(dst.at[s % B4, 0:F - FB * s], gm_hbm.at[FB * s:F], dst_sem.at[s % B4])

    def rows(n):
        return pl.ds(pl.multiple_of(RC * n, RC), RC)

    def out_copy(a, b, sem, n):
        return pltpu.make_async_copy(a.at[rows(n)], b.at[rows(n)], sem.at[n])

    def gw_copy(b, n):
        return pltpu.make_async_copy(gw.at[n], b.at[rows(n)], gw_sem.at[n])

    def piece_in(k):
        g, v = k // 2, k % 2
        return pltpu.make_async_copy(dw_hbm.at[g, :, pl.ds(W * v, W)], stage.at[v], ld_sem.at[v])

    def piece_out(k):
        g, v = k // 2, k % 2
        return pltpu.make_async_copy(stage.at[v], (gwk_hbm, gwv_hbm)[v].at[:, pl.ds(W * g, W)], st_sem.at[v])

    def vec(ref):
        return ref[...].astype(F32).reshape(1, D)

    def move(s):
        for k in range(NB // FB):
            z = src[s % B4, FB * k:FB * (k + 1)].reshape(QW, D)
            z = jnp.dot(perm[...], z, preferred_element_type=F32)
            dst[s % B4, :, FB * k:FB * (k + 1), :] = z.astype(BF).reshape(FB, FB, D)

    def job_y(n):
        hf = h[rows(n)].astype(F32)
        x_hat, _ = norm_parts(hf)
        x[rows(n)] = (x_hat * vec(gain) + vec(shift)).astype(BF)
        y[rows(n)] = (hf + jnp.dot(res[0, rows(n)], wo[...], preferred_element_type=F32) + vec(bo)).astype(BF)

    def job_wo(n):
        gw[n] = dotg(res[0, :, rows(n)], dy[...], 0, 0)

    def job_h(n):
        x_hat, inv_std = norm_parts(h[rows(n)].astype(F32))
        dyf = dy[rows(n)].astype(F32)
        d_x = dotg(res[1, rows(n)], wq[...], 1, 1)
        for k, a in enumerate((d_x * x_hat, d_x, dyf)):
            sums[k:k + 1] += jnp.sum(a, axis=0, keepdims=True)
        d_hat = d_x * vec(gain)
        d_h = inv_std * (d_hat - jnp.mean(d_hat, axis=-1, keepdims=True) - x_hat * jnp.mean(d_hat * x_hat, axis=-1, keepdims=True))
        gh[rows(n)] = (dyf + d_h).astype(BF)

    def job_wq(n):
        gw[n] = dotg(x[:, rows(n)], res[1], 0, 0)

    for k in range(B4 - 1):
        src_copy(k).start()
    for cp in loads:
        cp.start()
    piece_in(0).start()
    piece_in(1).start()
    sums[...] = jnp.zeros_like(sums)
    perm[...] = permutation(FB)
    for ref, k in ((dbq, 0), (dbv, B8)):
        ref[...] = jnp.concatenate([bias[k:k + 1], bias[k + 1:k + 2]], axis=1).reshape(D)
    outs = ((job_y, lambda n: out_copy(y, y_hbm, y_sem, n)), (job_wo, lambda n: gw_copy(gwo_hbm, n)),
            (job_h, lambda n: out_copy(gh, gh_hbm, gh_sem, n)), (job_wq, lambda n: gw_copy(gwq_hbm, n)))
    needs = (loads[:3], loads[3:4], loads[4:], ())

    def step(s, carry):
        src_copy(s).wait()

        @pl.when(s + B4 - 1 < NFB)
        def _():
            src_copy(s + B4 - 1).start()

        @pl.when(s >= B4)
        def _():
            dst_copy(s - B4).wait()

        job = s - JOB0
        n = job % JOBS
        for kind, (f, copy) in enumerate(outs):
            @pl.when((job >= kind * JOBS) & (job < (kind + 1) * JOBS))
            def _():
                if needs[kind]:
                    @pl.when(n == 0)
                    def _():
                        for cp in needs[kind]:
                            cp.wait()
                if kind == 3:
                    gw_copy(gwo_hbm, n).wait()
                move(s)
                f(n)
                copy(n).start()

        @pl.when((job < 0) | (job >= JOBS * JOBS))
        def _():
            move(s)

        @pl.when(s < NFB - 1)
        def _():
            dst_copy(s).start()

        for v in range(2):
            @pl.when(s == JOBS + v)
            def _():
                piece_in(v).wait()
                piece_out(v).start()

            @pl.when(s == B8 + v)
            def _():
                piece_out(v).wait()
                piece_in(v + 2).start()

            @pl.when(s == B8 + JOBS + v)
            def _():
                piece_in(v + 2).wait()
                piece_out(v + 2).start()
        return carry

    lax.fori_loop(0, NFB, step, 0)
    last_copy().start()
    for k, ref in enumerate((dg, db, dbo)):
        ref[...] = sums[k:k + 1].reshape(D)
    for k in range(JOBS):
        out_copy(y, y_hbm, y_sem, k).wait()
        out_copy(gh, gh_hbm, gh_sem, k).wait()
        gw_copy(gwq_hbm, k).wait()
    piece_out(2).wait()
    piece_out(3).wait()
    for k in range(2, JOBS + 1):
        dst_copy(NFB - k).wait()
    last_copy().wait()


def finish(dm, res, h, dy, w_o, w_q, dw, bias, gain, shift, b_o):
    hbm, vm = pl.BlockSpec(memory_space=pl.ANY), pl.BlockSpec(memory_space=VMEM)
    dma = pltpu.SemaphoreType.DMA
    mat, dj, d2, vec = VMEM((D, D), BF), dma((JOBS,)), dma((B2,)), SDS((D,), F32)
    return pl.pallas_call(
        finish_kernel, name="finish",
        out_shape=(SDS((F, NB, D), BF), SDS((TOK, D), BF), SDS((TOK, D), BF)) + (SDS((D, D), F32),) * B4 + (vec,) * (B4 + 1),
        in_specs=[hbm] * (B8 - 1) + [vm] * B4,
        out_specs=(hbm,) * (B8 - 1) + (vm,) * (B4 + 1),
        scratch_shapes=[
            VMEM((B4, NB, FB, D), BF), VMEM((B4, FB, NB, D), BF), VMEM((QW, QW), BF), VMEM((B2, TOK, D), BF), mat, mat, mat, mat, mat,
            mat, mat, VMEM((JOBS, RC, D), F32), VMEM((B2, D, W), F32), VMEM((B8, D), F32), dj, dj, dma((B8,)), dj, dj, dj, d2, d2],
        compiler_params=pltpu.CompilerParams(vmem_limit_bytes=50 << 20),
    )(dm, res, h, dy, w_o, w_q, dw, bias, gain, shift, b_o)


def block_mask():
    return lax.broadcasted_iota(jnp.int32, (128, 256), 0) // T == lax.broadcasted_iota(jnp.int32, (128, 256), 1) // HEAD


def block_diag(x, mask):
    return jnp.where(mask, jnp.concatenate([x] * 4, axis=0), jnp.zeros((), BF))


def when(cond):
    if isinstance(cond, bool):
        return (lambda f: f()) if cond else (lambda f: None)
    return pl.when(cond)


CH = (64, 128)
NCH = tuple(D // 2 // rows for rows in CH)
T3, T4 = (8, 4), (11, 6)


ALL, FILL, DRAIN = range(3)


def attn_kernel(m_hbm, h_hbm, dy_hbm, wq_hbm, wo_hbm, wk_hbm, wv_hbm, gain, shift, bq, bv,
                res_hbm, dw_hbm, bias_hbm, dm_hbm, dkv_hbm, mp_hbm,
                raw, perm, bv32, frames, q, do, wk, wv, kv, e_s, dp_s, mt, stats, coef, dkv, acc, bias, od, r1, keep, x2, r2, res, big1, big2,
                raw_sem, in_sem, dkv_sem, dm_sem, out_sem, st_send, st_recv, s1_send, s1_recv, s2_send, s2_recv,
                s3_send, s3_recv, s3s_send, s4_send, res_recv, e1_send, e1_recv, e2_send, e2_recv,
                e3_send, e3_recv, e3s_send, e4_send, acc_recv, b_send, b_recv, keep_sem, load_sem, free_sib, free_xn):
    me = lax.axis_index("cp")
    cx, cc = me // 2, me % 2
    sib, xn = 2 * cx + 1 - cc, 2 * (1 - cx) + cc

    def vec(ref):
        return ref[...].astype(F32).reshape(1, D)

    def remote(src, dst, ss, rs, dev):
        return pltpu.make_async_remote_copy(src_ref=src, dst_ref=dst, send_sem=ss, recv_sem=rs,
                                            device_id={"cp": dev}, device_id_type=MESH)

    def raw_copy(c):
        seqs = pl.ds(pl.multiple_of(B8 * (c // B4 % B4), B8), B8)
        return pltpu.make_async_copy(m_hbm.at[:, seqs, quarter(c)], raw.at[c % 2, 0:F], raw_sem.at[c % 2])

    def quarter(c):
        return pl.ds(pl.multiple_of(c % B4 * QW, QW), QW)

    def sort_frames(c):
        for n in range(NFC):
            x = raw[c % 2, FC * n:FC * (n + 1)].reshape(QW, QW)
            y = jnp.dot(perm[...], x, preferred_element_type=F32).astype(BF)
            for b in range(B8):
                frames[c // B4 % 2, FP * b + FC * n:FP * b + FC * (n + 1), quarter(c)] = y[FC * b:FC * (b + 1)]

    def dkv_copy(i):
        return pltpu.make_async_copy(dkv.at[i % 2], dkv_hbm.at[i // NP, i % NP], dkv_sem.at[i % 2])

    def stat_send(i):
        for k in range(1, B4):
            remote(stats.at[i % B4, me], stats.at[i % B4, me], st_send.at[i % B4], st_recv.at[i % B4], (me + k) % B4).start()

    def stat_wait(i):
        three = stats.at[i % B4, 0:3]
        for sem in (st_recv, st_send):
            pltpu.make_async_copy(three, three, sem.at[i % B4]).wait()

    def s1(b):
        return remote(od.at[b % 2, 1 - cc], r1.at[b % 4], s1_send.at[b % 4], s1_recv.at[b % 4], sib)

    def s2(b):
        return remote(x2.at[b % 4], r2.at[b % 8], s2_send.at[b % 8], s2_recv.at[b % 8], xn)

    def res_at(b, x):
        return res.at[cc, pl.ds(pl.multiple_of(64 * (b % NP) + T * x, T), T), pl.ds(pl.multiple_of(W * (b // NP), W), W)]

    def s3(b, x):
        return remote(res_at(b, x), res_at(b, x), s3_send, s3_recv.at[b % (2 * B8)], xn)

    def s3s(b):
        return remote(res_at(b, cx), res_at(b, cx), s3s_send, res_recv, sib)

    def s4(b):
        return remote(res_at(b, 1 - cx), res_at(b, 1 - cx), s4_send, res_recv, sib)

    def on(mode, b, k):
        return True if mode == ALL else b >= k if mode == FILL else b - k < STEPS

    def od_wait(b, mode):
        @when(on(mode, b, 8))
        def _():
            s3(b - 8, 1 - cx).wait_recv()

        @when(on(mode, b, 5))
        def _():
            s2(b - 5).wait_recv()
            s2(b - 5).wait_send()

        @when(on(mode, b, 2))
        def _():
            s1(b - 2).wait_send()
            s1(b - 2).wait_recv()

    def od_sum(b, mode):
        @when(on(mode, b, 5))
        def _():
            res_at(b - 5, cx)[...] = (keep[(b - 5) % B4] + r2[(b - 5) % B8]).astype(BF)

        @when(on(mode, b, 2))
        def _():
            for ref, x in ((keep, cx), (x2, 1 - cx)):
                rows = pl.ds(pl.multiple_of(T * x, T), T)
                ref[(b - 2) % B4] = od[b % 2, cc, rows, :] + r1[(b - 2) % B4, rows, :]

    def od_send(b, mode):
        @when(on(mode, b, 2))
        def _():
            s2(b - 2).start()

        @when(on(mode, b, 5))
        def _():
            s3(b - 5, cx).start()
            s3s(b - 5).start()

        @when(on(mode, b, 8))
        def _():
            s4(b - 8).start()

    own = pl.ds(pl.multiple_of(W * cc, W), W)
    other = pl.ds(pl.multiple_of(W * (1 - cc), W), W)

    def rows_of(g, x, n):
        return pl.ds(pl.multiple_of(x * (D // 2) + CH[g] * n, CH[g]), CH[g])

    def chunk_of(g, n):
        return big2.at[g, pl.ds(pl.multiple_of(CH[g] * n, CH[g]), CH[g])]

    def e1(g):
        return remote(acc.at[g, :, other], big1, e1_send.at[g], e1_recv.at[g], sib)

    def e2(g, n):
        return remote(acc.at[g, rows_of(g, 1 - cx, n), own], chunk_of(g, n), e2_send.at[g, n], e2_recv.at[g, n], xn)

    def e3(g, n, x):
        ref = acc.at[g, rows_of(g, x, n), own]
        return remote(ref, ref, e3_send.at[g, n], e3_recv.at[g, n], xn)

    def to_sib(g, n, x, sem):
        ref = acc.at[g, rows_of(g, x, n), own]
        return remote(ref, ref, sem.at[g, n], acc_recv.at[g], sib)

    def dw_copy(g):
        return pltpu.make_async_copy(acc.at[g], dw_hbm.at[g], out_sem.at[g])

    def reduce_core(g, n):
        for x in (cx, 1 - cx):
            acc[g, rows_of(g, x, n), own] += big1[rows_of(g, x, n), :]
        e2(g, n).start()

    def sent(g, n):
        e2(g, n).wait_send()
        pl.semaphore_signal(free_xn.at[g], inc=1, device_id={"cp": xn}, device_id_type=MESH)

    def reduce_chip(g, n):
        e2(g, n).wait_recv()
        pl.semaphore_wait(free_xn.at[g], 1)
        acc[g, rows_of(g, cx, n), own] += chunk_of(g, n)[...]
        e3(g, n, cx).start()
        to_sib(g, n, cx, e3s_send).start()

    def forward(g, n):
        e3(g, n, 1 - cx).wait_recv()
        to_sib(g, n, 1 - cx, e4_send).start()

    def gathered(g):
        half = acc.at[g, :, other]
        remote(half, half, e1_send.at[g], acc_recv.at[g], sib).wait_recv()
        for n in range(NCH[g]):
            e3(g, n, cx).wait_send()
            to_sib(g, n, cx, e3s_send).wait_send()
            to_sib(g, n, 1 - cx, e4_send).wait_send()
        dw_copy(g).start()

    def exchange(g, t, t3, t4):
        def chunk(t0, f):
            n = t - t0
            if isinstance(n, int):
                if 0 <= n < NCH[g]:
                    f(g, n)
            else:
                pl.when((n >= 0) & (n < NCH[g]))(lambda: f(g, n))

        @when(t == 0)
        def _():
            e1(g).start()

        @when(t == 1)
        def _():
            e1(g).wait_send()
            pl.semaphore_signal(free_sib.at[g], inc=1, device_id={"cp": sib}, device_id_type=MESH)
            e1(g).wait_recv()

        @when(t == t3)
        def _():
            pl.semaphore_wait(free_sib.at[g], 1)

        chunk(1, reduce_core)
        chunk(t3 - 1, sent)
        chunk(t3, reduce_chip)
        chunk(t4, forward)

    def operands(i, j, h):
        cols = pl.ds(pl.multiple_of(W * (i // NP) + 256 * h, 256), 256)
        rows = pl.ds(pl.multiple_of(64 * (i % NP) + T * j, T), T)
        mask = block_mask()
        return block_diag(q[rows, cols], mask), block_diag(do[rows, cols], mask), mask

    def rows_of_pair(i):
        return frames[i // B4 % 2, pl.ds(pl.multiple_of(i % B4 * ROWS, ROWS), ROWS), :]

    def project(i):
        cols = pl.ds(pl.multiple_of(W * (i // NP), W), W)
        m = rows_of_pair(i)
        kv[i % 3, :, 0:W] = jnp.dot(m, wk[:, cols], preferred_element_type=F32).astype(BF)
        kv[i % 3, :, W:] = (jnp.dot(m, wv[:, cols], preferred_element_type=F32) + bv32[:, cols]).astype(BF)
        mt[i % 3] = m.T

    def scores(i):
        slot = i % 2
        real = lax.broadcasted_iota(jnp.int32, (FP, LANES), 0) < F
        for j in range(2):
            rows = slice(FP * j, FP * (j + 1))
            for h in range(2):
                n = 2 * j + h
                qb, db, _ = operands(i, j, h)
                s = dotg(kv[i % 3, rows, QW * h:QW * (h + 1)], qb, 1, 1)
                dp = dotg(kv[i % 3, rows, W + QW * h:W + QW * (h + 1)], db, 1, 1)
                s = jnp.where(real, s, -1e30)
                top = jnp.max(s, axis=0, keepdims=True)
                e = jnp.exp2((s - top) * LOG2)
                e_s[slot, n] = e
                dp_s[slot, n] = dp
                for k, row in enumerate((top, jnp.sum(e, axis=0, keepdims=True), jnp.sum(e * dp, axis=0, keepdims=True))):
                    stats[i % B4, me, B4 * k + n:B4 * k + n + 1, :] = row

    def combine(i):
        slot = i % 4
        tops = [stats[slot, d, 0:4, :] for d in range(4)]
        top = jnp.maximum(jnp.maximum(tops[0], tops[1]), jnp.maximum(tops[2], tops[3]))
        ws = [jnp.exp2((t - top) * LOG2) for t in tops]
        total = sum(stats[slot, d, 4:8, :] * ws[d] for d in range(4))
        dots = sum(stats[slot, d, 8:12, :] * ws[d] for d in range(4))
        coef[0:4, :] = jnp.exp2((stats[slot, me, 0:4, :] - top) * LOG2) / total
        coef[4:8, :] = dots / total

    def grads(i):
        slot, grp = i % 2, i // NP
        blocks = []
        for j in range(2):
            rows = slice(FP * j, FP * (j + 1))
            for h in range(2):
                n = 2 * j + h
                qb, db, _ = operands(i, j, h)
                ck, cv = slice(QW * h, QW * (h + 1)), slice(W + QW * h, W + QW * (h + 1))
                p = e_s[slot, n] * coef[n:n + 1, :]
                pb = p.astype(BF)
                gb = (p * (dp_s[slot, n] - coef[B4 + n:B4 + n + 1, :]) * 0.125).astype(BF)
                dk = jnp.dot(gb, qb, preferred_element_type=F32)
                dv = jnp.dot(pb, db, preferred_element_type=F32)
                dkv[slot, rows, ck] = dk.astype(BF)
                dkv[slot, rows, cv] = dv.astype(BF)
                bias[me, pl.ds(grp, 1), cv] += jnp.sum(dv, axis=0, keepdims=True)
                blocks.append((j, h, pb, gb))
        return blocks

    def sums(i, blocks):
        mask = block_mask()
        for j, h, pb, gb in blocks:
            rows = slice(FP * j, FP * (j + 1))
            ck, cv = slice(QW * h, QW * (h + 1)), slice(W + QW * h, W + QW * (h + 1))
            for which, x in ((0, dotg(pb, kv[i % 3, rows, cv], 0, 0)), (1, dotg(gb, kv[i % 3, rows, ck], 0, 0))):
                x = jnp.where(mask, x, 0.0)
                x = (x[0:32] + x[32:64]) + (x[64:96] + x[96:128])
                od[i % 2, which, T * j:T * (j + 1), ck] = x
                if which == 1:
                    bias[me, pl.ds(i // NP, 1), ck] += jnp.sum(x, axis=0, keepdims=True)

    def keep_copy(n):
        return pltpu.make_async_copy(frames.at[n % 2], mp_hbm.at[n % B4], keep_sem)

    def load_copy(n):
        return pltpu.make_async_copy(mp_hbm.at[n % B4], frames.at[n % 2], load_sem)

    def tiles(i, do_sort):
        n = i // B4
        if do_sort:
            raw_copy(i + B4).wait()

            @pl.when(i + B4 + 1 < NP)
            def _():
                raw_copy(i + B4 + 1).start()

        @pl.when(i % B4 == 0)
        def _():
            @pl.when((n >= 1) & (n <= B4))
            def _():
                keep_copy(n - 1).wait()

            @pl.when(n < B4)
            def _():
                keep_copy(n).start()

            if not do_sort:
                @pl.when(n >= B4)
                def _():
                    load_copy(n).wait()

                @pl.when((n >= B4 - 1) & (n < B8 - 1))
                def _():
                    load_copy(n + 1).start()

    def step(i, do_a, do_b, do_sort, mode):
        b = i - 2
        if do_b:
            @pl.when(b >= NP)
            def _():
                exchange(0, b - NP, T3[0], T4[0])

            stat_wait(b)

            @when(on(mode, b, 2))
            def _():
                dkv_copy(b - 2).wait()

            od_wait(b, mode)
        if do_a:
            tiles(i, do_sort)
        if do_b:
            od_sum(b, mode)
            combine(b)
        if do_a:
            project(i)
        if do_b:
            blocks = grads(b)
        if do_a:
            scores(i)
            if do_sort:
                sort_frames(i + B4)
        if do_b:
            acc[b // NP] += jnp.dot(mt[b % 3], dkv[b % 2], preferred_element_type=F32)
            sums(b, blocks)
        if do_a:
            stat_send(i)
        if do_b:
            dkv_copy(b).start()
            s1(b).start()
            od_send(b, mode)

    barrier = pltpu.get_barrier_semaphore()
    for k in range(1, B4):
        pl.semaphore_signal(barrier, inc=1, device_id={"cp": (me + k) % B4}, device_id_type=MESH)
    top, low = pl.ds(0, ROWS), pl.ds(ROWS, D - ROWS)
    rest = pl.ds(0, D - ROWS)
    loads = [pltpu.make_async_copy(x, y, in_sem.at[k]) for k, (x, y) in enumerate((
        (h_hbm, res.at[0]), (wq_hbm.at[top], kv.at[0]), (wq_hbm.at[low], dkv.at[0, rest]), (dy_hbm, res.at[1]),
        (wo_hbm.at[top], kv.at[1]), (wo_hbm.at[low], dkv.at[1, rest]), (wk_hbm, wk), (wv_hbm, wv)))]
    raw_copy(0).start()
    for cp in loads:
        cp.start()
    raw[:, F:] = jnp.zeros((B2, FP - F, B8, QW), BF)
    perm[...] = permutation(FC)
    bv32[...] = vec(bv)
    bias[me] = jnp.zeros((B8, D), F32)
    for cp in loads[:3]:
        cp.wait()

    def first(n, carry):
        rows = pl.ds(pl.multiple_of(RC * n, RC), RC)
        x_hat, _ = norm_parts(res[0, rows].astype(F32))
        x = (x_hat * vec(gain) + vec(shift)).astype(BF)
        q[rows] = (jnp.dot(x[:, :ROWS], kv[0], preferred_element_type=F32)
                   + jnp.dot(x[:, ROWS:], dkv[0, rest], preferred_element_type=F32) + vec(bq)).astype(BF)
        for g in range(2):
            acc[g, rows] = jnp.zeros((RC, D), F32)
        return carry

    def second(n, carry):
        raw_copy(n).wait()
        raw_copy(n + 1).start()
        rows = pl.ds(pl.multiple_of(RC * n, RC), RC)
        sort_frames(n)
        do[rows, :ROWS] = dotg(res[1, rows], kv[1], 1, 1).astype(BF)
        do[rows, ROWS:] = dotg(res[1, rows], dkv[1, rest], 1, 1).astype(BF)
        return carry

    lax.fori_loop(0, TOK // RC, first, 0)
    for cp in loads[3:-2]:
        cp.wait()
    lax.fori_loop(0, TOK // RC, second, 0)
    for cp in loads[-2:]:
        cp.wait()
    pl.semaphore_wait(barrier, 3)

    def run(lo, hi, *what):
        def body(i, carry):
            step(i, *what)
            return carry
        lax.fori_loop(lo, hi, body, 0)

    run(0, 2, True, False, True, FILL)
    run(2, NP - B4, True, True, True, FILL)
    run(NP - B4, STEPS, True, True, False, ALL)
    run(STEPS, STEPS + 2, False, True, False, ALL)

    def b_copy(k, src):
        return remote(bias.at[src], bias.at[src], b_send.at[k - 1], b_recv.at[src], (me + k) % 4)

    for k in range(1, 4):
        b_copy(k, me).start()
    dkv_copy(STEPS - 2).wait()
    dkv_copy(STEPS - 1).wait()

    def part(u, k):
        return frames.at[u % 2, pl.ds(ROWS * k, ROWS)]

    def c_load(u, k):
        return pltpu.make_async_copy(dkv_hbm.at[k % 2, 2 * u + k // 2], part(u, k), in_sem.at[k])

    def dm_copy(u, k):
        return pltpu.make_async_copy((kv, dkv)[k].at[u % 2], dm_hbm.at[2 * u + k], dm_sem.at[k, u % 2])

    for k in range(B4):
        c_load(0, k).start()
    exchange(1, 0, T3[1], T4[1])

    def c_step(u, carry):
        for k in range(B4):
            c_load(u, k).wait()

        @pl.when(u + 1 < NP // 2)
        def _():
            for k in range(B4):
                c_load(u + 1, k).start()

        @pl.when(u >= 2)
        def _():
            for k in range(2):
                dm_copy(u - 2, k).wait()

        @pl.when(u < B4)
        def _():
            for k in range(2):
                od_wait(STEPS + 2 * u + k, DRAIN)
                od_sum(STEPS + 2 * u + k, DRAIN)
                od_send(STEPS + 2 * u + k, DRAIN)

        exchange(1, u + 1, T3[1], T4[1])

        @pl.when(u == 1)
        def _():
            for n in range(NP - T4[0], NCH[0]):
                forward(0, n)

        @pl.when(u == 3)
        def _():
            gathered(0)

        @pl.when(u == 6)
        def _():
            rows = res.at[0, 0:TOK // 2]
            for sem in (s3_send, s3s_send, s4_send):
                pltpu.make_async_copy(rows, rows, sem).wait()
            pltpu.make_async_copy(res.at[0], res.at[0], res_recv).wait()
            pltpu.make_async_copy(res, res_hbm, out_sem.at[2]).start()

        w = jnp.concatenate([wk[:, :W], wv[:, :W], wk[:, W:], wv[:, W:]], axis=1)
        for k in range(2):
            for j in range(2):
                rows = slice(FP * j, FP * (j + 1))
                x = jnp.concatenate([part(u, 2 * k)[rows], part(u, 2 * k + 1)[rows]], axis=1)
                (kv, dkv)[k][u % 2, rows] = dotg(x, w, 1, 1).astype(BF)
        for k in range(2):
            dm_copy(u, k).start()
        return carry

    lax.fori_loop(0, NP // 2, c_step, 0)
    for t in range(NP // 2 + 1, T4[1] + NCH[1]):
        exchange(1, t, T3[1], T4[1])
    gathered(1)
    for k in range(1, 4):
        b_copy(k, (me + k) % 4).wait_recv()
        b_copy(k, me).wait_send()
    big1[0:8, :] = (bias[0, :, 0:W] + bias[1, :, 0:W]) + (bias[2, :, 0:W] + bias[3, :, 0:W])
    big1[8:16, :] = (bias[0, :, W:] + bias[1, :, W:]) + (bias[2, :, W:] + bias[3, :, W:])
    bias_out = pltpu.make_async_copy(big1.at[0:16], bias_hbm, out_sem.at[3])
    bias_out.start()
    for u in (NP // 2 - 2, NP // 2 - 1):
        for k in range(2):
            dm_copy(u, k).wait()
    dw_copy(0).wait()
    dw_copy(1).wait()
    pltpu.make_async_copy(res, res_hbm, out_sem.at[2]).wait()
    bias_out.wait()


def attention(mt, h, dy, w_q, w_o, w_k, w_v, gain, shift, b_q, b_v):
    vm = pl.BlockSpec(memory_space=VMEM)
    hbm = pl.BlockSpec(memory_space=pl.ANY)
    dma = pltpu.SemaphoreType.DMA
    d2, d4, d8, dn = dma((B2,)), dma((B4,)), dma((B8,)), dma((B2, B8))
    credit = pltpu.SemaphoreType.REGULAR((B2,))
    probs, mat, rows32 = VMEM((B2, B4, FP, LANES), F32), VMEM((D, D), BF), VMEM((B4, T, W), F32)
    return pl.pallas_call(
        attn_kernel, name="attention",
        out_shape=(SDS((B2, TOK, D), BF), SDS((B2, D, D), F32), SDS((2 * B8, W), F32), SDS((NP, ROWS, D), BF),
                   SDS((B2, NP, ROWS, D), BF), SDS((B4, B8 * FP, D), BF)),
        in_specs=[hbm] * 7 + [vm] * B4,
        out_specs=(hbm,) * 6,
        scratch_shapes=[
            VMEM((B2, FP, B8, QW), BF), VMEM((QW, QW), BF), VMEM((1, D), F32), VMEM((B2, B8 * FP, D), BF), mat, mat, mat, mat,
            VMEM((3, ROWS, D), BF), probs, probs, VMEM((3, D, ROWS), BF), VMEM((B4, B4, 2 * B8, LANES), F32),
            VMEM((B8, LANES), F32), VMEM((B2, ROWS, D), BF), VMEM((B2, D, D), F32), VMEM((B4, B8, D), F32),
            VMEM((B2, B2, 2 * T, W), F32), VMEM((B4, 2 * T, W), F32), rows32, rows32, VMEM((B8, T, W), F32),
            VMEM((B2, TOK, D), BF), VMEM((D, W), F32), VMEM((B2, D // 2, W), F32),
            d2, d8, d2, dma((B2, B2)), d4, d4, d4, d4, d4, d8, d8, dma, dma((2 * B8,)), dma, dma, dma, d2, d2, dn, dn, dn, dn, dn, dn, d2, d4, d4,
            dma, dma, credit, credit],
        compiler_params=pltpu.CompilerParams(vmem_limit_bytes=67043328, collective_id=0, has_side_effects=True),
    )(mt, h, dy, w_q, w_o, w_k, w_v, gain, shift, b_q, b_v)


def solution(mesh):
    act_spec = P("dp", None, None)
    mem_spec = P("dp", "cp", None)
    vec_out = P("dp")
    mat_out = P("dp", None)
    in_specs = (act_spec, mem_spec, P(), P(), P(), P(), P(), P(), P(), P(), P(), act_spec)
    out_specs = (act_spec, act_spec, mem_spec, vec_out, vec_out, mat_out, vec_out, mat_out, mat_out, vec_out, mat_out, vec_out)

    def device_step(hidden, memory, ln_gain, ln_bias, w_q, b_q, w_k, w_v, b_v, w_o, b_o, grad_y):
        h = hidden.reshape(TOK, D)
        dy = grad_y.reshape(TOK, D)
        res, dw, bias, dm, _, _ = attention(memory.transpose(1, 0, 2), h, dy, w_q, w_o, w_k, w_v, ln_gain, ln_bias, b_q, b_v)
        gm, y, gh, gwo, gwq, gwk, gwv, dg, db, dbq, dbv, dbo = finish(
            dm.reshape(NB, FP, D), res, h, dy, w_o, w_q, dw, bias, ln_gain, ln_bias, b_o)
        return (y.reshape(NB, T, D), gh.reshape(NB, T, D), gm.transpose(1, 0, 2), dg, db, gwq, dbq, gwk, gwv, dbv, gwo, dbo)

    return jax.shard_map(device_step, mesh=mesh, in_specs=in_specs, out_specs=out_specs, check_vma=False)
```

```python
import functools
import math
import jax
import jax.numpy as jnp
from jax import lax
from jax.experimental import pallas as pl
from jax.experimental.pallas import tpu as pltpu
from jax.sharding import PartitionSpec as P

EPS = 1e-5
HEAD = 64
F, FP, D, T = 375, 384, 1024, 32
NB = 32
NP = NB // 2
STEPS = 2 * NP
W = 512
ROWS = 2 * FP
QW = 256
BF, F32 = jnp.bfloat16, jnp.float32
LOG2 = 0.125 * math.log2(math.e)
MESH = pl.DeviceIdType.MESH
VMEM = pltpu.VMEM
B2, B4, B8, LANES = 2, 4, 8, 128
RC = 256
TOK = NB * T
SDS = jax.ShapeDtypeStruct


def dotg(a, b, ca, cb):
    return lax.dot_general(a, b, (((ca,), (cb,)), ((), ())), preferred_element_type=F32)


FC = 32
NFC = FP // FC


def fixed(rows):
    return pl.BlockSpec((rows, D), lambda s: (0, 0), pipeline_mode=pl.Buffered(1))


def lanes(t):
    return slice(LANES * t, LANES * (t + 1))


def permutation(n):
    r = lax.broadcasted_iota(jnp.int32, (QW, QW), 0)
    k = lax.broadcasted_iota(jnp.int32, (QW, QW), 1)
    return (k == r % n * (QW // n) + r // n).astype(F32).astype(BF)


def norm_parts(h):
    centered = h - jnp.mean(h, axis=-1, keepdims=True)
    inv_std = lax.rsqrt(jnp.mean(centered * centered, axis=-1, keepdims=True) + EPS)
    return centered * inv_std, inv_std


JOB0, JOBS = 2, 4
FB = 16
NFB = FP // FB


def finish_kernel(dm_hbm, res_hbm, h_hbm, dy_hbm, wo_hbm, wq_hbm, dw_hbm, bias, gain, shift, bo,
                  gm_hbm, y_hbm, gh_hbm, gwo_hbm, gwq_hbm, gwk_hbm, gwv_hbm, dg, db, dbq, dbv, dbo,
                  src, dst, perm, res, h, dy, wo, wq, x, y, gh, gw, stage, sums,
                  src_sem, dst_sem, in_sem, y_sem, gh_sem, gw_sem, ld_sem, st_sem):
    loads = [pltpu.make_async_copy(a, b, in_sem.at[k]) for k, (a, b) in enumerate(
        ((h_hbm, h), (res_hbm, res), (wo_hbm, wo), (dy_hbm, dy), (wq_hbm, wq)))]

    def src_copy(s):
        return pltpu.make_async_copy(dm_hbm.at[:, pl.ds(pl.multiple_of(FB * s, FB), FB)], src.at[s % B4], src_sem.at[s % B4])

    def dst_copy(s):
        return pltpu.make_async_copy(dst.at[s % B4], gm_hbm.at[pl.ds(FB * s, FB)], dst_sem.at[s % B4])

    def last_copy():
        s = NFB - 1
        return pltpu.make_async_copy(dst.at[s % B4, 0:F - FB * s], gm_hbm.at[FB * s:F], dst_sem.at[s % B4])

    def rows(n):
        return pl.ds(pl.multiple_of(RC * n, RC), RC)

    def out_copy(a, b, sem, n):
        return pltpu.make_async_copy(a.at[rows(n)], b.at[rows(n)], sem.at[n])

    def gw_copy(b, n):
        return pltpu.make_async_copy(gw.at[n], b.at[rows(n)], gw_sem.at[n])

    def piece_in(k):
        g, v = k // 2, k % 2
        return pltpu.make_async_copy(dw_hbm.at[g, :, pl.ds(W * v, W)], stage.at[v], ld_sem.at[v])

    def piece_out(k):
        g, v = k // 2, k % 2
        return pltpu.make_async_copy(stage.at[v], (gwk_hbm, gwv_hbm)[v].at[:, pl.ds(W * g, W)], st_sem.at[v])

    def vec(ref):
        return ref[...].astype(F32).reshape(1, D)

    def move(s):
        for k in range(NB // FB):
            z = src[s % B4, FB * k:FB * (k + 1)].reshape(QW, D)
            z = jnp.dot(perm[...], z, preferred_element_type=F32)
            dst[s % B4, :, FB * k:FB * (k + 1), :] = z.astype(BF).reshape(FB, FB, D)

    def job_y(n):
        hf = h[rows(n)].astype(F32)
        x_hat, _ = norm_parts(hf)
        x[rows(n)] = (x_hat * vec(gain) + vec(shift)).astype(BF)
        y[rows(n)] = (hf + jnp.dot(res[0, rows(n)], wo[...], preferred_element_type=F32) + vec(bo)).astype(BF)

    def job_wo(n):
        gw[n] = dotg(res[0, :, rows(n)], dy[...], 0, 0)

    def job_h(n):
        x_hat, inv_std = norm_parts(h[rows(n)].astype(F32))
        dyf = dy[rows(n)].astype(F32)
        d_x = dotg(res[1, rows(n)], wq[...], 1, 1)
        for k, a in enumerate((d_x * x_hat, d_x, dyf)):
            sums[k:k + 1] += jnp.sum(a, axis=0, keepdims=True)
        d_hat = d_x * vec(gain)
        d_h = inv_std * (d_hat - jnp.mean(d_hat, axis=-1, keepdims=True) - x_hat * jnp.mean(d_hat * x_hat, axis=-1, keepdims=True))
        gh[rows(n)] = (dyf + d_h).astype(BF)

    def job_wq(n):
        gw[n] = dotg(x[:, rows(n)], res[1], 0, 0)

    for k in range(B4 - 1):
        src_copy(k).start()
    for cp in loads:
        cp.start()
    piece_in(0).start()
    piece_in(1).start()
    sums[...] = jnp.zeros_like(sums)
    perm[...] = permutation(FB)
    for ref, k in ((dbq, 0), (dbv, B8)):
        ref[...] = jnp.concatenate([bias[k:k + 1], bias[k + 1:k + 2]], axis=1).reshape(D)
    outs = ((job_y, lambda n: out_copy(y, y_hbm, y_sem, n)), (job_wo, lambda n: gw_copy(gwo_hbm, n)),
            (job_h, lambda n: out_copy(gh, gh_hbm, gh_sem, n)), (job_wq, lambda n: gw_copy(gwq_hbm, n)))
    needs = (loads[:3], loads[3:4], loads[4:], ())

    def step(s, carry):
        src_copy(s).wait()

        @pl.when(s + B4 - 1 < NFB)
        def _():
            src_copy(s + B4 - 1).start()

        @pl.when(s >= B4)
        def _():
            dst_copy(s - B4).wait()

        job = s - JOB0
        n = job % JOBS
        for kind, (f, copy) in enumerate(outs):
            @pl.when((job >= kind * JOBS) & (job < (kind + 1) * JOBS))
            def _():
                if needs[kind]:
                    @pl.when(n == 0)
                    def _():
                        for cp in needs[kind]:
                            cp.wait()
                if kind == 3:
                    gw_copy(gwo_hbm, n).wait()
                move(s)
                f(n)
                copy(n).start()

        @pl.when((job < 0) | (job >= JOBS * JOBS))
        def _():
            move(s)

        @pl.when(s < NFB - 1)
        def _():
            dst_copy(s).start()

        for v in range(2):
            @pl.when(s == JOBS + v)
            def _():
                piece_in(v).wait()
                piece_out(v).start()

            @pl.when(s == B8 + v)
            def _():
                piece_out(v).wait()
                piece_in(v + 2).start()

            @pl.when(s == B8 + JOBS + v)
            def _():
                piece_in(v + 2).wait()
                piece_out(v + 2).start()
        return carry

    lax.fori_loop(0, NFB, step, 0)
    last_copy().start()
    for k, ref in enumerate((dg, db, dbo)):
        ref[...] = sums[k:k + 1].reshape(D)
    for k in range(JOBS):
        out_copy(y, y_hbm, y_sem, k).wait()
        out_copy(gh, gh_hbm, gh_sem, k).wait()
        gw_copy(gwq_hbm, k).wait()
    piece_out(2).wait()
    piece_out(3).wait()
    for k in range(2, JOBS + 1):
        dst_copy(NFB - k).wait()
    last_copy().wait()


def finish(dm, res, h, dy, w_o, w_q, dw, bias, gain, shift, b_o):
    hbm, vm = pl.BlockSpec(memory_space=pl.ANY), pl.BlockSpec(memory_space=VMEM)
    dma = pltpu.SemaphoreType.DMA
    mat, dj, d2, vec = VMEM((D, D), BF), dma((JOBS,)), dma((B2,)), SDS((D,), F32)
    return pl.pallas_call(
        finish_kernel, name="finish",
        out_shape=(SDS((F, NB, D), BF), SDS((TOK, D), BF), SDS((TOK, D), BF)) + (SDS((D, D), F32),) * B4 + (vec,) * (B4 + 1),
        in_specs=[hbm] * (B8 - 1) + [vm] * B4,
        out_specs=(hbm,) * (B8 - 1) + (vm,) * (B4 + 1),
        scratch_shapes=[
            VMEM((B4, NB, FB, D), BF), VMEM((B4, FB, NB, D), BF), VMEM((QW, QW), BF), VMEM((B2, TOK, D), BF), mat, mat, mat, mat, mat,
            mat, mat, VMEM((JOBS, RC, D), F32), VMEM((B2, D, W), F32), VMEM((B8, D), F32), dj, dj, dma((B8,)), dj, dj, dj, d2, d2],
        compiler_params=pltpu.CompilerParams(vmem_limit_bytes=67043328),
    )(dm, res, h, dy, w_o, w_q, dw, bias, gain, shift, b_o)


def block_mask():
    return lax.broadcasted_iota(jnp.int32, (128, 256), 0) // T == lax.broadcasted_iota(jnp.int32, (128, 256), 1) // HEAD


def block_diag(x, mask):
    return jnp.where(mask, jnp.concatenate([x] * 4, axis=0), jnp.zeros((), BF))


def when(cond):
    if isinstance(cond, bool):
        return (lambda f: f()) if cond else (lambda f: None)
    return pl.when(cond)


CH = (64, 128)
NCH = tuple(D // 2 // rows for rows in CH)
T3, T4 = 4, 8


ALL, FILL, DRAIN = range(3)


def attn_kernel(m_hbm, h_hbm, dy_hbm, wq_hbm, wo_hbm, wk_hbm, wv_hbm, gain, shift, bq, bv,
                res_hbm, dw_hbm, bias_hbm, dm_hbm, dkv_hbm, mp_hbm,
                raw, perm, bv32, frames, q, do, wk, wv, kv, e_s, dp_s, mt, stats, coef, dkv, acc, bias, od, r1, keep, x2, r2, res, big1, big2,
                raw_sem, in_sem, dkv_sem, dm_sem, out_sem, st_send, st_recv, s1_send, s1_recv, s2_send, s2_recv,
                s3_send, s3_recv, s3s_send, s4_send, res_recv, e1_send, e1_recv, e2_send, e2_recv,
                e3_send, e3_recv, e3s_send, e4_send, acc_recv, b_send, b_recv, keep_sem, load_sem, free_sib, free_xn):
    me = lax.axis_index("cp")
    cx, cc = me // 2, me % 2
    sib, xn = 2 * cx + 1 - cc, 2 * (1 - cx) + cc

    def vec(ref):
        return ref[...].astype(F32).reshape(1, D)

    def remote(src, dst, ss, rs, dev):
        return pltpu.make_async_remote_copy(src_ref=src, dst_ref=dst, send_sem=ss, recv_sem=rs,
                                            device_id={"cp": dev}, device_id_type=MESH)

    def raw_copy(c):
        seqs = pl.ds(pl.multiple_of(B8 * (c // B4 % B4), B8), B8)
        return pltpu.make_async_copy(m_hbm.at[:, seqs, quarter(c)], raw.at[c % 2, 0:F], raw_sem.at[c % 2])

    def quarter(c):
        return pl.ds(pl.multiple_of(c % B4 * QW, QW), QW)

    def sort_frames(c):
        for n in range(NFC):
            x = raw[c % 2, FC * n:FC * (n + 1)].reshape(QW, QW)
            y = jnp.dot(perm[...], x, preferred_element_type=F32).astype(BF)
            for b in range(B8):
                frames[c // B4 % 2, FP * b + FC * n:FP * b + FC * (n + 1), quarter(c)] = y[FC * b:FC * (b + 1)]

    def dkv_copy(i):
        return pltpu.make_async_copy(dkv.at[i % 2], dkv_hbm.at[i // NP, i % NP], dkv_sem.at[i % 2])

    def stat_send(i):
        for k in range(1, B4):
            remote(stats.at[i % B4, me], stats.at[i % B4, me], st_send.at[i % B4], st_recv.at[i % B4], (me + k) % B4).start()

    def stat_wait(i):
        three = stats.at[i % B4, 0:3]
        for sem in (st_recv, st_send):
            pltpu.make_async_copy(three, three, sem.at[i % B4]).wait()

    def s1(b):
        return remote(od.at[b % 2, 1 - cc], r1.at[b % 4], s1_send.at[b % 4], s1_recv.at[b % 4], sib)

    def s2(b):
        return remote(x2.at[b % 4], r2.at[b % 8], s2_send.at[b % 8], s2_recv.at[b % 8], xn)

    def res_at(b, x):
        return res.at[cc, pl.ds(pl.multiple_of(64 * (b % NP) + T * x, T), T), pl.ds(pl.multiple_of(W * (b // NP), W), W)]

    def s3(b, x):
        return remote(res_at(b, x), res_at(b, x), s3_send, s3_recv.at[b % (2 * B8)], xn)

    def s3s(b):
        return remote(res_at(b, cx), res_at(b, cx), s3s_send, res_recv, sib)

    def s4(b):
        return remote(res_at(b, 1 - cx), res_at(b, 1 - cx), s4_send, res_recv, sib)

    def on(mode, b, k):
        return True if mode == ALL else b >= k if mode == FILL else b - k < STEPS

    def od_wait(b, mode):
        @when(on(mode, b, 8))
        def _():
            s3(b - 8, 1 - cx).wait_recv()

        @when(on(mode, b, 5))
        def _():
            s2(b - 5).wait_recv()
            s2(b - 5).wait_send()

        @when(on(mode, b, 2))
        def _():
            s1(b - 2).wait_send()
            s1(b - 2).wait_recv()

    def od_sum(b, mode):
        @when(on(mode, b, 5))
        def _():
            res_at(b - 5, cx)[...] = (keep[(b - 5) % B4] + r2[(b - 5) % B8]).astype(BF)

        @when(on(mode, b, 2))
        def _():
            for ref, x in ((keep, cx), (x2, 1 - cx)):
                rows = pl.ds(pl.multiple_of(T * x, T), T)
                ref[(b - 2) % B4] = od[b % 2, cc, rows, :] + r1[(b - 2) % B4, rows, :]

    def od_send(b, mode):
        @when(on(mode, b, 2))
        def _():
            s2(b - 2).start()

        @when(on(mode, b, 5))
        def _():
            s3(b - 5, cx).start()
            s3s(b - 5).start()

        @when(on(mode, b, 8))
        def _():
            s4(b - 8).start()

    own = pl.ds(pl.multiple_of(W * cc, W), W)
    other = pl.ds(pl.multiple_of(W * (1 - cc), W), W)

    def rows_of(g, x, n):
        return pl.ds(pl.multiple_of(x * (D // 2) + CH[g] * n, CH[g]), CH[g])

    def chunk_of(g, n):
        return big2.at[g, pl.ds(pl.multiple_of(CH[g] * n, CH[g]), CH[g])]

    def e1(g):
        return remote(acc.at[g, :, other], big1, e1_send.at[g], e1_recv.at[g], sib)

    def e2(g, n):
        return remote(acc.at[g, rows_of(g, 1 - cx, n), own], chunk_of(g, n), e2_send.at[g, n], e2_recv.at[g, n], xn)

    def e3(g, n, x):
        ref = acc.at[g, rows_of(g, x, n), own]
        return remote(ref, ref, e3_send.at[g, n], e3_recv.at[g, n], xn)

    def to_sib(g, n, x, sem):
        ref = acc.at[g, rows_of(g, x, n), own]
        return remote(ref, ref, sem.at[g, n], acc_recv.at[g], sib)

    def dw_copy(g):
        return pltpu.make_async_copy(acc.at[g], dw_hbm.at[g], out_sem.at[g])

    def reduce_core(g, n):
        for x in (cx, 1 - cx):
            acc[g, rows_of(g, x, n), own] += big1[rows_of(g, x, n), :]
        e2(g, n).start()

    def sent(g, n):
        e2(g, n).wait_send()
        pl.semaphore_signal(free_xn.at[g], inc=1, device_id={"cp": xn}, device_id_type=MESH)

    def reduce_chip(g, n):
        e2(g, n).wait_recv()
        pl.semaphore_wait(free_xn.at[g], 1)
        acc[g, rows_of(g, cx, n), own] += chunk_of(g, n)[...]
        e3(g, n, cx).start()
        to_sib(g, n, cx, e3s_send).start()

    def forward(g, n):
        e3(g, n, 1 - cx).wait_recv()
        to_sib(g, n, 1 - cx, e4_send).start()

    def gathered(g):
        half = acc.at[g, :, other]
        remote(half, half, e1_send.at[g], acc_recv.at[g], sib).wait_recv()
        for n in range(NCH[g]):
            e3(g, n, cx).wait_send()
            to_sib(g, n, cx, e3s_send).wait_send()
            to_sib(g, n, 1 - cx, e4_send).wait_send()
        dw_copy(g).start()

    def exchange(g, t, t3, t4):
        def chunk(t0, f):
            n = t - t0
            if isinstance(n, int):
                if 0 <= n < NCH[g]:
                    f(g, n)
            else:
                pl.when((n >= 0) & (n < NCH[g]))(lambda: f(g, n))

        @when(t == 0)
        def _():
            e1(g).start()

        @when(t == 1)
        def _():
            e1(g).wait_send()
            pl.semaphore_signal(free_sib.at[g], inc=1, device_id={"cp": sib}, device_id_type=MESH)
            e1(g).wait_recv()

        @when(t == t3)
        def _():
            pl.semaphore_wait(free_sib.at[g], 1)

        chunk(1, reduce_core)
        chunk(t3 - 1, sent)
        chunk(t3, reduce_chip)
        chunk(t4, forward)

    def exchange_first(t):
        @pl.when(t == 0)
        def _():
            e1(0).start()

        @pl.when(t == 1)
        def _():
            e1(0).wait_send()
            pl.semaphore_signal(free_sib.at[0], inc=1, device_id={"cp": sib}, device_id_type=MESH)
            e1(0).wait_recv()

        @pl.when((t >= 1) & (t < 12) & (t % 3 != 0))
        def _():
            reduce_core(0, t - 1 - t // 3)

        @pl.when((t >= 5) & (t < 13))
        def _():
            sent(0, t - 5)

        @pl.when(t >= 12)
        def _():
            @pl.when(t == 12)
            def _():
                pl.semaphore_wait(free_sib.at[0], 1)
            reduce_chip(0, t - 12)

    def operands(i, j, h):
        cols = pl.ds(pl.multiple_of(W * (i // NP) + 256 * h, 256), 256)
        rows = pl.ds(pl.multiple_of(64 * (i % NP) + T * j, T), T)
        mask = block_mask()
        return block_diag(q[rows, cols], mask), block_diag(do[rows, cols], mask), mask

    def rows_of_pair(i):
        return frames[i // B4 % 2, pl.ds(pl.multiple_of(i % B4 * ROWS, ROWS), ROWS), :]

    def project(i):
        cols = pl.ds(pl.multiple_of(W * (i // NP), W), W)
        m = rows_of_pair(i)
        kv[i % 3, :, 0:W] = jnp.dot(m, wk[:, cols], preferred_element_type=F32).astype(BF)
        kv[i % 3, :, W:] = (jnp.dot(m, wv[:, cols], preferred_element_type=F32) + bv32[:, cols]).astype(BF)
        mt[i % 3] = m.T

    def scores(i):
        slot = i % 2
        real = lax.broadcasted_iota(jnp.int32, (FP, LANES), 0) < F
        for j in range(2):
            rows = slice(FP * j, FP * (j + 1))
            for h in range(2):
                n = 2 * j + h
                qb, db, _ = operands(i, j, h)
                s = dotg(kv[i % 3, rows, QW * h:QW * (h + 1)], qb, 1, 1)
                dp = dotg(kv[i % 3, rows, W + QW * h:W + QW * (h + 1)], db, 1, 1)
                s = jnp.where(real, s, -1e30)
                top = jnp.max(s, axis=0, keepdims=True)
                e = jnp.exp2((s - top) * LOG2)
                e_s[slot, n] = e
                dp_s[slot, n] = dp
                for k, row in enumerate((top, jnp.sum(e, axis=0, keepdims=True), jnp.sum(e * dp, axis=0, keepdims=True))):
                    stats[i % B4, me, B4 * k + n:B4 * k + n + 1, :] = row

    def combine(i):
        slot = i % 4
        tops = [stats[slot, d, 0:4, :] for d in range(4)]
        top = jnp.maximum(jnp.maximum(tops[0], tops[1]), jnp.maximum(tops[2], tops[3]))
        ws = [jnp.exp2((t - top) * LOG2) for t in tops]
        total = sum(stats[slot, d, 4:8, :] * ws[d] for d in range(4))
        dots = sum(stats[slot, d, 8:12, :] * ws[d] for d in range(4))
        coef[0:4, :] = jnp.exp2((stats[slot, me, 0:4, :] - top) * LOG2) / total
        coef[4:8, :] = dots / total

    def grads(i):
        slot, grp = i % 2, i // NP
        blocks = []
        for j in range(2):
            rows = slice(FP * j, FP * (j + 1))
            for h in range(2):
                n = 2 * j + h
                qb, db, _ = operands(i, j, h)
                ck, cv = slice(QW * h, QW * (h + 1)), slice(W + QW * h, W + QW * (h + 1))
                p = e_s[slot, n] * coef[n:n + 1, :]
                pb = p.astype(BF)
                gb = (p * (dp_s[slot, n] - coef[B4 + n:B4 + n + 1, :]) * 0.125).astype(BF)
                dk = jnp.dot(gb, qb, preferred_element_type=F32)
                dv = jnp.dot(pb, db, preferred_element_type=F32)
                dkv[slot, rows, ck] = dk.astype(BF)
                dkv[slot, rows, cv] = dv.astype(BF)
                bias[me, pl.ds(grp, 1), cv] += jnp.sum(dv, axis=0, keepdims=True)
                blocks.append((j, h, pb, gb))
        return blocks

    def sums(i, blocks):
        mask = block_mask()
        for j, h, pb, gb in blocks:
            rows = slice(FP * j, FP * (j + 1))
            ck, cv = slice(QW * h, QW * (h + 1)), slice(W + QW * h, W + QW * (h + 1))
            for which, x in ((0, dotg(pb, kv[i % 3, rows, cv], 0, 0)), (1, dotg(gb, kv[i % 3, rows, ck], 0, 0))):
                x = jnp.where(mask, x, 0.0)
                x = (x[0:32] + x[32:64]) + (x[64:96] + x[96:128])
                od[i % 2, which, T * j:T * (j + 1), ck] = x
                if which == 1:
                    bias[me, pl.ds(i // NP, 1), ck] += jnp.sum(x, axis=0, keepdims=True)

    def keep_copy(n):
        return pltpu.make_async_copy(frames.at[n % 2], mp_hbm.at[n % B4], keep_sem)

    def load_copy(n):
        return pltpu.make_async_copy(mp_hbm.at[n % B4], frames.at[n % 2], load_sem)

    def tiles(i, do_sort):
        n = i // B4
        if do_sort:
            raw_copy(i + B4).wait()

            @pl.when(i + B4 + 1 < NP)
            def _():
                raw_copy(i + B4 + 1).start()

        @pl.when(i % B4 == 0)
        def _():
            @pl.when((n >= 1) & (n <= B4))
            def _():
                keep_copy(n - 1).wait()

            @pl.when(n < B4)
            def _():
                keep_copy(n).start()

            if not do_sort:
                @pl.when(n >= B4)
                def _():
                    load_copy(n).wait()

                @pl.when((n >= B4 - 1) & (n < B8 - 1))
                def _():
                    load_copy(n + 1).start()

    def step(i, do_a, do_b, do_sort, mode):
        b = i - 2
        if do_b:
            @pl.when(b >= NP)
            def _():
                exchange_first(b - NP)

            stat_wait(b)

            @when(on(mode, b, 2))
            def _():
                dkv_copy(b - 2).wait()

            od_wait(b, mode)
        if do_a:
            tiles(i, do_sort)
        if do_b:
            od_sum(b, mode)
            combine(b)
        if do_a:
            project(i)
        if do_b:
            blocks = grads(b)
        if do_a:
            scores(i)
            if do_sort:
                sort_frames(i + B4)
        if do_b:
            acc[b // NP] += jnp.dot(mt[b % 3], dkv[b % 2], preferred_element_type=F32)
            sums(b, blocks)
        if do_a:
            stat_send(i)
        if do_b:
            dkv_copy(b).start()
            s1(b).start()
            od_send(b, mode)

    barrier = pltpu.get_barrier_semaphore()
    for k in range(1, B4):
        pl.semaphore_signal(barrier, inc=1, device_id={"cp": (me + k) % B4}, device_id_type=MESH)
    top, low = pl.ds(0, ROWS), pl.ds(ROWS, D - ROWS)
    rest = pl.ds(0, D - ROWS)
    loads = [pltpu.make_async_copy(x, y, in_sem.at[k]) for k, (x, y) in enumerate((
        (h_hbm, res.at[0]), (wq_hbm.at[top], kv.at[0]), (wq_hbm.at[low], dkv.at[0, rest]), (dy_hbm, res.at[1]),
        (wo_hbm.at[top], kv.at[1]), (wo_hbm.at[low], dkv.at[1, rest]), (wk_hbm, wk), (wv_hbm, wv)))]
    raw_copy(0).start()
    for cp in loads:
        cp.start()
    raw[:, F:] = jnp.zeros((B2, FP - F, B8, QW), BF)
    perm[...] = permutation(FC)
    bv32[...] = vec(bv)
    bias[me] = jnp.zeros((B8, D), F32)
    for cp in loads[:3]:
        cp.wait()

    def first(n, carry):
        rows = pl.ds(pl.multiple_of(RC * n, RC), RC)
        x_hat, _ = norm_parts(res[0, rows].astype(F32))
        x = (x_hat * vec(gain) + vec(shift)).astype(BF)
        q[rows] = (jnp.dot(x[:, :ROWS], kv[0], preferred_element_type=F32)
                   + jnp.dot(x[:, ROWS:], dkv[0, rest], preferred_element_type=F32) + vec(bq)).astype(BF)
        for g in range(2):
            acc[g, rows] = jnp.zeros((RC, D), F32)
        return carry

    def second(n, carry):
        raw_copy(n).wait()
        raw_copy(n + 1).start()
        rows = pl.ds(pl.multiple_of(RC * n, RC), RC)
        sort_frames(n)
        do[rows, :ROWS] = dotg(res[1, rows], kv[1], 1, 1).astype(BF)
        do[rows, ROWS:] = dotg(res[1, rows], dkv[1, rest], 1, 1).astype(BF)
        return carry

    lax.fori_loop(0, TOK // RC, first, 0)
    for cp in loads[3:-2]:
        cp.wait()
    lax.fori_loop(0, TOK // RC, second, 0)
    for cp in loads[-2:]:
        cp.wait()
    pl.semaphore_wait(barrier, 3)

    def run(lo, hi, *what):
        def body(i, carry):
            step(i, *what)
            return carry
        lax.fori_loop(lo, hi, body, 0)

    run(0, 2, True, False, True, FILL)
    run(2, NP - B4, True, True, True, FILL)
    run(NP - B4, STEPS, True, True, False, ALL)
    run(STEPS, STEPS + 2, False, True, False, ALL)

    def b_copy(k, src):
        return remote(bias.at[src], bias.at[src], b_send.at[k - 1], b_recv.at[src], (me + k) % 4)

    for k in range(1, 4):
        b_copy(k, me).start()
    dkv_copy(STEPS - 2).wait()
    dkv_copy(STEPS - 1).wait()

    def part(u, k):
        return frames.at[u % 2, pl.ds(ROWS * k, ROWS)]

    def c_load(u, k):
        return pltpu.make_async_copy(dkv_hbm.at[k % 2, 2 * u + k // 2], part(u, k), in_sem.at[k])

    def dm_copy(u, k):
        return pltpu.make_async_copy((kv, dkv)[k].at[u % 2], dm_hbm.at[2 * u + k], dm_sem.at[k, u % 2])

    for k in range(B4):
        c_load(0, k).start()
    exchange(1, 0, T3, T4)

    def c_step(u, carry):
        for k in range(B4):
            c_load(u, k).wait()

        @pl.when(u + 1 < NP // 2)
        def _():
            for k in range(B4):
                c_load(u + 1, k).start()

        @pl.when(u >= 2)
        def _():
            for k in range(2):
                dm_copy(u - 2, k).wait()

        @pl.when(u < B4)
        def _():
            for k in range(2):
                od_wait(STEPS + 2 * u + k, DRAIN)
                od_sum(STEPS + 2 * u + k, DRAIN)
                od_send(STEPS + 2 * u + k, DRAIN)

        for v in range(2):
            @pl.when(u == v)
            def _():
                for k in range(2):
                    reduce_chip(0, B4 + 2 * v + k)

            @pl.when(u == 1 + 2 * v)
            def _():
                for n in range(B4):
                    forward(0, B4 * v + n)

        @pl.when(u == 5)
        def _():
            gathered(0)

        exchange(1, u + 1, T3, T4)

        @pl.when(u == 6)
        def _():
            rows = res.at[0, 0:TOK // 2]
            for sem in (s3_send, s3s_send, s4_send):
                pltpu.make_async_copy(rows, rows, sem).wait()
            pltpu.make_async_copy(res.at[0], res.at[0], res_recv).wait()
            pltpu.make_async_copy(res, res_hbm, out_sem.at[2]).start()

        w = jnp.concatenate([wk[:, :W], wv[:, :W], wk[:, W:], wv[:, W:]], axis=1)
        for k in range(2):
            for j in range(2):
                rows = slice(FP * j, FP * (j + 1))
                x = jnp.concatenate([part(u, 2 * k)[rows], part(u, 2 * k + 1)[rows]], axis=1)
                (kv, dkv)[k][u % 2, rows] = dotg(x, w, 1, 1).astype(BF)
        for k in range(2):
            dm_copy(u, k).start()
        return carry

    lax.fori_loop(0, NP // 2, c_step, 0)
    for t in range(NP // 2 + 1, T4 + NCH[1]):
        exchange(1, t, T3, T4)
    gathered(1)
    for k in range(1, 4):
        b_copy(k, (me + k) % 4).wait_recv()
        b_copy(k, me).wait_send()
    big1[0:8, :] = (bias[0, :, 0:W] + bias[1, :, 0:W]) + (bias[2, :, 0:W] + bias[3, :, 0:W])
    big1[8:16, :] = (bias[0, :, W:] + bias[1, :, W:]) + (bias[2, :, W:] + bias[3, :, W:])
    bias_out = pltpu.make_async_copy(big1.at[0:16], bias_hbm, out_sem.at[3])
    bias_out.start()
    for u in (NP // 2 - 2, NP // 2 - 1):
        for k in range(2):
            dm_copy(u, k).wait()
    dw_copy(0).wait()
    dw_copy(1).wait()
    pltpu.make_async_copy(res, res_hbm, out_sem.at[2]).wait()
    bias_out.wait()


def attention(mt, h, dy, w_q, w_o, w_k, w_v, gain, shift, b_q, b_v):
    vm = pl.BlockSpec(memory_space=VMEM)
    hbm = pl.BlockSpec(memory_space=pl.ANY)
    dma = pltpu.SemaphoreType.DMA
    d2, d4, d8, dn = dma((B2,)), dma((B4,)), dma((B8,)), dma((B2, B8))
    credit = pltpu.SemaphoreType.REGULAR((B2,))
    probs, mat, rows32 = VMEM((B2, B4, FP, LANES), F32), VMEM((D, D), BF), VMEM((B4, T, W), F32)
    return pl.pallas_call(
        attn_kernel, name="attention",
        out_shape=(SDS((B2, TOK, D), BF), SDS((B2, D, D), F32), SDS((2 * B8, W), F32), SDS((NP, ROWS, D), BF),
                   SDS((B2, NP, ROWS, D), BF), SDS((B4, B8 * FP, D), BF)),
        in_specs=[hbm] * 7 + [vm] * B4,
        out_specs=(hbm,) * 6,
        scratch_shapes=[
            VMEM((B2, FP, B8, QW), BF), VMEM((QW, QW), BF), VMEM((1, D), F32), VMEM((B2, B8 * FP, D), BF), mat, mat, mat, mat,
            VMEM((3, ROWS, D), BF), probs, probs, VMEM((3, D, ROWS), BF), VMEM((B4, B4, 2 * B8, LANES), F32),
            VMEM((B8, LANES), F32), VMEM((B2, ROWS, D), BF), VMEM((B2, D, D), F32), VMEM((B4, B8, D), F32),
            VMEM((B2, B2, 2 * T, W), F32), VMEM((B4, 2 * T, W), F32), rows32, rows32, VMEM((B8, T, W), F32),
            VMEM((B2, TOK, D), BF), VMEM((D, W), F32), VMEM((B2, D // 2, W), F32),
            d2, d8, d2, dma((B2, B2)), d4, d4, d4, d4, d4, d8, d8, dma, dma((2 * B8,)), dma, dma, dma, d2, d2, dn, dn, dn, dn, dn, dn, d2, d4, d4,
            dma, dma, credit, credit],
        compiler_params=pltpu.CompilerParams(vmem_limit_bytes=67043328, collective_id=0, has_side_effects=True),
    )(mt, h, dy, w_q, w_o, w_k, w_v, gain, shift, b_q, b_v)


def solution(mesh):
    act_spec = P("dp", None, None)
    mem_spec = P("dp", "cp", None)
    vec_out = P("dp")
    mat_out = P("dp", None)
    in_specs = (act_spec, mem_spec, P(), P(), P(), P(), P(), P(), P(), P(), P(), act_spec)
    out_specs = (act_spec, act_spec, mem_spec, vec_out, vec_out, mat_out, vec_out, mat_out, mat_out, vec_out, mat_out, vec_out)

    def device_step(hidden, memory, ln_gain, ln_bias, w_q, b_q, w_k, w_v, b_v, w_o, b_o, grad_y):
        h = hidden.reshape(TOK, D)
        dy = grad_y.reshape(TOK, D)
        res, dw, bias, dm, _, _ = attention(memory.transpose(1, 0, 2), h, dy, w_q, w_o, w_k, w_v, ln_gain, ln_bias, b_q, b_v)
        gm, y, gh, gwo, gwq, gwk, gwv, dg, db, dbq, dbv, dbo = finish(
            dm.reshape(NB, FP, D), res, h, dy, w_o, w_q, dw, bias, ln_gain, ln_bias, b_o)
        return (y.reshape(NB, T, D), gh.reshape(NB, T, D), gm.transpose(1, 0, 2), dg, db, gwq, dbq, gwk, gwv, dbv, gwo, dbo)

    return jax.shard_map(device_step, mesh=mesh, in_specs=in_specs, out_specs=out_specs, check_vma=False)
```

```python
import functools
import math
import jax
import jax.numpy as jnp
from jax import lax
from jax.experimental import pallas as pl
from jax.experimental.pallas import tpu as pltpu
from jax.sharding import PartitionSpec as P

EPS = 1e-5
HEAD = 64
F, FP, D, T = 375, 384, 1024, 32
NB = 32
NP = NB // 2
STEPS = 2 * NP
W = 512
ROWS = 2 * FP
QW = 256
BF, F32 = jnp.bfloat16, jnp.float32
LOG2 = 0.125 * math.log2(math.e)
MESH = pl.DeviceIdType.MESH
VMEM = pltpu.VMEM
B2, B4, B8, LANES = 2, 4, 8, 128
RC = 256
TOK = NB * T
SDS = jax.ShapeDtypeStruct


def dotg(a, b, ca, cb):
    return lax.dot_general(a, b, (((ca,), (cb,)), ((), ())), preferred_element_type=F32)


FC = 32
NFC = FP // FC


def fixed(rows):
    return pl.BlockSpec((rows, D), lambda s: (0, 0), pipeline_mode=pl.Buffered(1))


def lanes(t):
    return slice(LANES * t, LANES * (t + 1))


def permutation(n):
    r = lax.broadcasted_iota(jnp.int32, (QW, QW), 0)
    k = lax.broadcasted_iota(jnp.int32, (QW, QW), 1)
    return (k == r % n * (QW // n) + r // n).astype(F32).astype(BF)


def norm_parts(h):
    centered = h - jnp.mean(h, axis=-1, keepdims=True)
    inv_std = lax.rsqrt(jnp.mean(centered * centered, axis=-1, keepdims=True) + EPS)
    return centered * inv_std, inv_std


JOB0, JOBS = 6, 4
FB = 16
NFB = FP // FB


def finish_kernel(dm_hbm, res_hbm, h_hbm, dy_hbm, wo_hbm, wq_hbm, dw_hbm, bias, gain, shift, bo,
                  gm_hbm, y_hbm, gh_hbm, gwo_hbm, gwq_hbm, gwk_hbm, gwv_hbm, dg, db, dbq, dbv, dbo,
                  src, dst, perm, res, h, dy, wo, wq, x, y, gh, gw, stage, sums,
                  src_sem, dst_sem, in_sem, y_sem, gh_sem, gw_sem, ld_sem, st_sem):
    loads = [pltpu.make_async_copy(a, b, in_sem.at[k]) for k, (a, b) in enumerate(
        ((h_hbm, h), (res_hbm, res), (wo_hbm, wo), (dy_hbm, dy), (wq_hbm, wq)))]

    def src_copy(s):
        return pltpu.make_async_copy(dm_hbm.at[:, pl.ds(pl.multiple_of(FB * s, FB), FB)], src.at[s % B4], src_sem.at[s % B4])

    def dst_copy(s):
        return pltpu.make_async_copy(dst.at[s % B4], gm_hbm.at[pl.ds(FB * s, FB)], dst_sem.at[s % B4])

    def last_copy():
        s = NFB - 1
        return pltpu.make_async_copy(dst.at[s % B4, 0:F - FB * s], gm_hbm.at[FB * s:F], dst_sem.at[s % B4])

    def rows(n):
        return pl.ds(pl.multiple_of(RC * n, RC), RC)

    def out_copy(a, b, sem, n):
        return pltpu.make_async_copy(a.at[rows(n)], b.at[rows(n)], sem.at[n])

    def gw_copy(b, n):
        return pltpu.make_async_copy(gw.at[n], b.at[rows(n)], gw_sem.at[n])

    def piece_in(k):
        g, v = k // 2, k % 2
        return pltpu.make_async_copy(dw_hbm.at[g, :, pl.ds(W * v, W)], stage.at[v], ld_sem.at[v])

    def piece_out(k):
        g, v = k // 2, k % 2
        return pltpu.make_async_copy(stage.at[v], (gwk_hbm, gwv_hbm)[v].at[:, pl.ds(W * g, W)], st_sem.at[v])

    def vec(ref):
        return ref[...].astype(F32).reshape(1, D)

    def move(s):
        for k in range(NB // FB):
            z = src[s % B4, FB * k:FB * (k + 1)].reshape(QW, D)
            z = jnp.dot(perm[...], z, preferred_element_type=F32)
            dst[s % B4, :, FB * k:FB * (k + 1), :] = z.astype(BF).reshape(FB, FB, D)

    def job_y(n):
        hf = h[rows(n)].astype(F32)
        x_hat, _ = norm_parts(hf)
        x[rows(n)] = (x_hat * vec(gain) + vec(shift)).astype(BF)
        y[rows(n)] = (hf + jnp.dot(res[0, rows(n)], wo[...], preferred_element_type=F32) + vec(bo)).astype(BF)

    def job_wo(n):
        gw[n] = dotg(res[0, :, rows(n)], dy[...], 0, 0)

    def job_h(n):
        x_hat, inv_std = norm_parts(h[rows(n)].astype(F32))
        dyf = dy[rows(n)].astype(F32)
        d_x = dotg(res[1, rows(n)], wq[...], 1, 1)
        for k, a in enumerate((d_x * x_hat, d_x, dyf)):
            sums[k:k + 1] += jnp.sum(a, axis=0, keepdims=True)
        d_hat = d_x * vec(gain)
        d_h = inv_std * (d_hat - jnp.mean(d_hat, axis=-1, keepdims=True) - x_hat * jnp.mean(d_hat * x_hat, axis=-1, keepdims=True))
        gh[rows(n)] = (dyf + d_h).astype(BF)

    def job_wq(n):
        gw[n] = dotg(x[:, rows(n)], res[1], 0, 0)

    for k in range(B4 - 1):
        src_copy(k).start()
    piece_in(0).start()
    piece_in(1).start()
    sums[...] = jnp.zeros_like(sums)
    perm[...] = permutation(FB)
    for ref, k in ((dbq, 0), (dbv, B8)):
        ref[...] = jnp.concatenate([bias[k:k + 1], bias[k + 1:k + 2]], axis=1).reshape(D)
    outs = ((job_y, lambda n: out_copy(y, y_hbm, y_sem, n)), (job_wo, lambda n: gw_copy(gwo_hbm, n)),
            (job_h, lambda n: out_copy(gh, gh_hbm, gh_sem, n)), (job_wq, lambda n: gw_copy(gwq_hbm, n)))
    needs = (loads[:3], loads[3:4], loads[4:], ())

    def step(s, carry):
        src_copy(s).wait()

        @pl.when(s + B4 - 1 < NFB)
        def _():
            src_copy(s + B4 - 1).start()

        @pl.when(s >= B4)
        def _():
            dst_copy(s - B4).wait()

        @pl.when(s == 1)
        def _():
            for cp in loads:
                cp.start()

        job = s - JOB0
        n = job % JOBS
        for kind, (f, copy) in enumerate(outs):
            @pl.when((job >= kind * JOBS) & (job < (kind + 1) * JOBS))
            def _():
                if needs[kind]:
                    @pl.when(n == 0)
                    def _():
                        for cp in needs[kind]:
                            cp.wait()
                if kind == 3:
                    gw_copy(gwo_hbm, n).wait()
                move(s)
                f(n)
                copy(n).start()

        @pl.when((job < 0) | (job >= JOBS * JOBS))
        def _():
            move(s)

        @pl.when(s < NFB - 1)
        def _():
            dst_copy(s).start()

        for v in range(2):
            @pl.when(s == 2 + v)
            def _():
                piece_in(v).wait()
                piece_out(v).start()

            @pl.when(s == JOB0 + v)
            def _():
                piece_out(v).wait()
                piece_in(v + 2).start()

            @pl.when(s == JOB0 + JOBS + v)
            def _():
                piece_in(v + 2).wait()
                piece_out(v + 2).start()
        return carry

    lax.fori_loop(0, NFB, step, 0)
    last_copy().start()
    for k, ref in enumerate((dg, db, dbo)):
        ref[...] = sums[k:k + 1].reshape(D)
    for k in range(JOBS):
        out_copy(y, y_hbm, y_sem, k).wait()
        out_copy(gh, gh_hbm, gh_sem, k).wait()
        gw_copy(gwq_hbm, k).wait()
    piece_out(2).wait()
    piece_out(3).wait()
    for k in range(2, JOBS + 1):
        dst_copy(NFB - k).wait()
    last_copy().wait()


def finish(dm, res, h, dy, w_o, w_q, dw, bias, gain, shift, b_o):
    hbm, vm = pl.BlockSpec(memory_space=pl.ANY), pl.BlockSpec(memory_space=VMEM)
    dma = pltpu.SemaphoreType.DMA
    mat, dj, d2, vec = VMEM((D, D), BF), dma((JOBS,)), dma((B2,)), SDS((D,), F32)
    return pl.pallas_call(
        finish_kernel, name="finish",
        out_shape=(SDS((F, NB, D), BF), SDS((TOK, D), BF), SDS((TOK, D), BF)) + (SDS((D, D), F32),) * B4 + (vec,) * (B4 + 1),
        in_specs=[hbm] * (B8 - 1) + [vm] * B4,
        out_specs=(hbm,) * (B8 - 1) + (vm,) * (B4 + 1),
        scratch_shapes=[
            VMEM((B4, NB, FB, D), BF), VMEM((B4, FB, NB, D), BF), VMEM((QW, QW), BF), VMEM((B2, TOK, D), BF), mat, mat, mat, mat, mat,
            mat, mat, VMEM((JOBS, RC, D), F32), VMEM((B2, D, W), F32), VMEM((B8, D), F32), dj, dj, dma((B8,)), dj, dj, dj, d2, d2],
        compiler_params=pltpu.CompilerParams(vmem_limit_bytes=67043328),
    )(dm, res, h, dy, w_o, w_q, dw, bias, gain, shift, b_o)


def block_mask():
    return lax.broadcasted_iota(jnp.int32, (128, 256), 0) // T == lax.broadcasted_iota(jnp.int32, (128, 256), 1) // HEAD


def block_diag(x, mask):
    return jnp.where(mask, jnp.concatenate([x] * 4, axis=0), jnp.zeros((), BF))


def when(cond):
    if isinstance(cond, bool):
        return (lambda f: f()) if cond else (lambda f: None)
    return pl.when(cond)


CH = (64, 128)
NCH = tuple(D // 2 // rows for rows in CH)
T3, T4 = (8, 4), (11, 6)


ALL, FILL, DRAIN = range(3)


def attn_kernel(m_hbm, h_hbm, dy_hbm, wq_hbm, wo_hbm, wk_hbm, wv_hbm, gain, shift, bq, bv,
                res_hbm, dw_hbm, bias_hbm, dm_hbm, dkv_hbm, mp_hbm,
                raw, perm, bv32, frames, q, do, wk, wv, kv, e_s, dp_s, mt, stats, coef, dkv, acc, bias, od, r1, keep, x2, r2, res, big1, big2,
                raw_sem, in_sem, dkv_sem, dm_sem, out_sem, st_send, st_recv, s1_send, s1_recv, s2_send, s2_recv,
                s3_send, s3_recv, s3s_send, s4_send, res_recv, e1_send, e1_recv, e2_send, e2_recv,
                e3_send, e3_recv, e3s_send, e4_send, acc_recv, b_send, b_recv, keep_sem, load_sem, free_sib, free_xn):
    me = lax.axis_index("cp")
    cx, cc = me // 2, me % 2
    sib, xn = 2 * cx + 1 - cc, 2 * (1 - cx) + cc

    def vec(ref):
        return ref[...].astype(F32).reshape(1, D)

    def remote(src, dst, ss, rs, dev):
        return pltpu.make_async_remote_copy(src_ref=src, dst_ref=dst, send_sem=ss, recv_sem=rs,
                                            device_id={"cp": dev}, device_id_type=MESH)

    def raw_copy(c):
        seqs = pl.ds(pl.multiple_of(B8 * (c // B4 % B4), B8), B8)
        return pltpu.make_async_copy(m_hbm.at[:, seqs, quarter(c)], raw.at[c % 2, 0:F], raw_sem.at[c % 2])

    def quarter(c):
        return pl.ds(pl.multiple_of(c % B4 * QW, QW), QW)

    def sort_frames(c):
        for n in range(NFC):
            x = raw[c % 2, FC * n:FC * (n + 1)].reshape(QW, QW)
            y = jnp.dot(perm[...], x, preferred_element_type=F32).astype(BF)
            for b in range(B8):
                frames[c // B4 % 2, FP * b + FC * n:FP * b + FC * (n + 1), quarter(c)] = y[FC * b:FC * (b + 1)]

    def dkv_copy(i):
        return pltpu.make_async_copy(dkv.at[i % 2], dkv_hbm.at[i // NP, i % NP], dkv_sem.at[i % 2])

    def stat_send(i):
        for k in range(1, B4):
            remote(stats.at[i % B4, me], stats.at[i % B4, me], st_send.at[i % B4], st_recv.at[i % B4], (me + k) % B4).start()

    def stat_wait(i):
        three = stats.at[i % B4, 0:3]
        for sem in (st_recv, st_send):
            pltpu.make_async_copy(three, three, sem.at[i % B4]).wait()

    def s1(b):
        return remote(od.at[b % 2, 1 - cc], r1.at[b % 4], s1_send.at[b % 4], s1_recv.at[b % 4], sib)

    def s2(b):
        return remote(x2.at[b % 4], r2.at[b % 8], s2_send.at[b % 8], s2_recv.at[b % 8], xn)

    def res_at(b, x):
        return res.at[cc, pl.ds(pl.multiple_of(64 * (b % NP) + T * x, T), T), pl.ds(pl.multiple_of(W * (b // NP), W), W)]

    def s3(b, x):
        return remote(res_at(b, x), res_at(b, x), s3_send, s3_recv.at[b % (2 * B8)], xn)

    def s3s(b):
        return remote(res_at(b, cx), res_at(b, cx), s3s_send, res_recv, sib)

    def s4(b):
        return remote(res_at(b, 1 - cx), res_at(b, 1 - cx), s4_send, res_recv, sib)

    def on(mode, b, k):
        return True if mode == ALL else b >= k if mode == FILL else b - k < STEPS

    def od_wait(b, mode):
        @when(on(mode, b, 8))
        def _():
            s3(b - 8, 1 - cx).wait_recv()

        @when(on(mode, b, 5))
        def _():
            s2(b - 5).wait_recv()
            s2(b - 5).wait_send()

        @when(on(mode, b, 2))
        def _():
            s1(b - 2).wait_send()
            s1(b - 2).wait_recv()

    def od_sum(b, mode):
        @when(on(mode, b, 5))
        def _():
            res_at(b - 5, cx)[...] = (keep[(b - 5) % B4] + r2[(b - 5) % B8]).astype(BF)

        @when(on(mode, b, 2))
        def _():
            for ref, x in ((keep, cx), (x2, 1 - cx)):
                rows = pl.ds(pl.multiple_of(T * x, T), T)
                ref[(b - 2) % B4] = od[b % 2, cc, rows, :] + r1[(b - 2) % B4, rows, :]

    def od_send(b, mode):
        @when(on(mode, b, 2))
        def _():
            s2(b - 2).start()

        @when(on(mode, b, 5))
        def _():
            s3(b - 5, cx).start()
            s3s(b - 5).start()

        @when(on(mode, b, 8))
        def _():
            s4(b - 8).start()

    own = pl.ds(pl.multiple_of(W * cc, W), W)
    other = pl.ds(pl.multiple_of(W * (1 - cc), W), W)

    def rows_of(g, x, n):
        return pl.ds(pl.multiple_of(x * (D // 2) + CH[g] * n, CH[g]), CH[g])

    def chunk_of(g, n):
        return big2.at[g, pl.ds(pl.multiple_of(CH[g] * n, CH[g]), CH[g])]

    def e1(g):
        return remote(acc.at[g, :, other], big1, e1_send.at[g], e1_recv.at[g], sib)

    def e2(g, n):
        return remote(acc.at[g, rows_of(g, 1 - cx, n), own], chunk_of(g, n), e2_send.at[g, n], e2_recv.at[g, n], xn)

    def e3(g, n, x):
        ref = acc.at[g, rows_of(g, x, n), own]
        return remote(ref, ref, e3_send.at[g, n], e3_recv.at[g, n], xn)

    def to_sib(g, n, x, sem):
        ref = acc.at[g, rows_of(g, x, n), own]
        return remote(ref, ref, sem.at[g, n], acc_recv.at[g], sib)

    def dw_copy(g):
        return pltpu.make_async_copy(acc.at[g], dw_hbm.at[g], out_sem.at[g])

    def reduce_core(g, n):
        for x in (cx, 1 - cx):
            acc[g, rows_of(g, x, n), own] += big1[rows_of(g, x, n), :]
        e2(g, n).start()

    def sent(g, n):
        e2(g, n).wait_send()
        pl.semaphore_signal(free_xn.at[g], inc=1, device_id={"cp": xn}, device_id_type=MESH)

    def reduce_chip(g, n):
        e2(g, n).wait_recv()
        pl.semaphore_wait(free_xn.at[g], 1)
        acc[g, rows_of(g, cx, n), own] += chunk_of(g, n)[...]
        e3(g, n, cx).start()
        to_sib(g, n, cx, e3s_send).start()

    def forward(g, n):
        e3(g, n, 1 - cx).wait_recv()
        to_sib(g, n, 1 - cx, e4_send).start()

    def gathered(g):
        half = acc.at[g, :, other]
        remote(half, half, e1_send.at[g], acc_recv.at[g], sib).wait_recv()
        for n in range(NCH[g]):
            e3(g, n, cx).wait_send()
            to_sib(g, n, cx, e3s_send).wait_send()
            to_sib(g, n, 1 - cx, e4_send).wait_send()
        dw_copy(g).start()

    def exchange(g, t, t3, t4):
        def chunk(t0, f):
            n = t - t0
            if isinstance(n, int):
                if 0 <= n < NCH[g]:
                    f(g, n)
            else:
                pl.when((n >= 0) & (n < NCH[g]))(lambda: f(g, n))

        @when(t == 0)
        def _():
            e1(g).start()

        @when(t == 1)
        def _():
            e1(g).wait_send()
            pl.semaphore_signal(free_sib.at[g], inc=1, device_id={"cp": sib}, device_id_type=MESH)
            e1(g).wait_recv()

        @when(t == t3)
        def _():
            pl.semaphore_wait(free_sib.at[g], 1)

        chunk(1, reduce_core)
        chunk(t3 - 1, sent)
        chunk(t3, reduce_chip)
        chunk(t4, forward)

    def operands(i, j, h):
        cols = pl.ds(pl.multiple_of(W * (i // NP) + 256 * h, 256), 256)
        rows = pl.ds(pl.multiple_of(64 * (i % NP) + T * j, T), T)
        mask = block_mask()
        return block_diag(q[rows, cols], mask), block_diag(do[rows, cols], mask), mask

    def rows_of_pair(i):
        return frames[i // B4 % 2, pl.ds(pl.multiple_of(i % B4 * ROWS, ROWS), ROWS), :]

    def project(i):
        cols = pl.ds(pl.multiple_of(W * (i // NP), W), W)
        m = rows_of_pair(i)
        kv[i % 3, :, 0:W] = jnp.dot(m, wk[:, cols], preferred_element_type=F32).astype(BF)
        kv[i % 3, :, W:] = (jnp.dot(m, wv[:, cols], preferred_element_type=F32) + bv32[:, cols]).astype(BF)
        mt[i % 3] = m.T

    def scores(i):
        slot = i % 2
        real = lax.broadcasted_iota(jnp.int32, (FP, LANES), 0) < F
        for j in range(2):
            rows = slice(FP * j, FP * (j + 1))
            for h in range(2):
                n = 2 * j + h
                qb, db, _ = operands(i, j, h)
                s = dotg(kv[i % 3, rows, QW * h:QW * (h + 1)], qb, 1, 1)
                dp = dotg(kv[i % 3, rows, W + QW * h:W + QW * (h + 1)], db, 1, 1)
                s = jnp.where(real, s, -1e30)
                top = jnp.max(s, axis=0, keepdims=True)
                e = jnp.exp2((s - top) * LOG2)
                e_s[slot, n] = e
                dp_s[slot, n] = dp
                for k, row in enumerate((top, jnp.sum(e, axis=0, keepdims=True), jnp.sum(e * dp, axis=0, keepdims=True))):
                    stats[i % B4, me, B4 * k + n:B4 * k + n + 1, :] = row

    def combine(i):
        slot = i % 4
        tops = [stats[slot, d, 0:4, :] for d in range(4)]
        top = jnp.maximum(jnp.maximum(tops[0], tops[1]), jnp.maximum(tops[2], tops[3]))
        ws = [jnp.exp2((t - top) * LOG2) for t in tops]
        total = sum(stats[slot, d, 4:8, :] * ws[d] for d in range(4))
        dots = sum(stats[slot, d, 8:12, :] * ws[d] for d in range(4))
        coef[0:4, :] = jnp.exp2((stats[slot, me, 0:4, :] - top) * LOG2) / total
        coef[4:8, :] = dots / total

    def grads(i):
        slot, grp = i % 2, i // NP
        blocks = []
        for j in range(2):
            rows = slice(FP * j, FP * (j + 1))
            for h in range(2):
                n = 2 * j + h
                qb, db, _ = operands(i, j, h)
                ck, cv = slice(QW * h, QW * (h + 1)), slice(W + QW * h, W + QW * (h + 1))
                p = e_s[slot, n] * coef[n:n + 1, :]
                pb = p.astype(BF)
                gb = (p * (dp_s[slot, n] - coef[B4 + n:B4 + n + 1, :]) * 0.125).astype(BF)
                dk = jnp.dot(gb, qb, preferred_element_type=F32)
                dv = jnp.dot(pb, db, preferred_element_type=F32)
                dkv[slot, rows, ck] = dk.astype(BF)
                dkv[slot, rows, cv] = dv.astype(BF)
                bias[me, pl.ds(grp, 1), cv] += jnp.sum(dv, axis=0, keepdims=True)
                blocks.append((j, h, pb, gb))
        return blocks

    def sums(i, blocks):
        mask = block_mask()
        for j, h, pb, gb in blocks:
            rows = slice(FP * j, FP * (j + 1))
            ck, cv = slice(QW * h, QW * (h + 1)), slice(W + QW * h, W + QW * (h + 1))
            for which, x in ((0, dotg(pb, kv[i % 3, rows, cv], 0, 0)), (1, dotg(gb, kv[i % 3, rows, ck], 0, 0))):
                x = jnp.where(mask, x, 0.0)
                x = (x[0:32] + x[32:64]) + (x[64:96] + x[96:128])
                od[i % 2, which, T * j:T * (j + 1), ck] = x
                if which == 1:
                    bias[me, pl.ds(i // NP, 1), ck] += jnp.sum(x, axis=0, keepdims=True)

    def keep_copy(n):
        return pltpu.make_async_copy(frames.at[n % 2], mp_hbm.at[n % B4], keep_sem)

    def load_copy(n):
        return pltpu.make_async_copy(mp_hbm.at[n % B4], frames.at[n % 2], load_sem)

    def tiles(i, do_sort):
        n = i // B4
        if do_sort:
            raw_copy(i + B4).wait()

            @pl.when(i + B4 + 1 < NP)
            def _():
                raw_copy(i + B4 + 1).start()

        @pl.when(i % B4 == 0)
        def _():
            @pl.when((n >= 1) & (n <= B4))
            def _():
                keep_copy(n - 1).wait()

            @pl.when(n < B4)
            def _():
                keep_copy(n).start()

            if not do_sort:
                @pl.when(n >= B4)
                def _():
                    load_copy(n).wait()

                @pl.when((n >= B4 - 1) & (n < B8 - 1))
                def _():
                    load_copy(n + 1).start()

    def step(i, do_a, do_b, do_sort, mode):
        b = i - 2
        if do_b:
            @pl.when(b >= NP)
            def _():
                exchange(0, b - NP, T3[0], T4[0])

            stat_wait(b)

            @when(on(mode, b, 2))
            def _():
                dkv_copy(b - 2).wait()

            od_wait(b, mode)
        if do_a:
            tiles(i, do_sort)
        if do_b:
            od_sum(b, mode)
            combine(b)
        if do_a:
            project(i)
        if do_b:
            blocks = grads(b)
        if do_a:
            scores(i)
            if do_sort:
                sort_frames(i + B4)
        if do_b:
            acc[b // NP] += jnp.dot(mt[b % 3], dkv[b % 2], preferred_element_type=F32)
            sums(b, blocks)
        if do_a:
            stat_send(i)
        if do_b:
            dkv_copy(b).start()
            s1(b).start()
            od_send(b, mode)

    barrier = pltpu.get_barrier_semaphore()
    for k in range(1, B4):
        pl.semaphore_signal(barrier, inc=1, device_id={"cp": (me + k) % B4}, device_id_type=MESH)
    top, low = pl.ds(0, ROWS), pl.ds(ROWS, D - ROWS)
    rest = pl.ds(0, D - ROWS)
    loads = [pltpu.make_async_copy(x, y, in_sem.at[k]) for k, (x, y) in enumerate((
        (h_hbm, res.at[0]), (wq_hbm.at[top], kv.at[0]), (wq_hbm.at[low], dkv.at[0, rest]), (dy_hbm, res.at[1]),
        (wo_hbm.at[top], kv.at[1]), (wo_hbm.at[low], dkv.at[1, rest]), (wk_hbm, wk), (wv_hbm, wv)))]
    for cp in loads[:3]:
        cp.start()
    raw[:, F:] = jnp.zeros((B2, FP - F, B8, QW), BF)
    perm[...] = permutation(FC)
    bv32[...] = vec(bv)
    bias[me] = jnp.zeros((B8, D), F32)
    for cp in loads[:3]:
        cp.wait()
    for cp in loads[3:]:
        cp.start()
    raw_copy(0).start()

    def first(n, carry):
        rows = pl.ds(pl.multiple_of(RC * n, RC), RC)
        x_hat, _ = norm_parts(res[0, rows].astype(F32))
        x = (x_hat * vec(gain) + vec(shift)).astype(BF)
        q[rows] = (jnp.dot(x[:, :ROWS], kv[0], preferred_element_type=F32)
                   + jnp.dot(x[:, ROWS:], dkv[0, rest], preferred_element_type=F32) + vec(bq)).astype(BF)
        for g in range(2):
            acc[g, rows] = jnp.zeros((RC, D), F32)
        return carry

    def second(n, carry):
        raw_copy(n).wait()
        raw_copy(n + 1).start()
        rows = pl.ds(pl.multiple_of(RC * n, RC), RC)
        sort_frames(n)
        do[rows, :ROWS] = dotg(res[1, rows], kv[1], 1, 1).astype(BF)
        do[rows, ROWS:] = dotg(res[1, rows], dkv[1, rest], 1, 1).astype(BF)
        return carry

    lax.fori_loop(0, TOK // RC, first, 0)
    for cp in loads[3:-2]:
        cp.wait()
    lax.fori_loop(0, TOK // RC, second, 0)
    for cp in loads[-2:]:
        cp.wait()
    pl.semaphore_wait(barrier, 3)

    def run(lo, hi, *what):
        def body(i, carry):
            step(i, *what)
            return carry
        lax.fori_loop(lo, hi, body, 0)

    run(0, 2, True, False, True, FILL)
    run(2, NP - B4, True, True, True, FILL)
    run(NP - B4, STEPS, True, True, False, ALL)
    run(STEPS, STEPS + 2, False, True, False, ALL)

    def b_copy(k, src):
        return remote(bias.at[src], bias.at[src], b_send.at[k - 1], b_recv.at[src], (me + k) % 4)

    for k in range(1, 4):
        b_copy(k, me).start()
    dkv_copy(STEPS - 2).wait()
    dkv_copy(STEPS - 1).wait()

    def part(u, k):
        return frames.at[u % 2, pl.ds(ROWS * k, ROWS)]

    def c_load(u, k):
        return pltpu.make_async_copy(dkv_hbm.at[k % 2, 2 * u + k // 2], part(u, k), in_sem.at[k])

    def dm_copy(u, k):
        return pltpu.make_async_copy((kv, dkv)[k].at[u % 2], dm_hbm.at[2 * u + k], dm_sem.at[k, u % 2])

    for k in range(B4):
        c_load(0, k).start()
    exchange(1, 0, T3[1], T4[1])

    def c_step(u, carry):
        for k in range(B4):
            c_load(u, k).wait()

        @pl.when(u + 1 < NP // 2)
        def _():
            for k in range(B4):
                c_load(u + 1, k).start()

        @pl.when(u >= 2)
        def _():
            for k in range(2):
                dm_copy(u - 2, k).wait()

        @pl.when(u < B4)
        def _():
            for k in range(2):
                od_wait(STEPS + 2 * u + k, DRAIN)
                od_sum(STEPS + 2 * u + k, DRAIN)
                od_send(STEPS + 2 * u + k, DRAIN)

        exchange(1, u + 1, T3[1], T4[1])

        @pl.when(u == 1)
        def _():
            for n in range(NP - T4[0], NCH[0]):
                forward(0, n)

        @pl.when(u == 3)
        def _():
            gathered(0)

        @pl.when(u == 6)
        def _():
            rows = res.at[0, 0:TOK // 2]
            for sem in (s3_send, s3s_send, s4_send):
                pltpu.make_async_copy(rows, rows, sem).wait()
            pltpu.make_async_copy(res.at[0], res.at[0], res_recv).wait()
            pltpu.make_async_copy(res, res_hbm, out_sem.at[2]).start()

        w = jnp.concatenate([wk[:, :W], wv[:, :W], wk[:, W:], wv[:, W:]], axis=1)
        for k in range(2):
            for j in range(2):
                rows = slice(FP * j, FP * (j + 1))
                x = jnp.concatenate([part(u, 2 * k)[rows], part(u, 2 * k + 1)[rows]], axis=1)
                (kv, dkv)[k][u % 2, rows] = dotg(x, w, 1, 1).astype(BF)
        for k in range(2):
            dm_copy(u, k).start()
        return carry

    lax.fori_loop(0, NP // 2, c_step, 0)
    for t in range(NP // 2 + 1, T4[1] + NCH[1]):
        exchange(1, t, T3[1], T4[1])
    gathered(1)
    for k in range(1, 4):
        b_copy(k, (me + k) % 4).wait_recv()
        b_copy(k, me).wait_send()
    big1[0:8, :] = (bias[0, :, 0:W] + bias[1, :, 0:W]) + (bias[2, :, 0:W] + bias[3, :, 0:W])
    big1[8:16, :] = (bias[0, :, W:] + bias[1, :, W:]) + (bias[2, :, W:] + bias[3, :, W:])
    bias_out = pltpu.make_async_copy(big1.at[0:16], bias_hbm, out_sem.at[3])
    bias_out.start()
    for u in (NP // 2 - 2, NP // 2 - 1):
        for k in range(2):
            dm_copy(u, k).wait()
    dw_copy(0).wait()
    dw_copy(1).wait()
    pltpu.make_async_copy(res, res_hbm, out_sem.at[2]).wait()
    bias_out.wait()


def attention(mt, h, dy, w_q, w_o, w_k, w_v, gain, shift, b_q, b_v):
    vm = pl.BlockSpec(memory_space=VMEM)
    hbm = pl.BlockSpec(memory_space=pl.ANY)
    dma = pltpu.SemaphoreType.DMA
    d2, d4, d8, dn = dma((B2,)), dma((B4,)), dma((B8,)), dma((B2, B8))
    credit = pltpu.SemaphoreType.REGULAR((B2,))
    probs, mat, rows32 = VMEM((B2, B4, FP, LANES), F32), VMEM((D, D), BF), VMEM((B4, T, W), F32)
    return pl.pallas_call(
        attn_kernel, name="attention",
        out_shape=(SDS((B2, TOK, D), BF), SDS((B2, D, D), F32), SDS((2 * B8, W), F32), SDS((NP, ROWS, D), BF),
                   SDS((B2, NP, ROWS, D), BF), SDS((B4, B8 * FP, D), BF)),
        in_specs=[hbm] * 7 + [vm] * B4,
        out_specs=(hbm,) * 6,
        scratch_shapes=[
            VMEM((B2, FP, B8, QW), BF), VMEM((QW, QW), BF), VMEM((1, D), F32), VMEM((B2, B8 * FP, D), BF), mat, mat, mat, mat,
            VMEM((3, ROWS, D), BF), probs, probs, VMEM((3, D, ROWS), BF), VMEM((B4, B4, 3 * B4, LANES), F32),
            VMEM((B8, LANES), F32), VMEM((B2, ROWS, D), BF), VMEM((B2, D, D), F32), VMEM((B4, B8, D), F32),
            VMEM((B2, B2, 2 * T, W), F32), VMEM((B4, 2 * T, W), F32), rows32, rows32, VMEM((B8, T, W), F32),
            VMEM((B2, TOK, D), BF), VMEM((D, W), F32), VMEM((B2, D // 2, W), F32),
            d2, d8, d2, dma((B2, B2)), d4, d4, d4, d4, d4, d8, d8, dma, dma((2 * B8,)), dma, dma, dma, d2, d2, dn, dn, dn, dn, dn, dn, d2, d4, d4,
            dma, dma, credit, credit],
        compiler_params=pltpu.CompilerParams(vmem_limit_bytes=67043328, collective_id=0, has_side_effects=True),
    )(mt, h, dy, w_q, w_o, w_k, w_v, gain, shift, b_q, b_v)


def solution(mesh):
    act_spec = P("dp", None, None)
    mem_spec = P("dp", "cp", None)
    vec_out = P("dp")
    mat_out = P("dp", None)
    in_specs = (act_spec, mem_spec, P(), P(), P(), P(), P(), P(), P(), P(), P(), act_spec)
    out_specs = (act_spec, act_spec, mem_spec, vec_out, vec_out, mat_out, vec_out, mat_out, mat_out, vec_out, mat_out, vec_out)

    def device_step(hidden, memory, ln_gain, ln_bias, w_q, b_q, w_k, w_v, b_v, w_o, b_o, grad_y):
        h = hidden.reshape(TOK, D)
        dy = grad_y.reshape(TOK, D)
        res, dw, bias, dm, _, _ = attention(memory.transpose(1, 0, 2), h, dy, w_q, w_o, w_k, w_v, ln_gain, ln_bias, b_q, b_v)
        gm, y, gh, gwo, gwq, gwk, gwv, dg, db, dbq, dbv, dbo = finish(
            dm.reshape(NB, FP, D), res, h, dy, w_o, w_q, dw, bias, ln_gain, ln_bias, b_o)
        return (y.reshape(NB, T, D), gh.reshape(NB, T, D), gm.transpose(1, 0, 2), dg, db, gwq, dbq, gwk, gwv, dbv, gwo, dbo)

    return jax.shard_map(device_step, mesh=mesh, in_specs=in_specs, out_specs=out_specs, check_vma=False)
```

```python
import functools
import math
import jax
import jax.numpy as jnp
from jax import lax
from jax.experimental import pallas as pl
from jax.experimental.pallas import tpu as pltpu
from jax.sharding import PartitionSpec as P

EPS = 1e-5
HEAD = 64
F, FP, D, T = 375, 384, 1024, 32
NB = 32
NP = NB // 2
STEPS = 2 * NP
W = 512
ROWS = 2 * FP
QW = 256
BF, F32 = jnp.bfloat16, jnp.float32
LOG2 = 0.125 * math.log2(math.e)
MESH = pl.DeviceIdType.MESH
VMEM = pltpu.VMEM
B2, B4, B8, LANES = 2, 4, 8, 128
RC = 256
TOK = NB * T
SDS = jax.ShapeDtypeStruct


def dotg(a, b, ca, cb):
    return lax.dot_general(a, b, (((ca,), (cb,)), ((), ())), preferred_element_type=F32)


FC = 32
NFC = FP // FC


def fixed(rows):
    return pl.BlockSpec((rows, D), lambda s: (0, 0), pipeline_mode=pl.Buffered(1))


def lanes(t):
    return slice(LANES * t, LANES * (t + 1))


def permutation(n):
    r = lax.broadcasted_iota(jnp.int32, (QW, QW), 0)
    k = lax.broadcasted_iota(jnp.int32, (QW, QW), 1)
    return (k == r % n * (QW // n) + r // n).astype(F32).astype(BF)


def norm_parts(h):
    centered = h - jnp.mean(h, axis=-1, keepdims=True)
    inv_std = lax.rsqrt(jnp.mean(centered * centered, axis=-1, keepdims=True) + EPS)
    return centered * inv_std, inv_std


JOB0, JOBS = 2, 4
FB = 16
NFB = FP // FB


def finish_kernel(dm_hbm, res_hbm, h_hbm, dy_hbm, wo_hbm, wq_hbm, dw_hbm, bias, gain, shift, bo,
                  gm_hbm, y_hbm, gh_hbm, gwo_hbm, gwq_hbm, gwk_hbm, gwv_hbm, dg, db, dbq, dbv, dbo,
                  src, dst, perm, res, h, dy, wo, wq, x, y, gh, gw, stage, sums,
                  src_sem, dst_sem, in_sem, y_sem, gh_sem, gw_sem, ld_sem, st_sem):
    loads = [pltpu.make_async_copy(a, b, in_sem.at[k]) for k, (a, b) in enumerate(
        ((h_hbm, h), (res_hbm, res), (wo_hbm, wo), (dy_hbm, dy), (wq_hbm, wq)))]

    def src_copy(s):
        return pltpu.make_async_copy(dm_hbm.at[:, pl.ds(pl.multiple_of(FB * s, FB), FB)], src.at[s % B8], src_sem.at[s % B8])

    def dst_copy(s):
        return pltpu.make_async_copy(dst.at[s % B8], gm_hbm.at[pl.ds(FB * s, FB)], dst_sem.at[s % B8])

    def last_copy():
        s = NFB - 1
        return pltpu.make_async_copy(dst.at[s % B8, 0:F - FB * s], gm_hbm.at[FB * s:F], dst_sem.at[s % B8])

    def rows(n):
        return pl.ds(pl.multiple_of(RC * n, RC), RC)

    def out_copy(a, b, sem, n):
        return pltpu.make_async_copy(a.at[rows(n)], b.at[rows(n)], sem.at[n])

    def gw_copy(b, n):
        return pltpu.make_async_copy(gw.at[n], b.at[rows(n)], gw_sem.at[n])

    def piece_in(k):
        g, v = k // 2, k % 2
        return pltpu.make_async_copy(dw_hbm.at[g, :, pl.ds(W * v, W)], stage.at[v], ld_sem.at[v])

    def piece_out(k):
        g, v = k // 2, k % 2
        return pltpu.make_async_copy(stage.at[v], (gwk_hbm, gwv_hbm)[v].at[:, pl.ds(W * g, W)], st_sem.at[v])

    def vec(ref):
        return ref[...].astype(F32).reshape(1, D)

    def move(s):
        for k in range(NB // FB):
            z = src[s % B8, FB * k:FB * (k + 1)].reshape(QW, D)
            z = jnp.dot(perm[...], z, preferred_element_type=F32)
            dst[s % B8, :, FB * k:FB * (k + 1), :] = z.astype(BF).reshape(FB, FB, D)

    def job_y(n):
        hf = h[rows(n)].astype(F32)
        x_hat, _ = norm_parts(hf)
        x[rows(n)] = (x_hat * vec(gain) + vec(shift)).astype(BF)
        y[rows(n)] = (hf + jnp.dot(res[0, rows(n)], wo[...], preferred_element_type=F32) + vec(bo)).astype(BF)

    def job_wo(n):
        gw[n] = dotg(res[0, :, rows(n)], dy[...], 0, 0)

    def job_h(n):
        x_hat, inv_std = norm_parts(h[rows(n)].astype(F32))
        dyf = dy[rows(n)].astype(F32)
        d_x = dotg(res[1, rows(n)], wq[...], 1, 1)
        for k, a in enumerate((d_x * x_hat, d_x, dyf)):
            sums[k:k + 1] += jnp.sum(a, axis=0, keepdims=True)
        d_hat = d_x * vec(gain)
        d_h = inv_std * (d_hat - jnp.mean(d_hat, axis=-1, keepdims=True) - x_hat * jnp.mean(d_hat * x_hat, axis=-1, keepdims=True))
        gh[rows(n)] = (dyf + d_h).astype(BF)

    def job_wq(n):
        gw[n] = dotg(x[:, rows(n)], res[1], 0, 0)

    for k in range(B8 - 1):
        src_copy(k).start()
    for cp in loads:
        cp.start()
    piece_in(0).start()
    piece_in(1).start()
    sums[...] = jnp.zeros_like(sums)
    perm[...] = permutation(FB)
    for ref, k in ((dbq, 0), (dbv, B8)):
        ref[...] = jnp.concatenate([bias[k:k + 1], bias[k + 1:k + 2]], axis=1).reshape(D)
    outs = ((job_y, lambda n: out_copy(y, y_hbm, y_sem, n)), (job_wo, lambda n: gw_copy(gwo_hbm, n)),
            (job_h, lambda n: out_copy(gh, gh_hbm, gh_sem, n)), (job_wq, lambda n: gw_copy(gwq_hbm, n)))
    needs = (loads[:3], loads[3:4], loads[4:], ())

    def step(s, carry):
        src_copy(s).wait()

        @pl.when(s + B8 - 1 < NFB)
        def _():
            src_copy(s + B8 - 1).start()

        @pl.when(s >= B8)
        def _():
            dst_copy(s - B8).wait()

        job = s - JOB0
        n = job % JOBS
        for kind, (f, copy) in enumerate(outs):
            @pl.when((job >= kind * JOBS) & (job < (kind + 1) * JOBS))
            def _():
                if needs[kind]:
                    @pl.when(n == 0)
                    def _():
                        for cp in needs[kind]:
                            cp.wait()
                if kind == 3:
                    gw_copy(gwo_hbm, n).wait()
                move(s)
                f(n)
                copy(n).start()

        @pl.when((job < 0) | (job >= JOBS * JOBS))
        def _():
            move(s)

        @pl.when(s < NFB - 1)
        def _():
            dst_copy(s).start()

        for v in range(2):
            @pl.when(s == JOBS + v)
            def _():
                piece_in(v).wait()
                piece_out(v).start()

            @pl.when(s == B8 + v)
            def _():
                piece_out(v).wait()
                piece_in(v + 2).start()

            @pl.when(s == B8 + JOBS + v)
            def _():
                piece_in(v + 2).wait()
                piece_out(v + 2).start()
        return carry

    lax.fori_loop(0, NFB, step, 0)
    last_copy().start()
    for k, ref in enumerate((dg, db, dbo)):
        ref[...] = sums[k:k + 1].reshape(D)
    for k in range(JOBS):
        out_copy(y, y_hbm, y_sem, k).wait()
        out_copy(gh, gh_hbm, gh_sem, k).wait()
        gw_copy(gwq_hbm, k).wait()
    piece_out(2).wait()
    piece_out(3).wait()
    for k in range(2, B8 + 1):
        dst_copy(NFB - k).wait()
    last_copy().wait()


def finish(dm, res, h, dy, w_o, w_q, dw, bias, gain, shift, b_o):
    hbm, vm = pl.BlockSpec(memory_space=pl.ANY), pl.BlockSpec(memory_space=VMEM)
    dma = pltpu.SemaphoreType.DMA
    mat, dj, d2, d8, vec = VMEM((D, D), BF), dma((JOBS,)), dma((B2,)), dma((B8,)), SDS((D,), F32)
    return pl.pallas_call(
        finish_kernel, name="finish",
        out_shape=(SDS((F, NB, D), BF), SDS((TOK, D), BF), SDS((TOK, D), BF)) + (SDS((D, D), F32),) * B4 + (vec,) * (B4 + 1),
        in_specs=[hbm] * (B8 - 1) + [vm] * B4,
        out_specs=(hbm,) * (B8 - 1) + (vm,) * (B4 + 1),
        scratch_shapes=[
            VMEM((B8, NB, FB, D), BF), VMEM((B8, FB, NB, D), BF), VMEM((QW, QW), BF), VMEM((B2, TOK, D), BF), mat, mat, mat, mat, mat,
            mat, mat, VMEM((JOBS, RC, D), F32), VMEM((B2, D, W), F32), VMEM((B8, D), F32), d8, d8, d8, dj, dj, dj, d2, d2],
        compiler_params=pltpu.CompilerParams(vmem_limit_bytes=67043328),
    )(dm, res, h, dy, w_o, w_q, dw, bias, gain, shift, b_o)


def block_mask():
    return lax.broadcasted_iota(jnp.int32, (128, 256), 0) // T == lax.broadcasted_iota(jnp.int32, (128, 256), 1) // HEAD


def block_diag(x, mask):
    return jnp.where(mask, jnp.concatenate([x] * 4, axis=0), jnp.zeros((), BF))


def when(cond):
    if isinstance(cond, bool):
        return (lambda f: f()) if cond else (lambda f: None)
    return pl.when(cond)


CH = (64, 128)
NCH = tuple(D // 2 // rows for rows in CH)
TS = (7, 3)
T3, T4 = (10, 4), (13, 6)


ALL, FILL, DRAIN = range(3)


def attn_kernel(m_hbm, h_hbm, dy_hbm, wq_hbm, wo_hbm, wk_hbm, wv_hbm, gain, shift, bq, bv,
                res_hbm, dw_hbm, bias_hbm, dm_hbm, dkv_hbm, mp_hbm,
                raw, perm, bv32, frames, q, do, wk, wv, kv, e_s, dp_s, mt, stats, coef, dkv, acc, bias, od, r1, keep, x2, r2, res, big1, big2,
                raw_sem, in_sem, dkv_sem, dm_sem, out_sem, st_send, st_recv, s1_send, s1_recv, s2_send, s2_recv,
                s3_send, s3_recv, s3s_send, s4_send, res_recv, e1_send, e1_recv, e2_send, e2_recv,
                e3_send, e3_recv, e3s_send, e4_send, acc_recv, b_send, b_recv, keep_sem, load_sem, e1p_send, e1p_recv, free_sib, free_xn):
    me = lax.axis_index("cp")
    cx, cc = me // 2, me % 2
    sib, xn = 2 * cx + 1 - cc, 2 * (1 - cx) + cc

    def vec(ref):
        return ref[...].astype(F32).reshape(1, D)

    def remote(src, dst, ss, rs, dev):
        return pltpu.make_async_remote_copy(src_ref=src, dst_ref=dst, send_sem=ss, recv_sem=rs,
                                            device_id={"cp": dev}, device_id_type=MESH)

    def raw_copy(c):
        seqs = pl.ds(pl.multiple_of(B8 * (c // B4 % B4), B8), B8)
        return pltpu.make_async_copy(m_hbm.at[:, seqs, quarter(c)], raw.at[c % 2, 0:F], raw_sem.at[c % 2])

    def quarter(c):
        return pl.ds(pl.multiple_of(c % B4 * QW, QW), QW)

    def sort_frames(c):
        for n in range(NFC):
            x = raw[c % 2, FC * n:FC * (n + 1)].reshape(QW, QW)
            y = jnp.dot(perm[...], x, preferred_element_type=F32).astype(BF)
            for b in range(B8):
                frames[c // B4 % 2, FP * b + FC * n:FP * b + FC * (n + 1), quarter(c)] = y[FC * b:FC * (b + 1)]

    def dkv_copy(i):
        return pltpu.make_async_copy(dkv.at[i % 2], dkv_hbm.at[i // NP, i % NP], dkv_sem.at[i % 2])

    def stat_send(i):
        for k in range(1, B4):
            remote(stats.at[i % B4, me], stats.at[i % B4, me], st_send.at[i % B4], st_recv.at[i % B4], (me + k) % B4).start()

    def stat_wait(i):
        three = stats.at[i % B4, 0:3]
        for sem in (st_recv, st_send):
            pltpu.make_async_copy(three, three, sem.at[i % B4]).wait()

    def s1(b):
        return remote(od.at[b % 2, 1 - cc], r1.at[b % 4], s1_send.at[b % 4], s1_recv.at[b % 4], sib)

    def s2(b):
        return remote(x2.at[b % 4], r2.at[b % 8], s2_send.at[b % 8], s2_recv.at[b % 8], xn)

    def res_at(b, x):
        return res.at[cc, pl.ds(pl.multiple_of(64 * (b % NP) + T * x, T), T), pl.ds(pl.multiple_of(W * (b // NP), W), W)]

    def s3(b, x):
        return remote(res_at(b, x), res_at(b, x), s3_send, s3_recv.at[b % (2 * B8)], xn)

    def s3s(b):
        return remote(res_at(b, cx), res_at(b, cx), s3s_send, res_recv, sib)

    def s4(b):
        return remote(res_at(b, 1 - cx), res_at(b, 1 - cx), s4_send, res_recv, sib)

    def on(mode, b, k):
        return True if mode == ALL else b >= k if mode == FILL else b - k < STEPS

    def od_wait(b, mode):
        @when(on(mode, b, 8))
        def _():
            s3(b - 8, 1 - cx).wait_recv()

        @when(on(mode, b, 5))
        def _():
            s2(b - 5).wait_recv()
            s2(b - 5).wait_send()

        @when(on(mode, b, 2))
        def _():
            s1(b - 2).wait_send()
            s1(b - 2).wait_recv()

    def od_sum(b, mode):
        @when(on(mode, b, 5))
        def _():
            res_at(b - 5, cx)[...] = (keep[(b - 5) % B4] + r2[(b - 5) % B8]).astype(BF)

        @when(on(mode, b, 2))
        def _():
            for ref, x in ((keep, cx), (x2, 1 - cx)):
                rows = pl.ds(pl.multiple_of(T * x, T), T)
                ref[(b - 2) % B4] = od[b % 2, cc, rows, :] + r1[(b - 2) % B4, rows, :]

    def od_send(b, mode):
        @when(on(mode, b, 2))
        def _():
            s2(b - 2).start()

        @when(on(mode, b, 5))
        def _():
            s3(b - 5, cx).start()
            s3s(b - 5).start()

        @when(on(mode, b, 8))
        def _():
            s4(b - 8).start()

    own = pl.ds(pl.multiple_of(W * cc, W), W)
    other = pl.ds(pl.multiple_of(W * (1 - cc), W), W)

    def rows_of(g, x, n):
        return pl.ds(pl.multiple_of(x * (D // 2) + CH[g] * n, CH[g]), CH[g])

    def chunk_of(g, n):
        return big2.at[g, pl.ds(pl.multiple_of(CH[g] * n, CH[g]), CH[g])]

    def e1(g):
        return remote(acc.at[g, :, other], big1, e1_send.at[g], e1_recv.at[g], sib)

    def e1_part(n, x):
        rows = rows_of(1, x, n)
        return remote(acc.at[1, rows, other], big1.at[rows], e1p_send.at[n], e1p_recv.at[n], sib)

    def e1_wait(n, sem):
        both = big1.at[0:2 * CH[1]]
        pltpu.make_async_copy(both, both, sem.at[n]).wait()

    def e2(g, n):
        return remote(acc.at[g, rows_of(g, 1 - cx, n), own], chunk_of(g, n), e2_send.at[g, n], e2_recv.at[g, n], xn)

    def e3(g, n, x):
        ref = acc.at[g, rows_of(g, x, n), own]
        return remote(ref, ref, e3_send.at[g, n], e3_recv.at[g, n], xn)

    def to_sib(g, n, x, sem):
        ref = acc.at[g, rows_of(g, x, n), own]
        return remote(ref, ref, sem.at[g, n], acc_recv.at[g], sib)

    def dw_copy(g):
        return pltpu.make_async_copy(acc.at[g], dw_hbm.at[g], out_sem.at[g])

    def reduce_core(g, n):
        if g == 1:
            e1_wait(n, e1p_recv)
        for x in (cx, 1 - cx):
            acc[g, rows_of(g, x, n), own] += big1[rows_of(g, x, n), :]
        e2(g, n).start()

    def sent(g, n):
        e2(g, n).wait_send()
        pl.semaphore_signal(free_xn.at[g], inc=1, device_id={"cp": xn}, device_id_type=MESH)

    def reduce_chip(g, n):
        e2(g, n).wait_recv()
        pl.semaphore_wait(free_xn.at[g], 1)
        acc[g, rows_of(g, cx, n), own] += chunk_of(g, n)[...]
        e3(g, n, cx).start()
        to_sib(g, n, cx, e3s_send).start()

    def forward(g, n):
        e3(g, n, 1 - cx).wait_recv()
        to_sib(g, n, 1 - cx, e4_send).start()

    def gathered(g):
        half = acc.at[g, :, other]
        remote(half, half, e1_send.at[g], acc_recv.at[g], sib).wait_recv()
        for n in range(NCH[g]):
            e3(g, n, cx).wait_send()
            to_sib(g, n, cx, e3s_send).wait_send()
            to_sib(g, n, 1 - cx, e4_send).wait_send()
        dw_copy(g).start()

    def exchange(g, t, t3, t4):
        def chunk(t0, f):
            n = t - t0
            if isinstance(n, int):
                if 0 <= n < NCH[g]:
                    f(g, n)
            else:
                pl.when((n >= 0) & (n < NCH[g]))(lambda: f(g, n))

        @when(t == 0)
        def _():
            if g == 0:
                e1(g).start()
            else:
                for n in range(NCH[1]):
                    e1_part(n, 0).start()
                    e1_part(n, 1).start()

        @when(t == 1 + g)
        def _():
            if g == 0:
                e1(g).wait_send()
                e1(g).wait_recv()
            else:
                for n in range(NCH[1]):
                    e1_wait(n, e1p_send)
            pl.semaphore_signal(free_sib.at[g], inc=1, device_id={"cp": sib}, device_id_type=MESH)

        @when(t == t3)
        def _():
            pl.semaphore_wait(free_sib.at[g], 1)

        chunk(1, reduce_core)
        chunk(TS[g], sent)
        chunk(t3, reduce_chip)
        chunk(t4, forward)

    def operands(i, j, h):
        cols = pl.ds(pl.multiple_of(W * (i // NP) + 256 * h, 256), 256)
        rows = pl.ds(pl.multiple_of(64 * (i % NP) + T * j, T), T)
        mask = block_mask()
        return block_diag(q[rows, cols], mask), block_diag(do[rows, cols], mask), mask

    def rows_of_pair(i):
        return frames[i // B4 % 2, pl.ds(pl.multiple_of(i % B4 * ROWS, ROWS), ROWS), :]

    def project(i):
        cols = pl.ds(pl.multiple_of(W * (i // NP), W), W)
        m = rows_of_pair(i)
        kv[i % 3, :, 0:W] = jnp.dot(m, wk[:, cols], preferred_element_type=F32).astype(BF)
        kv[i % 3, :, W:] = (jnp.dot(m, wv[:, cols], preferred_element_type=F32) + bv32[:, cols]).astype(BF)
        mt[i % 3] = m.T

    def scores(i):
        slot = i % 2
        real = lax.broadcasted_iota(jnp.int32, (FP, LANES), 0) < F
        for j in range(2):
            rows = slice(FP * j, FP * (j + 1))
            for h in range(2):
                n = 2 * j + h
                qb, db, _ = operands(i, j, h)
                s = dotg(kv[i % 3, rows, QW * h:QW * (h + 1)], qb, 1, 1)
                dp = dotg(kv[i % 3, rows, W + QW * h:W + QW * (h + 1)], db, 1, 1)
                s = jnp.where(real, s, -1e30)
                top = jnp.max(s, axis=0, keepdims=True)
                e = jnp.exp2((s - top) * LOG2)
                e_s[slot, n] = e
                dp_s[slot, n] = dp
                for k, row in enumerate((top, jnp.sum(e, axis=0, keepdims=True), jnp.sum(e * dp, axis=0, keepdims=True))):
                    stats[i % B4, me, B4 * k + n:B4 * k + n + 1, :] = row

    def combine(i):
        slot = i % 4
        tops = [stats[slot, d, 0:4, :] for d in range(4)]
        top = jnp.maximum(jnp.maximum(tops[0], tops[1]), jnp.maximum(tops[2], tops[3]))
        ws = [jnp.exp2((t - top) * LOG2) for t in tops]
        total = sum(stats[slot, d, 4:8, :] * ws[d] for d in range(4))
        dots = sum(stats[slot, d, 8:12, :] * ws[d] for d in range(4))
        coef[0:4, :] = jnp.exp2((stats[slot, me, 0:4, :] - top) * LOG2) / total
        coef[4:8, :] = dots / total

    def grads(i):
        slot, grp = i % 2, i // NP
        blocks = []
        for j in range(2):
            rows = slice(FP * j, FP * (j + 1))
            for h in range(2):
                n = 2 * j + h
                qb, db, _ = operands(i, j, h)
                ck, cv = slice(QW * h, QW * (h + 1)), slice(W + QW * h, W + QW * (h + 1))
                p = e_s[slot, n] * coef[n:n + 1, :]
                pb = p.astype(BF)
                gb = (p * (dp_s[slot, n] - coef[B4 + n:B4 + n + 1, :]) * 0.125).astype(BF)
                dk = jnp.dot(gb, qb, preferred_element_type=F32)
                dv = jnp.dot(pb, db, preferred_element_type=F32)
                dkv[slot, rows, ck] = dk.astype(BF)
                dkv[slot, rows, cv] = dv.astype(BF)
                bias[me, pl.ds(grp, 1), cv] += jnp.sum(dv, axis=0, keepdims=True)
                blocks.append((j, h, pb, gb))
        return blocks

    def sums(i, blocks):
        mask = block_mask()
        for j, h, pb, gb in blocks:
            rows = slice(FP * j, FP * (j + 1))
            ck, cv = slice(QW * h, QW * (h + 1)), slice(W + QW * h, W + QW * (h + 1))
            for which, x in ((0, dotg(pb, kv[i % 3, rows, cv], 0, 0)), (1, dotg(gb, kv[i % 3, rows, ck], 0, 0))):
                x = jnp.where(mask, x, 0.0)
                x = (x[0:32] + x[32:64]) + (x[64:96] + x[96:128])
                od[i % 2, which, T * j:T * (j + 1), ck] = x
                if which == 1:
                    bias[me, pl.ds(i // NP, 1), ck] += jnp.sum(x, axis=0, keepdims=True)

    def keep_copy(n):
        return pltpu.make_async_copy(frames.at[n % 2], mp_hbm.at[n % B4], keep_sem)

    def load_copy(n):
        return pltpu.make_async_copy(mp_hbm.at[n % B4], frames.at[n % 2], load_sem)

    def tiles(i, do_sort):
        n = i // B4
        if do_sort:
            raw_copy(i + B4).wait()

            @pl.when(i + B4 + 1 < NP)
            def _():
                raw_copy(i + B4 + 1).start()

        @pl.when(i % B4 == 0)
        def _():
            @pl.when((n >= 1) & (n <= B4))
            def _():
                keep_copy(n - 1).wait()

            @pl.when(n < B4)
            def _():
                keep_copy(n).start()

            if not do_sort:
                @pl.when(n >= B4)
                def _():
                    load_copy(n).wait()

                @pl.when((n >= B4 - 1) & (n < B8 - 1))
                def _():
                    load_copy(n + 1).start()

    def step(i, do_a, do_b, do_sort, mode):
        b = i - 2
        if do_b:
            @pl.when(b >= NP)
            def _():
                exchange(0, b - NP, T3[0], T4[0])

            stat_wait(b)

            @when(on(mode, b, 2))
            def _():
                dkv_copy(b - 2).wait()

            od_wait(b, mode)
        if do_a:
            tiles(i, do_sort)
        if do_b:
            od_sum(b, mode)
            combine(b)
        if do_a:
            project(i)
        if do_b:
            blocks = grads(b)
        if do_a:
            scores(i)
            if do_sort:
                sort_frames(i + B4)
        if do_b:
            acc[b // NP] += jnp.dot(mt[b % 3], dkv[b % 2], preferred_element_type=F32)
            sums(b, blocks)
        if do_a:
            stat_send(i)
        if do_b:
            dkv_copy(b).start()
            s1(b).start()
            od_send(b, mode)

    barrier = pltpu.get_barrier_semaphore()
    for k in range(1, B4):
        pl.semaphore_signal(barrier, inc=1, device_id={"cp": (me + k) % B4}, device_id_type=MESH)
    top, low = pl.ds(0, ROWS), pl.ds(ROWS, D - ROWS)
    rest = pl.ds(0, D - ROWS)
    loads = [pltpu.make_async_copy(x, y, in_sem.at[k]) for k, (x, y) in enumerate((
        (h_hbm, res.at[0]), (wq_hbm.at[top], kv.at[0]), (wq_hbm.at[low], dkv.at[0, rest]), (dy_hbm, res.at[1]),
        (wo_hbm.at[top], kv.at[1]), (wo_hbm.at[low], dkv.at[1, rest]), (wk_hbm, wk), (wv_hbm, wv)))]
    for cp in loads[:3]:
        cp.start()
    raw[:, F:] = jnp.zeros((B2, FP - F, B8, QW), BF)
    perm[...] = permutation(FC)
    bv32[...] = vec(bv)
    bias[me] = jnp.zeros((B8, D), F32)
    for cp in loads[:3]:
        cp.wait()
    for cp in loads[3:]:
        cp.start()
    raw_copy(0).start()

    def first(n, carry):
        rows = pl.ds(pl.multiple_of(RC * n, RC), RC)
        x_hat, _ = norm_parts(res[0, rows].astype(F32))
        x = (x_hat * vec(gain) + vec(shift)).astype(BF)
        q[rows] = (jnp.dot(x[:, :ROWS], kv[0], preferred_element_type=F32)
                   + jnp.dot(x[:, ROWS:], dkv[0, rest], preferred_element_type=F32) + vec(bq)).astype(BF)
        for g in range(2):
            acc[g, rows] = jnp.zeros((RC, D), F32)
        return carry

    def second(n, carry):
        raw_copy(n).wait()
        raw_copy(n + 1).start()
        rows = pl.ds(pl.multiple_of(RC * n, RC), RC)
        sort_frames(n)
        do[rows, :ROWS] = dotg(res[1, rows], kv[1], 1, 1).astype(BF)
        do[rows, ROWS:] = dotg(res[1, rows], dkv[1, rest], 1, 1).astype(BF)
        return carry

    lax.fori_loop(0, TOK // RC, first, 0)
    for cp in loads[3:-2]:
        cp.wait()
    lax.fori_loop(0, TOK // RC, second, 0)
    for cp in loads[-2:]:
        cp.wait()
    pl.semaphore_wait(barrier, 3)

    def run(lo, hi, *what):
        def body(i, carry):
            step(i, *what)
            return carry
        lax.fori_loop(lo, hi, body, 0)

    run(0, 2, True, False, True, FILL)
    run(2, NP - B4, True, True, True, FILL)
    run(NP - B4, STEPS, True, True, False, ALL)
    run(STEPS, STEPS + 2, False, True, False, ALL)

    def b_copy(k, src):
        return remote(bias.at[src], bias.at[src], b_send.at[k - 1], b_recv.at[src], (me + k) % 4)

    for k in range(1, 4):
        b_copy(k, me).start()
    dkv_copy(STEPS - 2).wait()
    dkv_copy(STEPS - 1).wait()

    def part(u, k):
        return frames.at[u % 2, pl.ds(ROWS * k, ROWS)]

    def c_load(u, k):
        return pltpu.make_async_copy(dkv_hbm.at[k % 2, 2 * u + k // 2], part(u, k), in_sem.at[k])

    def dm_copy(u, k):
        return pltpu.make_async_copy((kv, dkv)[k].at[u % 2], dm_hbm.at[2 * u + k], dm_sem.at[k, u % 2])

    for k in range(B4):
        c_load(0, k).start()
    exchange(1, 0, T3[1], T4[1])

    def c_step(u, carry):
        for k in range(B4):
            c_load(u, k).wait()

        @pl.when(u + 1 < NP // 2)
        def _():
            for k in range(B4):
                c_load(u + 1, k).start()

        @pl.when(u >= 2)
        def _():
            for k in range(2):
                dm_copy(u - 2, k).wait()

        @pl.when(u < B4)
        def _():
            for k in range(2):
                od_wait(STEPS + 2 * u + k, DRAIN)
                od_sum(STEPS + 2 * u + k, DRAIN)
                od_send(STEPS + 2 * u + k, DRAIN)

        exchange(1, u + 1, T3[1], T4[1])

        @pl.when(u == 0)
        def _():
            for n in range(NP - T3[0], NCH[0]):
                reduce_chip(0, n)

        @pl.when(u == 2)
        def _():
            for n in range(NP - T4[0], NCH[0]):
                forward(0, n)

        @pl.when(u == 4)
        def _():
            gathered(0)

        @pl.when(u == 6)
        def _():
            rows = res.at[0, 0:TOK // 2]
            for sem in (s3_send, s3s_send, s4_send):
                pltpu.make_async_copy(rows, rows, sem).wait()
            pltpu.make_async_copy(res.at[0], res.at[0], res_recv).wait()
            pltpu.make_async_copy(res, res_hbm, out_sem.at[2]).start()

        w = jnp.concatenate([wk[:, :W], wv[:, :W], wk[:, W:], wv[:, W:]], axis=1)
        for k in range(2):
            for j in range(2):
                rows = slice(FP * j, FP * (j + 1))
                x = jnp.concatenate([part(u, 2 * k)[rows], part(u, 2 * k + 1)[rows]], axis=1)
                (kv, dkv)[k][u % 2, rows] = dotg(x, w, 1, 1).astype(BF)
        for k in range(2):
            dm_copy(u, k).start()
        return carry

    lax.fori_loop(0, NP // 2, c_step, 0)
    for t in range(NP // 2 + 1, T4[1] + NCH[1]):
        exchange(1, t, T3[1], T4[1])
    gathered(1)
    for k in range(1, 4):
        b_copy(k, (me + k) % 4).wait_recv()
        b_copy(k, me).wait_send()
    big1[0:8, :] = (bias[0, :, 0:W] + bias[1, :, 0:W]) + (bias[2, :, 0:W] + bias[3, :, 0:W])
    big1[8:16, :] = (bias[0, :, W:] + bias[1, :, W:]) + (bias[2, :, W:] + bias[3, :, W:])
    bias_out = pltpu.make_async_copy(big1.at[0:16], bias_hbm, out_sem.at[3])
    bias_out.start()
    for u in (NP // 2 - 2, NP // 2 - 1):
        for k in range(2):
            dm_copy(u, k).wait()
    dw_copy(0).wait()
    dw_copy(1).wait()
    pltpu.make_async_copy(res, res_hbm, out_sem.at[2]).wait()
    bias_out.wait()


def attention(mt, h, dy, w_q, w_o, w_k, w_v, gain, shift, b_q, b_v):
    vm = pl.BlockSpec(memory_space=VMEM)
    hbm = pl.BlockSpec(memory_space=pl.ANY)
    dma = pltpu.SemaphoreType.DMA
    d2, d4, d8, dn = dma((B2,)), dma((B4,)), dma((B8,)), dma((B2, B8))
    credit = pltpu.SemaphoreType.REGULAR((B2,))
    probs, mat, rows32 = VMEM((B2, B4, FP, LANES), F32), VMEM((D, D), BF), VMEM((B4, T, W), F32)
    return pl.pallas_call(
        attn_kernel, name="attention",
        out_shape=(SDS((B2, TOK, D), BF), SDS((B2, D, D), F32), SDS((2 * B8, W), F32), SDS((NP, ROWS, D), BF),
                   SDS((B2, NP, ROWS, D), BF), SDS((B4, B8 * FP, D), BF)),
        in_specs=[hbm] * 7 + [vm] * B4,
        out_specs=(hbm,) * 6,
        scratch_shapes=[
            VMEM((B2, FP, B8, QW), BF), VMEM((QW, QW), BF), VMEM((1, D), F32), VMEM((B2, B8 * FP, D), BF), mat, mat, mat, mat,
            VMEM((3, ROWS, D), BF), probs, probs, VMEM((3, D, ROWS), BF), VMEM((B4, B4, 3 * B4, LANES), F32),
            VMEM((B8, LANES), F32), VMEM((B2, ROWS, D), BF), VMEM((B2, D, D), F32), VMEM((B4, B8, D), F32),
            VMEM((B2, B2, 2 * T, W), F32), VMEM((B4, 2 * T, W), F32), rows32, rows32, VMEM((B8, T, W), F32),
            VMEM((B2, TOK, D), BF), VMEM((D, W), F32), VMEM((B2, D // 2, W), F32),
            d2, d8, d2, dma((B2, B2)), d4, d4, d4, d4, d4, d8, d8, dma, dma((2 * B8,)), dma, dma, dma, d2, d2, dn, dn, dn, dn, dn, dn, d2, d4, d4,
            dma, dma, d4, d4, credit, credit],
        compiler_params=pltpu.CompilerParams(vmem_limit_bytes=67043328, collective_id=0, has_side_effects=True),
    )(mt, h, dy, w_q, w_o, w_k, w_v, gain, shift, b_q, b_v)


def solution(mesh):
    act_spec = P("dp", None, None)
    mem_spec = P("dp", "cp", None)
    vec_out = P("dp")
    mat_out = P("dp", None)
    in_specs = (act_spec, mem_spec, P(), P(), P(), P(), P(), P(), P(), P(), P(), act_spec)
    out_specs = (act_spec, act_spec, mem_spec, vec_out, vec_out, mat_out, vec_out, mat_out, mat_out, vec_out, mat_out, vec_out)

    def device_step(hidden, memory, ln_gain, ln_bias, w_q, b_q, w_k, w_v, b_v, w_o, b_o, grad_y):
        h = hidden.reshape(TOK, D)
        dy = grad_y.reshape(TOK, D)
        res, dw, bias, dm, _, _ = attention(memory.transpose(1, 0, 2), h, dy, w_q, w_o, w_k, w_v, ln_gain, ln_bias, b_q, b_v)
        gm, y, gh, gwo, gwq, gwk, gwv, dg, db, dbq, dbv, dbo = finish(
            dm.reshape(NB, FP, D), res, h, dy, w_o, w_q, dw, bias, ln_gain, ln_bias, b_o)
        return (y.reshape(NB, T, D), gh.reshape(NB, T, D), gm.transpose(1, 0, 2), dg, db, gwq, dbq, gwk, gwv, dbv, gwo, dbo)

    return jax.shard_map(device_step, mesh=mesh, in_specs=in_specs, out_specs=out_specs, check_vma=False)
```

```python
import functools
import math
import jax
import jax.numpy as jnp
from jax import lax
from jax.experimental import pallas as pl
from jax.experimental.pallas import tpu as pltpu
from jax.sharding import PartitionSpec as P

EPS = 1e-5
HEAD = 64
F, FP, D, T = 375, 384, 1024, 32
NB = 32
NP = NB // 2
STEPS = 2 * NP
W = 512
ROWS = 2 * FP
QW = 256
BF, F32 = jnp.bfloat16, jnp.float32
LOG2 = 0.125 * math.log2(math.e)
MESH = pl.DeviceIdType.MESH
VMEM = pltpu.VMEM
B2, B4, B8, LANES = 2, 4, 8, 128
RC = 256
TOK = NB * T
SDS = jax.ShapeDtypeStruct


def dotg(a, b, ca, cb):
    return lax.dot_general(a, b, (((ca,), (cb,)), ((), ())), preferred_element_type=F32)


FC = 32
NFC = FP // FC


def fixed(rows):
    return pl.BlockSpec((rows, D), lambda s: (0, 0), pipeline_mode=pl.Buffered(1))


def lanes(t):
    return slice(LANES * t, LANES * (t + 1))


def permutation(n):
    r = lax.broadcasted_iota(jnp.int32, (QW, QW), 0)
    k = lax.broadcasted_iota(jnp.int32, (QW, QW), 1)
    return (k == r % n * (QW // n) + r // n).astype(F32).astype(BF)


def norm_parts(h):
    centered = h - jnp.mean(h, axis=-1, keepdims=True)
    inv_std = lax.rsqrt(jnp.mean(centered * centered, axis=-1, keepdims=True) + EPS)
    return centered * inv_std, inv_std


JOB0, JOBS = 2, 4
FB = 16
NFB = FP // FB


def finish_kernel(dm_hbm, res_hbm, h_hbm, dy_hbm, wo_hbm, wq_hbm, dw_hbm, bias, gain, shift, bo,
                  gm_hbm, y_hbm, gh_hbm, gwo_hbm, gwq_hbm, gwk_hbm, gwv_hbm, dg, db, dbq, dbv, dbo,
                  src, dst, perm, res, h, dy, wo, wq, x, y, gh, gw, stage, sums,
                  src_sem, dst_sem, in_sem, y_sem, gh_sem, gw_sem, ld_sem, st_sem):
    loads = [pltpu.make_async_copy(a, b, in_sem.at[k]) for k, (a, b) in enumerate(
        ((h_hbm, h), (res_hbm, res), (wo_hbm, wo), (dy_hbm, dy), (wq_hbm, wq)))]

    def src_copy(s):
        return pltpu.make_async_copy(dm_hbm.at[:, pl.ds(pl.multiple_of(FB * s, FB), FB)], src.at[s % B8], src_sem.at[s % B8])

    def dst_copy(s):
        return pltpu.make_async_copy(dst.at[s % B8], gm_hbm.at[pl.ds(FB * s, FB)], dst_sem.at[s % B8])

    def last_copy():
        s = NFB - 1
        return pltpu.make_async_copy(dst.at[s % B8, 0:F - FB * s], gm_hbm.at[FB * s:F], dst_sem.at[s % B8])

    def rows(n):
        return pl.ds(pl.multiple_of(RC * n, RC), RC)

    def out_copy(a, b, sem, n):
        return pltpu.make_async_copy(a.at[rows(n)], b.at[rows(n)], sem.at[n])

    def gw_copy(b, n):
        return pltpu.make_async_copy(gw.at[n], b.at[rows(n)], gw_sem.at[n])

    def piece_in(k):
        g, v = k // 2, k % 2
        return pltpu.make_async_copy(dw_hbm.at[g, :, pl.ds(W * v, W)], stage.at[v], ld_sem.at[v])

    def piece_out(k):
        g, v = k // 2, k % 2
        return pltpu.make_async_copy(stage.at[v], (gwk_hbm, gwv_hbm)[v].at[:, pl.ds(W * g, W)], st_sem.at[v])

    def vec(ref):
        return ref[...].astype(F32).reshape(1, D)

    def move(s):
        for k in range(NB // FB):
            z = src[s % B8, FB * k:FB * (k + 1)].reshape(QW, D)
            z = jnp.dot(perm[...], z, preferred_element_type=F32)
            dst[s % B8, :, FB * k:FB * (k + 1), :] = z.astype(BF).reshape(FB, FB, D)

    def job_y(n):
        hf = h[rows(n)].astype(F32)
        x_hat, _ = norm_parts(hf)
        x[rows(n)] = (x_hat * vec(gain) + vec(shift)).astype(BF)
        y[rows(n)] = (hf + jnp.dot(res[0, rows(n)], wo[...], preferred_element_type=F32) + vec(bo)).astype(BF)

    def job_wo(n):
        gw[n] = dotg(res[0, :, rows(n)], dy[...], 0, 0)

    def job_h(n):
        x_hat, inv_std = norm_parts(h[rows(n)].astype(F32))
        dyf = dy[rows(n)].astype(F32)
        d_x = dotg(res[1, rows(n)], wq[...], 1, 1)
        for k, a in enumerate((d_x * x_hat, d_x, dyf)):
            sums[k:k + 1] += jnp.sum(a, axis=0, keepdims=True)
        d_hat = d_x * vec(gain)
        d_h = inv_std * (d_hat - jnp.mean(d_hat, axis=-1, keepdims=True) - x_hat * jnp.mean(d_hat * x_hat, axis=-1, keepdims=True))
        gh[rows(n)] = (dyf + d_h).astype(BF)

    def job_wq(n):
        gw[n] = dotg(x[:, rows(n)], res[1], 0, 0)

    for k in range(B8 - 1):
        src_copy(k).start()
    for cp in loads:
        cp.start()
    piece_in(0).start()
    piece_in(1).start()
    sums[...] = jnp.zeros_like(sums)
    perm[...] = permutation(FB)
    for ref, k in ((dbq, 0), (dbv, B8)):
        ref[...] = jnp.concatenate([bias[k:k + 1], bias[k + 1:k + 2]], axis=1).reshape(D)
    outs = ((job_y, lambda n: out_copy(y, y_hbm, y_sem, n)), (job_wo, lambda n: gw_copy(gwo_hbm, n)),
            (job_h, lambda n: out_copy(gh, gh_hbm, gh_sem, n)), (job_wq, lambda n: gw_copy(gwq_hbm, n)))
    needs = (loads[:3], loads[3:4], loads[4:], ())

    def step(s, carry):
        src_copy(s).wait()

        @pl.when(s + B8 - 1 < NFB)
        def _():
            src_copy(s + B8 - 1).start()

        @pl.when(s >= B8)
        def _():
            dst_copy(s - B8).wait()

        job = s - JOB0
        n = job % JOBS
        for kind, (f, copy) in enumerate(outs):
            @pl.when((job >= kind * JOBS) & (job < (kind + 1) * JOBS))
            def _():
                if needs[kind]:
                    @pl.when(n == 0)
                    def _():
                        for cp in needs[kind]:
                            cp.wait()
                if kind == 3:
                    gw_copy(gwo_hbm, n).wait()
                move(s)
                f(n)
                copy(n).start()

        @pl.when((job < 0) | (job >= JOBS * JOBS))
        def _():
            move(s)

        @pl.when(s < NFB - 1)
        def _():
            dst_copy(s).start()

        for v in range(2):
            @pl.when(s == JOBS + v)
            def _():
                piece_in(v).wait()
                piece_out(v).start()

            @pl.when(s == B8 + v)
            def _():
                piece_out(v).wait()
                piece_in(v + 2).start()

            @pl.when(s == B8 + JOBS + v)
            def _():
                piece_in(v + 2).wait()
                piece_out(v + 2).start()
        return carry

    lax.fori_loop(0, NFB, step, 0)
    last_copy().start()
    for k, ref in enumerate((dg, db, dbo)):
        ref[...] = sums[k:k + 1].reshape(D)
    for k in range(JOBS):
        out_copy(y, y_hbm, y_sem, k).wait()
        out_copy(gh, gh_hbm, gh_sem, k).wait()
        gw_copy(gwq_hbm, k).wait()
    piece_out(2).wait()
    piece_out(3).wait()
    for k in range(2, B8 + 1):
        dst_copy(NFB - k).wait()
    last_copy().wait()


def finish(dm, res, h, dy, w_o, w_q, dw, bias, gain, shift, b_o):
    hbm, vm = pl.BlockSpec(memory_space=pl.ANY), pl.BlockSpec(memory_space=VMEM)
    dma = pltpu.SemaphoreType.DMA
    mat, dj, d2, d8, vec = VMEM((D, D), BF), dma((JOBS,)), dma((B2,)), dma((B8,)), SDS((D,), F32)
    return pl.pallas_call(
        finish_kernel, name="finish",
        out_shape=(SDS((F, NB, D), BF), SDS((TOK, D), BF), SDS((TOK, D), BF)) + (SDS((D, D), F32),) * B4 + (vec,) * (B4 + 1),
        in_specs=[hbm] * (B8 - 1) + [vm] * B4,
        out_specs=(hbm,) * (B8 - 1) + (vm,) * (B4 + 1),
        scratch_shapes=[
            VMEM((B8, NB, FB, D), BF), VMEM((B8, FB, NB, D), BF), VMEM((QW, QW), BF), VMEM((B2, TOK, D), BF), mat, mat, mat, mat, mat,
            mat, mat, VMEM((JOBS, RC, D), F32), VMEM((B2, D, W), F32), VMEM((B8, D), F32), d8, d8, d8, dj, dj, dj, d2, d2],
        compiler_params=pltpu.CompilerParams(vmem_limit_bytes=67043328),
    )(dm, res, h, dy, w_o, w_q, dw, bias, gain, shift, b_o)


def block_mask():
    return lax.broadcasted_iota(jnp.int32, (128, 256), 0) // T == lax.broadcasted_iota(jnp.int32, (128, 256), 1) // HEAD


def block_diag(x, mask):
    return jnp.where(mask, jnp.concatenate([x] * 4, axis=0), jnp.zeros((), BF))


def when(cond):
    if isinstance(cond, bool):
        return (lambda f: f()) if cond else (lambda f: None)
    return pl.when(cond)


CH = (64, 128)
NCH = tuple(D // 2 // rows for rows in CH)
TS = (7, 3)
T3, T4 = (10, 4), (13, 6)


ALL, FILL, DRAIN = range(3)


def attn_kernel(m_hbm, h_hbm, dy_hbm, wq_hbm, wo_hbm, wk_hbm, wv_hbm, gain, shift, bq, bv,
                res_hbm, dw_hbm, bias_hbm, dm_hbm, dkv_hbm, mp_hbm,
                raw, perm, bv32, frames, q, do, wk, wv, kv, e_s, dp_s, mt, stats, coef, dkv, acc, bias, od, r1, keep, x2, r2, res, big1, big2,
                raw_sem, in_sem, dkv_sem, dm_sem, out_sem, st_send, st_recv, s1_send, s1_recv, s2_send, s2_recv,
                s3_send, s3_recv, s3s_send, s4_send, res_recv, e1_send, e1_recv, e2_send, e2_recv,
                e3_send, e3_recv, e3s_send, e4_send, acc_recv, b_send, b_recv, keep_sem, load_sem, e1p_send, e1p_recv, free_sib, free_xn):
    me = lax.axis_index("cp")
    cx, cc = me // 2, me % 2
    sib, xn = 2 * cx + 1 - cc, 2 * (1 - cx) + cc

    def vec(ref):
        return ref[...].astype(F32).reshape(1, D)

    def remote(src, dst, ss, rs, dev):
        return pltpu.make_async_remote_copy(src_ref=src, dst_ref=dst, send_sem=ss, recv_sem=rs,
                                            device_id={"cp": dev}, device_id_type=MESH)

    def raw_copy(c):
        seqs = pl.ds(pl.multiple_of(B8 * (c // B4 % B4), B8), B8)
        return pltpu.make_async_copy(m_hbm.at[:, seqs, quarter(c)], raw.at[c % 2, 0:F], raw_sem.at[c % 2])

    def quarter(c):
        return pl.ds(pl.multiple_of(c % B4 * QW, QW), QW)

    def sort_frames(c):
        for n in range(NFC):
            x = raw[c % 2, FC * n:FC * (n + 1)].reshape(QW, QW)
            y = jnp.dot(perm[...], x, preferred_element_type=F32).astype(BF)
            for b in range(B8):
                frames[c // B4 % 2, FP * b + FC * n:FP * b + FC * (n + 1), quarter(c)] = y[FC * b:FC * (b + 1)]

    def dkv_copy(i):
        return pltpu.make_async_copy(dkv.at[i % 2], dkv_hbm.at[i // NP, i % NP], dkv_sem.at[i % 2])

    def stat_send(i):
        for k in range(1, B4):
            remote(stats.at[i % B4, me], stats.at[i % B4, me], st_send.at[i % B4], st_recv.at[i % B4], (me + k) % B4).start()

    def stat_wait(i):
        three = stats.at[i % B4, 0:3]
        for sem in (st_recv, st_send):
            pltpu.make_async_copy(three, three, sem.at[i % B4]).wait()

    def s1(b):
        return remote(od.at[b % 2, 1 - cc], r1.at[b % 4], s1_send.at[b % 4], s1_recv.at[b % 4], sib)

    def s2(b):
        return remote(x2.at[b % 4], r2.at[b % 8], s2_send.at[b % 8], s2_recv.at[b % 8], xn)

    def res_at(b, x):
        return res.at[cc, pl.ds(pl.multiple_of(64 * (b % NP) + T * x, T), T), pl.ds(pl.multiple_of(W * (b // NP), W), W)]

    def s3(b, x):
        return remote(res_at(b, x), res_at(b, x), s3_send, s3_recv.at[b % (2 * B8)], xn)

    def s3s(b):
        return remote(res_at(b, cx), res_at(b, cx), s3s_send, res_recv, sib)

    def s4(b):
        return remote(res_at(b, 1 - cx), res_at(b, 1 - cx), s4_send, res_recv, sib)

    def on(mode, b, k):
        return True if mode == ALL else b >= k if mode == FILL else b - k < STEPS

    def od_wait(b, mode):
        @when(on(mode, b, 8))
        def _():
            s3(b - 8, 1 - cx).wait_recv()

        @when(on(mode, b, 5))
        def _():
            s2(b - 5).wait_recv()
            s2(b - 5).wait_send()

        @when(on(mode, b, 2))
        def _():
            s1(b - 2).wait_send()
            s1(b - 2).wait_recv()

    def od_sum(b, mode):
        @when(on(mode, b, 5))
        def _():
            res_at(b - 5, cx)[...] = (keep[(b - 5) % B4] + r2[(b - 5) % B8]).astype(BF)

        @when(on(mode, b, 2))
        def _():
            for ref, x in ((keep, cx), (x2, 1 - cx)):
                rows = pl.ds(pl.multiple_of(T * x, T), T)
                ref[(b - 2) % B4] = od[b % 2, cc, rows, :] + r1[(b - 2) % B4, rows, :]

    def od_send(b, mode):
        @when(on(mode, b, 2))
        def _():
            s2(b - 2).start()

        @when(on(mode, b, 5))
        def _():
            s3(b - 5, cx).start()
            s3s(b - 5).start()

        @when(on(mode, b, 8))
        def _():
            s4(b - 8).start()

    own = pl.ds(pl.multiple_of(W * cc, W), W)
    other = pl.ds(pl.multiple_of(W * (1 - cc), W), W)

    def rows_of(g, x, n):
        return pl.ds(pl.multiple_of(x * (D // 2) + CH[g] * n, CH[g]), CH[g])

    def chunk_of(g, n):
        return big2.at[g, pl.ds(pl.multiple_of(CH[g] * n, CH[g]), CH[g])]

    def e1(g):
        return remote(acc.at[g, :, other], big1, e1_send.at[g], e1_recv.at[g], sib)

    def e1_part(n, x):
        rows = rows_of(1, x, n)
        return remote(acc.at[1, rows, other], big1.at[rows], e1p_send.at[n], e1p_recv.at[n], sib)

    def e1_wait(n, sem):
        both = big1.at[0:2 * CH[1]]
        pltpu.make_async_copy(both, both, sem.at[n]).wait()

    def e2(g, n):
        return remote(acc.at[g, rows_of(g, 1 - cx, n), own], chunk_of(g, n), e2_send.at[g, n], e2_recv.at[g, n], xn)

    def e3(g, n, x):
        ref = acc.at[g, rows_of(g, x, n), own]
        return remote(ref, ref, e3_send.at[g, n], e3_recv.at[g, n], xn)

    def to_sib(g, n, x, sem):
        ref = acc.at[g, rows_of(g, x, n), own]
        return remote(ref, ref, sem.at[g, n], acc_recv.at[g], sib)

    def dw_copy(g):
        return pltpu.make_async_copy(acc.at[g], dw_hbm.at[g], out_sem.at[g])

    def reduce_core(g, n):
        if g == 1:
            e1_wait(n, e1p_recv)
        for x in (cx, 1 - cx):
            acc[g, rows_of(g, x, n), own] += big1[rows_of(g, x, n), :]
        e2(g, n).start()

    def sent(g, n):
        e2(g, n).wait_send()
        pl.semaphore_signal(free_xn.at[g], inc=1, device_id={"cp": xn}, device_id_type=MESH)

    def reduce_chip(g, n):
        e2(g, n).wait_recv()
        pl.semaphore_wait(free_xn.at[g], 1)
        acc[g, rows_of(g, cx, n), own] += chunk_of(g, n)[...]
        e3(g, n, cx).start()
        to_sib(g, n, cx, e3s_send).start()

    def forward(g, n):
        e3(g, n, 1 - cx).wait_recv()
        to_sib(g, n, 1 - cx, e4_send).start()

    def gathered(g):
        half = acc.at[g, :, other]
        remote(half, half, e1_send.at[g], acc_recv.at[g], sib).wait_recv()
        for n in range(NCH[g]):
            e3(g, n, cx).wait_send()
            to_sib(g, n, cx, e3s_send).wait_send()
            to_sib(g, n, 1 - cx, e4_send).wait_send()
        dw_copy(g).start()

    def exchange(g, t, t3, t4):
        def chunk(t0, f):
            n = t - t0
            if isinstance(n, int):
                if 0 <= n < NCH[g]:
                    f(g, n)
            else:
                pl.when((n >= 0) & (n < NCH[g]))(lambda: f(g, n))

        @when(t == 0)
        def _():
            if g == 0:
                e1(g).start()
            else:
                for n in range(NCH[1]):
                    e1_part(n, 0).start()
                    e1_part(n, 1).start()

        @when(t == 1 + g)
        def _():
            if g == 0:
                e1(g).wait_send()
                e1(g).wait_recv()
            else:
                for n in range(NCH[1]):
                    e1_wait(n, e1p_send)
            pl.semaphore_signal(free_sib.at[g], inc=1, device_id={"cp": sib}, device_id_type=MESH)

        @when(t == t3)
        def _():
            pl.semaphore_wait(free_sib.at[g], 1)

        chunk(1, reduce_core)
        chunk(TS[g], sent)
        chunk(t3, reduce_chip)
        chunk(t4, forward)

    def operands(i, j, h):
        cols = pl.ds(pl.multiple_of(W * (i // NP) + 256 * h, 256), 256)
        rows = pl.ds(pl.multiple_of(64 * (i % NP) + T * j, T), T)
        mask = block_mask()
        return block_diag(q[rows, cols], mask), block_diag(do[rows, cols], mask), mask

    def rows_of_pair(i):
        return frames[i // B4 % 2, pl.ds(pl.multiple_of(i % B4 * ROWS, ROWS), ROWS), :]

    def project(i):
        cols = pl.ds(pl.multiple_of(W * (i // NP), W), W)
        m = rows_of_pair(i)
        kv[i % 3, :, 0:W] = jnp.dot(m, wk[:, cols], preferred_element_type=F32).astype(BF)
        kv[i % 3, :, W:] = (jnp.dot(m, wv[:, cols], preferred_element_type=F32) + bv32[:, cols]).astype(BF)
        mt[i % 3] = m.T

    def scores(i):
        slot = i % 2
        full = FP - 2 * B8
        real = lax.broadcasted_iota(jnp.int32, (FP - full, LANES), 0) < F - full
        for j in range(2):
            rows = slice(FP * j, FP * (j + 1))
            for h in range(2):
                n = 2 * j + h
                qb, db, _ = operands(i, j, h)
                s = dotg(kv[i % 3, rows, QW * h:QW * (h + 1)], qb, 1, 1)
                dp = dotg(kv[i % 3, rows, W + QW * h:W + QW * (h + 1)], db, 1, 1)
                s = jnp.concatenate([s[:full], jnp.where(real, s[full:], -1e30)], axis=0)
                top = jnp.max(s, axis=0, keepdims=True)
                e = jnp.exp2((s - top) * LOG2)
                e_s[slot, n] = e
                dp_s[slot, n] = dp
                for k, row in enumerate((top, jnp.sum(e, axis=0, keepdims=True), jnp.sum(e * dp, axis=0, keepdims=True))):
                    stats[i % B4, me, B4 * k + n:B4 * k + n + 1, :] = row

    def combine(i):
        slot = i % 4
        tops = [stats[slot, d, 0:4, :] for d in range(4)]
        top = jnp.maximum(jnp.maximum(tops[0], tops[1]), jnp.maximum(tops[2], tops[3]))
        ws = [jnp.exp2((t - top) * LOG2) for t in tops]
        total = sum(stats[slot, d, 4:8, :] * ws[d] for d in range(4))
        dots = sum(stats[slot, d, 8:12, :] * ws[d] for d in range(4))
        coef[0:4, :] = jnp.exp2((stats[slot, me, 0:4, :] - top) * LOG2) / total
        coef[4:8, :] = dots / total

    def grads(i):
        slot, grp = i % 2, i // NP
        blocks = []
        for j in range(2):
            rows = slice(FP * j, FP * (j + 1))
            for h in range(2):
                n = 2 * j + h
                qb, db, _ = operands(i, j, h)
                ck, cv = slice(QW * h, QW * (h + 1)), slice(W + QW * h, W + QW * (h + 1))
                p = e_s[slot, n] * coef[n:n + 1, :]
                pb = p.astype(BF)
                gb = (p * (dp_s[slot, n] - coef[B4 + n:B4 + n + 1, :]) * 0.125).astype(BF)
                dk = jnp.dot(gb, qb, preferred_element_type=F32)
                dv = jnp.dot(pb, db, preferred_element_type=F32)
                dkv[slot, rows, ck] = dk.astype(BF)
                dkv[slot, rows, cv] = dv.astype(BF)
                bias[me, pl.ds(grp, 1), cv] += jnp.sum(dv, axis=0, keepdims=True)
                blocks.append((j, h, pb, gb))
        return blocks

    def sums(i, blocks):
        mask = block_mask()
        for j, h, pb, gb in blocks:
            rows = slice(FP * j, FP * (j + 1))
            ck, cv = slice(QW * h, QW * (h + 1)), slice(W + QW * h, W + QW * (h + 1))
            for which, x in ((0, dotg(pb, kv[i % 3, rows, cv], 0, 0)), (1, dotg(gb, kv[i % 3, rows, ck], 0, 0))):
                x = jnp.where(mask, x, 0.0)
                x = (x[0:32] + x[32:64]) + (x[64:96] + x[96:128])
                od[i % 2, which, T * j:T * (j + 1), ck] = x
                if which == 1:
                    bias[me, pl.ds(i // NP, 1), ck] += jnp.sum(x, axis=0, keepdims=True)

    def keep_copy(n):
        return pltpu.make_async_copy(frames.at[n % 2], mp_hbm.at[n % B4], keep_sem)

    def load_copy(n):
        return pltpu.make_async_copy(mp_hbm.at[n % B4], frames.at[n % 2], load_sem)

    def tiles(i, do_sort):
        n = i // B4
        if do_sort:
            raw_copy(i + B4).wait()

            @pl.when(i + B4 + 1 < NP)
            def _():
                raw_copy(i + B4 + 1).start()

        @pl.when(i % B4 == 0)
        def _():
            @pl.when((n >= 1) & (n <= B4))
            def _():
                keep_copy(n - 1).wait()

            @pl.when(n < B4)
            def _():
                keep_copy(n).start()

            if not do_sort:
                @pl.when(n >= B4)
                def _():
                    load_copy(n).wait()

                @pl.when((n >= B4 - 1) & (n < B8 - 1))
                def _():
                    load_copy(n + 1).start()

    def step(i, do_a, do_b, do_sort, mode):
        b = i - 2
        if do_b:
            @pl.when(b >= NP)
            def _():
                exchange(0, b - NP, T3[0], T4[0])

            stat_wait(b)

            @when(on(mode, b, 2))
            def _():
                dkv_copy(b - 2).wait()

            od_wait(b, mode)
        if do_a:
            tiles(i, do_sort)
        if do_b:
            od_sum(b, mode)
            combine(b)
        if do_a:
            project(i)
        if do_b:
            blocks = grads(b)
        if do_a:
            scores(i)
            if do_sort:
                sort_frames(i + B4)
        if do_b:
            acc[b // NP] += jnp.dot(mt[b % 3], dkv[b % 2], preferred_element_type=F32)
            sums(b, blocks)
        if do_a:
            stat_send(i)
        if do_b:
            dkv_copy(b).start()
            s1(b).start()
            od_send(b, mode)

    barrier = pltpu.get_barrier_semaphore()
    for k in range(1, B4):
        pl.semaphore_signal(barrier, inc=1, device_id={"cp": (me + k) % B4}, device_id_type=MESH)
    top, low = pl.ds(0, ROWS), pl.ds(ROWS, D - ROWS)
    rest = pl.ds(0, D - ROWS)
    loads = [pltpu.make_async_copy(x, y, in_sem.at[k]) for k, (x, y) in enumerate((
        (h_hbm, res.at[0]), (wq_hbm.at[top], kv.at[0]), (wq_hbm.at[low], dkv.at[0, rest]), (dy_hbm, res.at[1]),
        (wo_hbm.at[top], kv.at[1]), (wo_hbm.at[low], dkv.at[1, rest]), (wk_hbm, wk), (wv_hbm, wv)))]
    for cp in loads[:3]:
        cp.start()
    raw[:, F:] = jnp.zeros((B2, FP - F, B8, QW), BF)
    perm[...] = permutation(FC)
    bv32[...] = vec(bv)
    bias[me] = jnp.zeros((B8, D), F32)
    for cp in loads[:3]:
        cp.wait()
    for cp in loads[3:]:
        cp.start()
    raw_copy(0).start()

    def first(n, carry):
        rows = pl.ds(pl.multiple_of(RC * n, RC), RC)
        x_hat, _ = norm_parts(res[0, rows].astype(F32))
        x = (x_hat * vec(gain) + vec(shift)).astype(BF)
        q[rows] = (jnp.dot(x[:, :ROWS], kv[0], preferred_element_type=F32)
                   + jnp.dot(x[:, ROWS:], dkv[0, rest], preferred_element_type=F32) + vec(bq)).astype(BF)
        for g in range(2):
            acc[g, rows] = jnp.zeros((RC, D), F32)
        return carry

    def second(n, carry):
        raw_copy(n).wait()
        raw_copy(n + 1).start()
        rows = pl.ds(pl.multiple_of(RC * n, RC), RC)
        sort_frames(n)
        do[rows, :ROWS] = dotg(res[1, rows], kv[1], 1, 1).astype(BF)
        do[rows, ROWS:] = dotg(res[1, rows], dkv[1, rest], 1, 1).astype(BF)
        return carry

    lax.fori_loop(0, TOK // RC, first, 0)
    for cp in loads[3:-2]:
        cp.wait()
    lax.fori_loop(0, TOK // RC, second, 0)
    for cp in loads[-2:]:
        cp.wait()
    pl.semaphore_wait(barrier, 3)

    def run(lo, hi, *what):
        def body(i, carry):
            step(i, *what)
            return carry
        lax.fori_loop(lo, hi, body, 0)

    run(0, 2, True, False, True, FILL)
    run(2, NP - B4, True, True, True, FILL)
    run(NP - B4, STEPS, True, True, False, ALL)
    run(STEPS, STEPS + 2, False, True, False, ALL)

    def b_copy(k, src):
        return remote(bias.at[src], bias.at[src], b_send.at[k - 1], b_recv.at[src], (me + k) % 4)

    for k in range(1, 4):
        b_copy(k, me).start()
    dkv_copy(STEPS - 2).wait()
    dkv_copy(STEPS - 1).wait()

    def part(u, k):
        return frames.at[u % 2, pl.ds(ROWS * k, ROWS)]

    def c_load(u, k):
        return pltpu.make_async_copy(dkv_hbm.at[k % 2, 2 * u + k // 2], part(u, k), in_sem.at[k])

    def dm_copy(u, k):
        return pltpu.make_async_copy((kv, dkv)[k].at[u % 2], dm_hbm.at[2 * u + k], dm_sem.at[k, u % 2])

    for k in range(B4):
        c_load(0, k).start()
    exchange(1, 0, T3[1], T4[1])

    def c_step(u, carry):
        for k in range(B4):
            c_load(u, k).wait()

        @pl.when(u + 1 < NP // 2)
        def _():
            for k in range(B4):
                c_load(u + 1, k).start()

        @pl.when(u >= 2)
        def _():
            for k in range(2):
                dm_copy(u - 2, k).wait()

        @pl.when(u < B4)
        def _():
            for k in range(2):
                od_wait(STEPS + 2 * u + k, DRAIN)
                od_sum(STEPS + 2 * u + k, DRAIN)
                od_send(STEPS + 2 * u + k, DRAIN)

        exchange(1, u + 1, T3[1], T4[1])

        @pl.when(u == 0)
        def _():
            for n in range(NP - T3[0], NCH[0]):
                reduce_chip(0, n)

        @pl.when(u == 2)
        def _():
            for n in range(NP - T4[0], NCH[0]):
                forward(0, n)

        @pl.when(u == 4)
        def _():
            gathered(0)

        @pl.when(u == 6)
        def _():
            rows = res.at[0, 0:TOK // 2]
            for sem in (s3_send, s3s_send, s4_send):
                pltpu.make_async_copy(rows, rows, sem).wait()
            pltpu.make_async_copy(res.at[0], res.at[0], res_recv).wait()
            pltpu.make_async_copy(res, res_hbm, out_sem.at[2]).start()

        w = jnp.concatenate([wk[:, :W], wv[:, :W], wk[:, W:], wv[:, W:]], axis=1)
        for k in range(2):
            for j in range(2):
                rows = slice(FP * j, FP * (j + 1))
                x = jnp.concatenate([part(u, 2 * k)[rows], part(u, 2 * k + 1)[rows]], axis=1)
                (kv, dkv)[k][u % 2, rows] = dotg(x, w, 1, 1).astype(BF)
        for k in range(2):
            dm_copy(u, k).start()
        return carry

    lax.fori_loop(0, NP // 2, c_step, 0)
    for t in range(NP // 2 + 1, T4[1] + NCH[1]):
        exchange(1, t, T3[1], T4[1])
    gathered(1)
    for k in range(1, 4):
        b_copy(k, (me + k) % 4).wait_recv()
        b_copy(k, me).wait_send()
    big1[0:8, :] = (bias[0, :, 0:W] + bias[1, :, 0:W]) + (bias[2, :, 0:W] + bias[3, :, 0:W])
    big1[8:16, :] = (bias[0, :, W:] + bias[1, :, W:]) + (bias[2, :, W:] + bias[3, :, W:])
    bias_out = pltpu.make_async_copy(big1.at[0:16], bias_hbm, out_sem.at[3])
    bias_out.start()
    for u in (NP // 2 - 2, NP // 2 - 1):
        for k in range(2):
            dm_copy(u, k).wait()
    dw_copy(0).wait()
    dw_copy(1).wait()
    pltpu.make_async_copy(res, res_hbm, out_sem.at[2]).wait()
    bias_out.wait()


def attention(mt, h, dy, w_q, w_o, w_k, w_v, gain, shift, b_q, b_v):
    vm = pl.BlockSpec(memory_space=VMEM)
    hbm = pl.BlockSpec(memory_space=pl.ANY)
    dma = pltpu.SemaphoreType.DMA
    d2, d4, d8, dn = dma((B2,)), dma((B4,)), dma((B8,)), dma((B2, B8))
    credit = pltpu.SemaphoreType.REGULAR((B2,))
    probs, mat, rows32 = VMEM((B2, B4, FP, LANES), F32), VMEM((D, D), BF), VMEM((B4, T, W), F32)
    return pl.pallas_call(
        attn_kernel, name="attention",
        out_shape=(SDS((B2, TOK, D), BF), SDS((B2, D, D), F32), SDS((2 * B8, W), F32), SDS((NP, ROWS, D), BF),
                   SDS((B2, NP, ROWS, D), BF), SDS((B4, B8 * FP, D), BF)),
        in_specs=[hbm] * 7 + [vm] * B4,
        out_specs=(hbm,) * 6,
        scratch_shapes=[
            VMEM((B2, FP, B8, QW), BF), VMEM((QW, QW), BF), VMEM((1, D), F32), VMEM((B2, B8 * FP, D), BF), mat, mat, mat, mat,
            VMEM((3, ROWS, D), BF), probs, probs, VMEM((3, D, ROWS), BF), VMEM((B4, B4, 3 * B4, LANES), F32),
            VMEM((B8, LANES), F32), VMEM((B2, ROWS, D), BF), VMEM((B2, D, D), F32), VMEM((B4, B8, D), F32),
            VMEM((B2, B2, 2 * T, W), F32), VMEM((B4, 2 * T, W), F32), rows32, rows32, VMEM((B8, T, W), F32),
            VMEM((B2, TOK, D), BF), VMEM((D, W), F32), VMEM((B2, D // 2, W), F32),
            d2, d8, d2, dma((B2, B2)), d4, d4, d4, d4, d4, d8, d8, dma, dma((2 * B8,)), dma, dma, dma, d2, d2, dn, dn, dn, dn, dn, dn, d2, d4, d4,
            dma, dma, d4, d4, credit, credit],
        compiler_params=pltpu.CompilerParams(vmem_limit_bytes=67043328, collective_id=0, has_side_effects=True),
    )(mt, h, dy, w_q, w_o, w_k, w_v, gain, shift, b_q, b_v)


def solution(mesh):
    act_spec = P("dp", None, None)
    mem_spec = P("dp", "cp", None)
    vec_out = P("dp")
    mat_out = P("dp", None)
    in_specs = (act_spec, mem_spec, P(), P(), P(), P(), P(), P(), P(), P(), P(), act_spec)
    out_specs = (act_spec, act_spec, mem_spec, vec_out, vec_out, mat_out, vec_out, mat_out, mat_out, vec_out, mat_out, vec_out)

    def device_step(hidden, memory, ln_gain, ln_bias, w_q, b_q, w_k, w_v, b_v, w_o, b_o, grad_y):
        h = hidden.reshape(TOK, D)
        dy = grad_y.reshape(TOK, D)
        res, dw, bias, dm, _, _ = attention(memory.transpose(1, 0, 2), h, dy, w_q, w_o, w_k, w_v, ln_gain, ln_bias, b_q, b_v)
        gm, y, gh, gwo, gwq, gwk, gwv, dg, db, dbq, dbv, dbo = finish(
            dm.reshape(NB, FP, D), res, h, dy, w_o, w_q, dw, bias, ln_gain, ln_bias, b_o)
        return (y.reshape(NB, T, D), gh.reshape(NB, T, D), gm.transpose(1, 0, 2), dg, db, gwq, dbq, gwk, gwv, dbv, gwo, dbo)

    return jax.shard_map(device_step, mesh=mesh, in_specs=in_specs, out_specs=out_specs, check_vma=False)
```
